32 devices in a mesh: freq: 8 (over y, x, core), base: 4 (over z).
Axes of the slice: x: 2, y: 2, z: 4, core: 2. Of those that a mesh axis runs over, the one named last changes fastest.
Arguments:
- visibility: float32 [2, 16, 2048], P(None, 'freq', 'base'), may hold values from -6 to 6
- tile_of: int32 [16, 2048, 1], P('freq', 'base'), may hold values from 0 to 3; in each aligned block of 512 rows (0 to 511, 512 to 1023, ..., all dimensions but the last counted through in order) at most 256 rows name the same one
- u_within: int32 [16, 2048], P('freq', 'base'), may hold values from 0 to 255
- v_cell: int32 [16, 2048], P('freq', 'base'), may hold values from 0 to 1016
- kernel_index: int32 [2, 16, 2048], P(None, 'freq', 'base'), may hold values from 0 to 127
- kernel: float32 [128, 8], replicated, may hold values from 0.1 to 1
- live_count: int32 [16, 4], P('freq', 'base'), may hold values from 64 to 512, as said below
- bin_map: int32 [1024, 1024], P('base'), may hold values from 0 to 511, as said below
Outputs:
- power_map: float32 [1024, 1024], P('freq', 'base')
- spectrum: float32 [512], replicated
The draws below stay inside these ranges and needn't reach their ends.
Inputs may be any that keep to these rules, and one draw needn't show every extreme that they name: `tile_of`: among the visibilities of one channel on one device, at most 256 name the same tile, and in some device's visibilities a tile is named by exactly 256. `live_count`: the first device along base holds 512 used slots in every channel; the used slots of a device are its first ones. `bin_map`: every bin number occurs.
All inputs are finite; a program needn't handle non-finite values.
Results may differ from the reference program's by a relative error of at most 0.0003.
Values sent between devices are 32-bit elements; how exact they have to be, the bound alone decides.
A program may use at most 128 MiB of HBM per device.

```python
import math
import jax
import jax.numpy as jnp
import numpy as np
from jax import lax

G = 1024
NBINS = 512
KW = 8
OVER = 128
VIS_DEV = 512
CH_DEV = 2
TILE = 256
CAP = 256
CH = 16
VIS = 2048
N_FREQ = 8
N_BASE = 4


def draw_visibility(key, part):
    channels = CH_DEV * N_FREQ
    visits = VIS_DEV * N_BASE
    frequency = 100.0 + 60.0 * jnp.arange(channels, dtype=jnp.float32) / max(channels - 1, 1)
    falloff = (frequency / 100.0) ** (-2.6)
    values = jnp.clip(jax.random.normal(key, (2, channels, visits), jnp.float32), -6.0, 6.0)
    return values * falloff[None, :, None]


def draw_live_count(key, part):
    channels = CH_DEV * N_FREQ
    floor_count = VIS_DEV // 8
    device = jnp.arange(N_BASE, dtype=jnp.int32)
    spread = (VIS_DEV - floor_count) * (N_BASE - device) // N_BASE + 1
    additional = jax.random.randint(key, (channels, N_BASE), 0, spread[None, :])
    counts = floor_count + additional
    return jnp.where(device[None, :] == 0, VIS_DEV, counts).astype(jnp.int32)


def draw_bin_map(key, part):
    centre = jax.random.randint(key, (2,), -(G // 8), G // 8 + 1)
    positions = jnp.arange(G, dtype=jnp.int32)
    along_u = (positions - centre[0] + G // 2) % G - G // 2
    along_v = (positions - centre[1] + G // 2) % G - G // 2
    radius_sq = along_u[:, None] * along_u[:, None] + along_v[None, :] * along_v[None, :]
    return jnp.minimum(radius_sq * NBINS // (G // 2 * (G // 2)), NBINS - 1).astype(jnp.int32)


def plant(entries, stream_key, low, high):
    extent = entries.shape
    spot = [jax.random.randint(jax.random.fold_in(stream_key, axis), (), 0, extent[axis]) for axis in range(len(extent))]
    entries = entries.at[tuple(spot)].set(low)
    longest = extent.index(max(extent))
    spot[longest] = (spot[longest] + 1) % extent[longest]
    return entries.at[tuple(spot)].set(high)


def deal_out(key, own, number, rows, number_of, top, bound, slope):
    order = jax.random.permutation(key, number_of)
    heavy_load, usual = shares(number_of, rows * top, bound, slope, True), shares(number_of, rows * top, bound, slope, False)
    places = jnp.arange(number_of)

    def named(tallies, rotation):
        used = int((tallies > 0).sum())
        fixed = max(1, used // 4)
        passed = fixed + (places - fixed + rotation * (used - fixed)) % max(1, number_of - fixed)
        return jnp.zeros((number_of,), jnp.int32).at[order[jnp.where(places < fixed, places, passed)]].set(jnp.asarray(tallies, jnp.int32))

    tallies = jnp.where(number % 4 == 0, named(heavy_load, number // 4), named(usual, number - number // 4 - 1))
    mixed = jax.random.permutation(jax.random.fold_in(own, 3), number_of)
    giver, receiver = mixed[0:number_of // 2 * 2:2], mixed[1:number_of // 2 * 2:2]
    margin = jnp.minimum(tallies[giver] - 1, bound - tallies[receiver]) // 2
    margin = jnp.where((giver == order[0]) | (receiver == order[0]) | (tallies[receiver] == 0), 0, jnp.maximum(margin, 0))
    passed = jax.random.randint(jax.random.fold_in(own, 4), (number_of // 2,), 0, 1 << 20) % (margin + 1)
    tallies = tallies.at[giver].add(-passed).at[receiver].add(passed)
    items = jnp.searchsorted(jnp.cumsum(tallies), jnp.arange(rows * top), side="right").astype(jnp.int32)
    table = items.reshape(top, rows).T
    table = table[jax.random.permutation(jax.random.fold_in(own, 1), rows)]
    rotation = jax.random.randint(jax.random.fold_in(own, 2), (rows, 1), 0, top)
    return jnp.take_along_axis(table, (jnp.arange(top)[None, :] + rotation) % top, axis=1)


def shares(count, total, limit, skew, full):
    loads = [(1 << 20) // math.isqrt(rank ** skew) + 1 for rank in range(1, count + 1)]
    largest = limit if full else min(limit, max(-(-total // count), total * loads[0] // sum(loads)))
    least = 1 if total - largest >= count - 1 else 0
    given, surplus = [largest] + [least] * (count - 1), total - largest - least * (count - 1)
    while surplus > 0:
        free = [i for i in range(1, count) if given[i] < largest] or [i for i in range(1, count) if given[i] < limit]
        pool, remaining = sum([loads[i] for i in free]), surplus
        for i in free:
            more = min(limit - given[i], max(1, remaining * loads[i] // pool), surplus)
            given[i] = given[i] + more
            surplus = surplus - more
    return np.array(given)


def setup_inputs(seed: int = 0) -> dict:
    key_list = jax.random.split(jax.random.key(seed), 9)
    visibility = draw_visibility(jax.random.fold_in(key_list[8], 71), 0)
    tile_of_keys = jax.random.split(jax.random.fold_in(key_list[1], 1), CH * VIS // VIS_DEV)
    tile_of_turns = jax.random.permutation(jax.random.fold_in(key_list[1], 3), CH * VIS // VIS_DEV)
    tile_of = jax.vmap(lambda own, number: deal_out(jax.random.fold_in(key_list[1], 2), own, number, VIS_DEV, N_BASE, 1, CAP, 2))(tile_of_keys, tile_of_turns).reshape((CH, VIS, 1))
    u_within = plant(jax.random.randint(key_list[2], (CH, VIS), 0, TILE), jax.random.fold_in(key_list[2], 1), 0, TILE - 1).astype(jnp.int32)
    v_cell = plant(jax.random.randint(key_list[3], (CH, VIS), 0, G - KW + 1), jax.random.fold_in(key_list[3], 1), 0, G - KW).astype(jnp.int32)
    kernel_index = plant(jax.random.randint(key_list[4], (2, CH, VIS), 0, OVER), jax.random.fold_in(key_list[4], 1), 0, OVER - 1).astype(jnp.int32)
    kernel = jnp.clip(jnp.exp(jax.random.uniform(key_list[5], (OVER, KW), jnp.float32, math.log(0.1), math.log(1.0))), 0.1, 1.0)
    live_count = draw_live_count(jax.random.fold_in(key_list[8], 71), 0)
    bin_map = draw_bin_map(jax.random.fold_in(key_list[8], 71), 0)
    return {"visibility": visibility, "tile_of": tile_of, "u_within": u_within, "v_cell": v_cell, "kernel_index": kernel_index, "kernel": kernel, "live_count": live_count, "bin_map": bin_map}


def channel_power(visibility_re, visibility_im, tile_row, u_within, v_cell, index_u, index_v, used_slots, kernel):
    tile_rows = G // N_BASE
    u_cell = jnp.minimum(tile_row * tile_rows + u_within, G - KW)
    position = jnp.arange(VIS_DEV * N_BASE, dtype=jnp.int32)
    holder = position // VIS_DEV
    is_live = (position % VIS_DEV) < used_slots[holder]
    zeroed = jnp.zeros_like(visibility_re)
    real_part = jnp.where(is_live, visibility_re, zeroed)
    imag_part = jnp.where(is_live, visibility_im, zeroed)
    taps_u = kernel[index_u]
    taps_v = kernel[index_v]
    weight = taps_u[:, :, None] * taps_v[:, None, :]
    offsets = jnp.arange(KW, dtype=jnp.int32)
    row_cells = jnp.broadcast_to(u_cell[:, None, None] + offsets[None, :, None], weight.shape)
    col_cells = jnp.broadcast_to(v_cell[:, None, None] + offsets[None, None, :], weight.shape)
    grid_re = jnp.zeros((G, G), jnp.float32).at[row_cells, col_cells].add(weight * real_part[:, None, None])
    grid_im = jnp.zeros((G, G), jnp.float32).at[row_cells, col_cells].add(weight * imag_part[:, None, None])
    transformed = jnp.fft.fft2(grid_re + 1j * grid_im)
    return transformed.real * transformed.real + transformed.imag * transformed.imag


def reference(visibility, tile_of, u_within, v_cell, kernel_index, kernel, live_count, bin_map):
    def accumulate(running, channel_items):
        vis_re, vis_im, tile_row, within, column, index_u, index_v, used_slots = channel_items
        return running + channel_power(vis_re, vis_im, tile_row, within, column, index_u, index_v, used_slots, kernel), None

    channel_items = (visibility[0], visibility[1], tile_of[:, :, 0], u_within, v_cell, kernel_index[0], kernel_index[1], live_count)
    power_sum, _ = lax.scan(accumulate, jnp.zeros((G, G), jnp.float32), channel_items)
    channels = CH_DEV * N_FREQ
    visits = VIS_DEV * N_BASE
    power_map = power_sum / (channels * visits)
    flat_bins = bin_map.T.reshape(-1)
    totals = jax.ops.segment_sum(power_map.reshape(-1), flat_bins, num_segments=NBINS)
    counts = jax.ops.segment_sum(jnp.ones_like(power_map).reshape(-1), flat_bins, num_segments=NBINS)
    return power_map, totals / counts
```

```python
import functools
import math

import jax
import jax.numpy as jnp
import numpy as np
from jax import lax
from jax.experimental import pallas as pl
from jax.experimental.pallas import tpu as pltpu
from jax.sharding import PartitionSpec as P

NBINS = 512
BIN_LOW = 32
KW = 8
FINE = 32
SPREAD = FINE + KW
RADIX = 4
GROUP = 16
FIELDS = 8
LANES = 128
MESH = pl.DeviceIdType.MESH


def halves_of(x):
    high = x.astype(jnp.bfloat16)
    low = (x - high.astype(jnp.float32)).astype(jnp.bfloat16)
    return high, low


@functools.lru_cache(None)
def transform_tables(grid):
    slab = grid // RADIX
    u = RADIX * np.arange(slab)[None, None, :] + np.arange(RADIX)[:, None, None]
    angle = ((np.arange(slab)[None, :, None] * u) % grid) * (2.0 * math.pi / grid)
    x = np.concatenate([np.cos(angle), np.sin(angle)], axis=1).astype(np.float32)
    high = x.astype(jnp.bfloat16)
    low = (x - high.astype(np.float32)).astype(jnp.bfloat16)
    return high, low


def dot(a, b):
    return jnp.dot(a, b, preferred_element_type=jnp.float32)


def dot_rows(a, b):
    return lax.dot_general(a, b, (((1,), (1,)), ((), ())), preferred_element_type=jnp.float32)


def enter(peers):
    barrier = pltpu.get_barrier_semaphore()
    for peer in peers:
        pl.semaphore_signal(barrier, inc=1, device_id=peer, device_id_type=MESH)
    pl.semaphore_wait(barrier, len(peers))


def gather_kernel(
    split, base_count, tile_rows, grid, vis_ref, tile_ref, within_ref, column_ref, index_ref, live_ref,
    out_ref, send_sems, recv_sems
):
    freq, base = lax.axis_index("freq"), lax.axis_index("base")
    part = lax.rem(freq, split)
    first = freq - part
    channels, slots = within_ref.shape
    spot = pl.ds(pl.multiple_of(base * slots, slots), slots)
    lane = lax.broadcasted_iota(jnp.int32, (1, slots), 1)
    for c in range(channels):
        live = live_ref[c:c + 1, 0:1]
        is_live = lane < live
        u = jnp.minimum(tile_ref[c:c + 1, :] * tile_rows + within_ref[c:c + 1, :], grid - KW)
        rows = [
            jnp.where(is_live, vis_ref[0, c:c + 1, :], 0.0),
            jnp.where(is_live, vis_ref[1, c:c + 1, :], 0.0),
            u.astype(jnp.float32),
            column_ref[c:c + 1, :].astype(jnp.float32),
            index_ref[0, c:c + 1, :].astype(jnp.float32),
            index_ref[1, c:c + 1, :].astype(jnp.float32),
            jnp.broadcast_to(live, (1, slots)).astype(jnp.float32),
            jnp.zeros((1, slots), jnp.float32),
        ]
        out_ref[part * channels + c, :, spot] = jnp.concatenate(rows, axis=0)
    peers = []
    for d_part in range(split):
        for d_base in range(base_count):
            if d_part or d_base:
                peers.append({
                    "freq": first + lax.rem(part + d_part, split),
                    "base": lax.rem(base + d_base, base_count),
                })
    enter(peers)
    mine = out_ref.at[pl.ds(part * channels, channels), :, spot]
    copies = []
    for k, peer in enumerate(peers):
        copy = pltpu.make_async_remote_copy(
            src_ref=mine, dst_ref=mine, send_sem=send_sems.at[k], recv_sem=recv_sems.at[k],
            device_id=peer, device_id_type=MESH,
        )
        copy.start()
        copies.append(copy)
    for copy in copies:
        copy.wait()


def gather_fields(split, base_count, tile_rows, grid, *arrays):
    channels, slots = arrays[2].shape
    peers = split * base_count - 1
    vmem = pl.BlockSpec(memory_space=pltpu.VMEM)
    return pl.pallas_call(
        functools.partial(gather_kernel, split, base_count, tile_rows, grid),
        out_shape=jax.ShapeDtypeStruct((channels * split, FIELDS, slots * base_count), jnp.float32),
        in_specs=[vmem] * len(arrays),
        out_specs=vmem,
        scratch_shapes=[pltpu.SemaphoreType.DMA((peers,)), pltpu.SemaphoreType.DMA((peers,))],
        compiler_params=pltpu.CompilerParams(collective_id=0, has_side_effects=True),
    )(*arrays)


def phase(product, grid):
    half = grid // 2
    angle = ((product + half) & (grid - 1)) - half
    angle = angle.astype(jnp.float32) * (2.0 * math.pi / grid)
    return jnp.cos(angle), jnp.sin(angle)


def image_kernel(
    grid, scale, split, slots, f_ref, kernel_ref, dh_hbm, dl_hbm, out_ref,
    fine_ref, coarse_ref, h_ref, y_ref, dh_ref, dl_ref, sems
):
    channel = pl.program_id(0)
    cols = out_ref.shape[1]
    slab = grid // RADIX
    period = RADIX * GROUP
    coarse_count = grid // FINE
    piece = min(256, slots)
    load_h = pltpu.make_async_copy(dh_hbm, dh_ref, sems.at[0])
    load_l = pltpu.make_async_copy(dl_hbm, dl_ref, sems.at[1])

    @pl.when(channel == 0)
    def _():
        load_h.start()
        load_l.start()
        out_ref[...] = jnp.zeros_like(out_ref)
        left = (lax.axis_index("base") * split + lax.rem(lax.axis_index("freq"), split)) * cols
        l = left + lax.broadcasted_iota(jnp.int32, (cols, SPREAD), 0)
        c, s = phase(l * lax.broadcasted_iota(jnp.int32, (cols, SPREAD), 1), grid)
        fine = jnp.concatenate(
            [jnp.concatenate([c, s], axis=1), jnp.concatenate([-s, c], axis=1)], axis=0
        )
        fh, fl = halves_of(fine)
        fine_ref[...] = jnp.zeros_like(fine_ref)
        fine_ref[:, 0:2 * SPREAD] = fh
        fine_ref[:, 2 * SPREAD:4 * SPREAD] = fl
        fine_ref[:, 4 * SPREAD:6 * SPREAD] = fh
        l = left + lax.broadcasted_iota(jnp.int32, (cols, coarse_count), 0)
        c, s = phase(l * lax.broadcasted_iota(jnp.int32, (cols, coarse_count), 1) * FINE, grid)
        ch, cl = halves_of(jnp.concatenate([c, -s], axis=0))
        coarse_ref[:, 0:coarse_count] = ch
        coarse_ref[:, coarse_count:] = cl

    h_ref[...] = jnp.zeros_like(h_ref)
    taps_table = kernel_ref[...]

    def look_up(row):
        pieces = []
        for at in range(0, piece, LANES):
            index = jnp.broadcast_to(row[:, at:at + LANES], (KW, LANES))
            pieces.append(jnp.take_along_axis(taps_table, index, axis=1))
        return jnp.concatenate(pieces, axis=1)

    def piece_step(start):
        at = pl.ds(pl.multiple_of(start, piece), piece)
        re, im = f_ref[0, 0:1, at], f_ref[0, 1:2, at]
        u = f_ref[0, 2:3, at].astype(jnp.int32)
        v = f_ref[0, 3:4, at].astype(jnp.int32)
        taps_u = look_up(f_ref[0, 4:5, at].astype(jnp.int32))
        taps_v = look_up(f_ref[0, 5:6, at].astype(jnp.int32))

        offset = lax.broadcasted_iota(jnp.int32, (SPREAD, piece), 0) - (v & (FINE - 1))
        spread = jnp.zeros((SPREAD, piece), jnp.float32)
        for t in range(KW):
            spread = jnp.where(offset == t, taps_v[t:t + 1, :], spread)
        both = jnp.concatenate([spread * re, spread * im], axis=0)
        bh, bl = halves_of(both)
        pad = jnp.zeros((256 - 6 * SPREAD, piece), jnp.bfloat16)
        zb = dot(fine_ref[...], jnp.concatenate([bh, bh, bl, pad], axis=0))
        pick = lax.broadcasted_iota(jnp.int32, (2 * coarse_count, piece), 0) & (coarse_count - 1)
        onehot = jnp.where(pick == v // FINE, 1.0, 0.0).astype(jnp.bfloat16)
        e = dot(coarse_ref[...], onehot)
        zr, zi = zb[:cols], zb[cols:]
        er, ei = e[:cols], e[cols:]
        z = jnp.concatenate([zr * er - zi * ei, zr * ei + zi * er], axis=0)
        zh, zl = halves_of(z)

        for first in range(RADIX):
            residue = RADIX * lax.broadcasted_iota(jnp.int32, (GROUP, piece), 0) + first
            tap = (residue - u) & (period - 1)
            group = (u + tap - residue) // period
            r = jnp.zeros((GROUP, piece), jnp.float32)
            for t in range(KW):
                r = jnp.where(tap == t, taps_u[t:t + 1, :], r)
            rh, rl = halves_of(r)
            q = group.astype(jnp.float32).astype(jnp.bfloat16)
            zero = jnp.zeros_like(rh)
            hits = [q == jnp.bfloat16(g) for g in range(slab // GROUP)]
            wh = jnp.concatenate([jnp.where(hit, rh, zero) for hit in hits], axis=0)
            wl = jnp.concatenate([jnp.where(hit, rl, zero) for hit in hits], axis=0)
            h_ref[first] += dot_rows(wh, zh) + dot_rows(wh, zl) + dot_rows(wl, zh)

    blocks = f_ref.shape[2] // slots

    def block_step(block, carry):
        live = jnp.max(f_ref[0, 6:7, pl.ds(pl.multiple_of(block * slots, slots), LANES)])
        for inner in range(slots // piece):
            @pl.when(live > float(inner * piece))
            def _():
                piece_step(block * slots + inner * piece)
        return carry

    lax.fori_loop(0, blocks, block_step, 0)

    @pl.when(channel == 0)
    def _():
        load_h.wait()
        load_l.wait()

    def transform_step(first, carry):
        hh, hl = halves_of(h_ref[first])
        dh = dh_ref[first]
        y_ref[first] = dot(dh, hh) + dot(dh, hl) + dot(dl_ref[first], hh)
        return carry

    lax.fori_loop(0, RADIX, transform_step, 0)

    def combine(block, carry):
        rows = 32
        top = pl.multiple_of(block * rows, rows)
        low = pl.multiple_of(slab + block * rows, rows)
        yr, yi = [], []
        for first in range(RADIX):
            cy = y_ref[first, pl.ds(top, rows), :]
            sy = y_ref[first, pl.ds(low, rows), :]
            yr.append(cy[:, :cols] + sy[:, cols:])
            yi.append(cy[:, cols:] - sy[:, :cols])
        ar, ai = yr[0] + yr[2], yi[0] + yi[2]
        br, bi = yr[0] - yr[2], yi[0] - yi[2]
        cr, ci = yr[1] + yr[3], yi[1] + yi[3]
        dr, di = yr[1] - yr[3], yi[1] - yi[3]
        parts = [
            (ar + cr, ai + ci), (br + di, bi - dr), (ar - cr, ai - ci), (br - di, bi + dr)
        ]
        for k, (xr, xi) in enumerate(parts):
            at = pl.ds(pl.multiple_of(k * slab + block * rows, rows), rows)
            out_ref[at, :] += (xr * xr + xi * xi) * scale
        return carry

    lax.fori_loop(0, slab // 32, combine, 0)


def image_power(fields, taps_table, dh, dl, grid, cols, split, slots, scale):
    channels, field_count, total = fields.shape
    slab = grid // RADIX
    bf16, f32 = jnp.bfloat16, jnp.float32
    anywhere = pl.BlockSpec(memory_space=pl.ANY)
    return pl.pallas_call(
        functools.partial(image_kernel, grid, scale, split, slots),
        grid=(channels,),
        out_shape=jax.ShapeDtypeStruct((grid, cols), f32),
        in_specs=[
            pl.BlockSpec((1, field_count, total), lambda c: (c, 0, 0)),
            pl.BlockSpec(taps_table.shape, lambda c: (0, 0)),
            anywhere, anywhere,
        ],
        out_specs=pl.BlockSpec((grid, cols), lambda c: (0, 0)),
        scratch_shapes=[
            pltpu.VMEM((2 * cols, 256), bf16),
            pltpu.VMEM((2 * cols, 2 * (grid // FINE)), bf16),
            pltpu.VMEM((RADIX, slab, 2 * cols), f32),
            pltpu.VMEM((RADIX, 2 * slab, 2 * cols), f32),
            pltpu.VMEM(dh.shape, bf16),
            pltpu.VMEM(dl.shape, bf16),
            pltpu.SemaphoreType.DMA((2,)),
        ],
        compiler_params=pltpu.CompilerParams(
            vmem_limit_bytes=40 * 2**20, dimension_semantics=("arbitrary",)
        ),
    )(fields, taps_table, dh, dl)


def exchange_kernel(
    freq_count, base_count, split, power_ref, bins_ref, share_ref, spectrum_ref,
    recv_ref, a_ref, b_ref, stage_ref, stage2_ref, send_sems, recv_sems
):
    freq, base = lax.axis_index("freq"), lax.axis_index("base")
    share_rows, width = share_ref.shape
    cols = width // split
    ring = [{"freq": lax.rem(freq + d, freq_count), "base": base} for d in range(1, freq_count)]
    line = [{"freq": freq, "base": lax.rem(base + d, base_count)} for d in range(1, base_count)]
    enter(ring + line)
    copies = []
    for k, peer in enumerate(ring):
        top = pl.multiple_of(peer["freq"] * share_rows, share_rows)
        copy = pltpu.make_async_remote_copy(
            src_ref=power_ref.at[pl.ds(top, share_rows), :],
            dst_ref=recv_ref.at[freq],
            send_sem=send_sems.at[k], recv_sem=recv_sems.at[k],
            device_id=peer, device_id_type=MESH,
        )
        copy.start()
        copies.append(copy)
    recv_ref[freq] = power_ref[pl.ds(pl.multiple_of(freq * share_rows, share_rows), share_rows), :]
    bins = bins_ref[...].T
    for copy in copies:
        copy.wait()
    halves = []
    for part in range(split):
        total = recv_ref[part]
        for group in range(1, freq_count // split):
            total = total + recv_ref[group * split + part]
        halves.append(total)
    share_ref[...] = jnp.concatenate(halves, axis=1)

    rows, columns = share_rows, width
    high_count = NBINS // BIN_LOW
    for k in range(rows):
        at = slice(k * columns, (k + 1) * columns)
        value = share_ref[k:k + 1, :]
        bin_id = bins[k:k + 1, :]
        hit = lax.broadcasted_iota(jnp.int32, (high_count, columns), 0) == bin_id // BIN_LOW
        high = value.astype(jnp.bfloat16).astype(jnp.float32)
        low = value - high
        a_ref[0:high_count, at] = jnp.where(hit, high, 0.0).astype(jnp.bfloat16)
        a_ref[high_count:2 * high_count, at] = jnp.where(hit, low, 0.0).astype(jnp.bfloat16)
        a_ref[2 * high_count:, at] = jnp.where(hit, 1.0, 0.0).astype(jnp.bfloat16)
        hit = lax.broadcasted_iota(jnp.int32, (BIN_LOW, columns), 0) == bin_id % BIN_LOW
        b_ref[:, at] = jnp.where(hit, 1.0, 0.0).astype(jnp.bfloat16)
    sums = dot_rows(a_ref[...], b_ref[...])
    stage_ref[freq, 0] = sums[:high_count] + sums[high_count:2 * high_count]
    stage_ref[freq, 1] = sums[2 * high_count:]

    def share_out(ref, me, peers, offset):
        copies = []
        for k, peer in enumerate(peers):
            copy = pltpu.make_async_remote_copy(
                src_ref=ref.at[me], dst_ref=ref.at[me],
                send_sem=send_sems.at[offset + k], recv_sem=recv_sems.at[offset + k],
                device_id=peer, device_id_type=MESH,
            )
            copy.start()
            copies.append(copy)
        for copy in copies:
            copy.wait()
        total = ref[0]
        for other in range(1, ref.shape[0]):
            total = total + ref[other]
        return total

    stage2_ref[base] = share_out(stage_ref, freq, ring, len(ring))
    total = share_out(stage2_ref, base, line, 2 * len(ring))
    spectrum_ref[...] = total[0] / total[1]


def exchange(power, bins, freq_count, base_count, split, width):
    grid, cols = power.shape
    share_rows = grid // freq_count
    high_count = NBINS // BIN_LOW
    cells = share_rows * width
    sems = 2 * (freq_count - 1) + base_count - 1
    f32, bf16 = jnp.float32, jnp.bfloat16
    vmem = pl.BlockSpec(memory_space=pltpu.VMEM)
    return pl.pallas_call(
        functools.partial(exchange_kernel, freq_count, base_count, split),
        out_shape=(
            jax.ShapeDtypeStruct((share_rows, width), f32),
            jax.ShapeDtypeStruct((high_count, BIN_LOW), f32),
        ),
        in_specs=[vmem, vmem],
        out_specs=(vmem, vmem),
        scratch_shapes=[
            pltpu.VMEM((freq_count, share_rows, cols), f32),
            pltpu.VMEM((3 * high_count, cells), bf16),
            pltpu.VMEM((BIN_LOW, cells), bf16),
            pltpu.VMEM((freq_count, 2, high_count, BIN_LOW), f32),
            pltpu.VMEM((base_count, 2, high_count, BIN_LOW), f32),
            pltpu.SemaphoreType.DMA((sems,)),
            pltpu.SemaphoreType.DMA((sems,)),
        ],
        compiler_params=pltpu.CompilerParams(
            collective_id=1, has_side_effects=True, vmem_limit_bytes=40 * 2**20
        ),
    )(power, bins)


def per_device(visibility, tile_of, u_within, v_cell, kernel_index, kernel, live_count, bin_map):
    base_count = lax.axis_size("base")
    freq_count = lax.axis_size("freq")
    grid = bin_map.shape[1]
    width = grid // base_count
    split = 2 if width % (2 * LANES) == 0 and freq_count % 2 == 0 else 1
    channels_here, slots = u_within.shape
    dh, dl = transform_tables(grid)
    scale = 1.0 / (channels_here * freq_count * slots * base_count)
    fields = gather_fields(
        split, base_count, grid // base_count, grid,
        visibility, tile_of[:, :, 0], u_within, v_cell, kernel_index, live_count,
    )
    power = image_power(
        fields, kernel.T, jnp.asarray(dh), jnp.asarray(dl), grid, width // split, split, slots, scale
    )
    share_rows = grid // freq_count
    bins = lax.dynamic_slice_in_dim(bin_map, lax.axis_index("freq") * share_rows, share_rows, 1)
    share, spectrum = exchange(power, bins, freq_count, base_count, split, width)
    return share, spectrum.reshape(NBINS)


def solution(mesh):
    in_specs = (
        P(None, "freq", "base"),
        P("freq", "base", None),
        P("freq", "base"),
        P("freq", "base"),
        P(None, "freq", "base"),
        P(),
        P("freq", "base"),
        P("base", None),
    )
    out_specs = (P("freq", "base"), P())
    return jax.shard_map(
        per_device, mesh=mesh, in_specs=in_specs, out_specs=out_specs, check_vma=False
    )
```

```python
import functools
import math

import jax
import jax.numpy as jnp
import numpy as np
from jax import lax
from jax.experimental import pallas as pl
from jax.experimental.pallas import tpu as pltpu
from jax.sharding import PartitionSpec as P

NBINS = 512
BIN_LOW = 32
KW = 8
FINE = 32
SPREAD = FINE + KW
RADIX = 4
GROUP = 16
FIELDS = 6
LANES = 128
MESH = pl.DeviceIdType.MESH


def halves_of(x):
    high = x.astype(jnp.bfloat16)
    low = (x - high.astype(jnp.float32)).astype(jnp.bfloat16)
    return high, low


@functools.lru_cache(None)
def transform_tables(grid):
    slab = grid // RADIX
    u = RADIX * np.arange(slab)[None, None, :] + np.arange(RADIX)[:, None, None]
    angle = ((np.arange(slab)[None, :, None] * u) % grid) * (2.0 * math.pi / grid)
    x = np.concatenate([np.cos(angle), np.sin(angle)], axis=1).astype(np.float32)
    high = x.astype(jnp.bfloat16)
    low = (x - high.astype(np.float32)).astype(jnp.bfloat16)
    return high, low


def dot(a, b):
    return jnp.dot(a, b, preferred_element_type=jnp.float32)


def dot_rows(a, b):
    return lax.dot_general(a, b, (((1,), (1,)), ((), ())), preferred_element_type=jnp.float32)


def greet(peers):
    barrier = pltpu.get_barrier_semaphore()
    for peer in peers:
        pl.semaphore_signal(barrier, inc=1, device_id=peer, device_id_type=MESH)
    return barrier


def gather_kernel(
    split, base_count, tile_rows, grid, vis_ref, tile_ref, within_ref, column_ref, index_ref, live_ref,
    out_ref, send_sems, recv_sems
):
    freq, base = lax.axis_index("freq"), lax.axis_index("base")
    part = lax.rem(freq, split)
    first = freq - part
    channels, slots = within_ref.shape
    lane = lax.broadcasted_iota(jnp.int32, (1, slots), 1)
    line = [{"freq": freq, "base": lax.rem(base + d, base_count)} for d in range(1, base_count)]
    mates = [{"freq": first + lax.rem(part + d, split), "base": base} for d in range(1, split)]
    barrier = greet(line + mates)
    for c in range(channels):
        is_live = lane < live_ref[0:1, c:c + 1]
        u = jnp.minimum(tile_ref[c] * tile_rows + within_ref[c:c + 1, :], grid - KW)
        fields = [
            jnp.where(is_live, vis_ref[0, c:c + 1, :], 0.0),
            jnp.where(is_live, vis_ref[1, c:c + 1, :], 0.0),
            u.astype(jnp.float32),
            column_ref[c:c + 1, :].astype(jnp.float32),
            jnp.where(is_live, index_ref[0, c:c + 1, :], -1).astype(jnp.float32),
            index_ref[1, c:c + 1, :].astype(jnp.float32),
        ]
        rows = [x[:, at:at + LANES] for x in fields for at in range(0, slots, LANES)]
        out_ref[part * channels + c, base] = jnp.concatenate(rows, axis=0)
    pl.semaphore_wait(barrier, len(line) + len(mates))

    def block_copy(owner, peer, k):
        block = out_ref.at[pl.ds(part * channels, channels), owner]
        return pltpu.make_async_remote_copy(
            src_ref=block, dst_ref=block, send_sem=send_sems.at[k], recv_sem=recv_sems.at[k],
            device_id=peer, device_id_type=MESH,
        )

    sent = [block_copy(base, peer, k) for k, peer in enumerate(line)]
    for copy in sent:
        copy.start()
    passed = []
    for d in range(base_count):
        if d:
            sent[d - 1].wait_recv()
        for k, mate in enumerate(mates):
            copy = block_copy(
                lax.rem(base + base_count - d, base_count), mate, len(line) + k * base_count + d
            )
            copy.start()
            passed.append(copy)
    for copy in passed:
        copy.wait()
    for copy in sent:
        copy.wait_send()


def gather_fields(split, base_count, tile_rows, grid, *arrays):
    channels, slots = arrays[2].shape
    sems = base_count - 1 + (split - 1) * base_count
    vmem = pl.BlockSpec(memory_space=pltpu.VMEM)
    return pl.pallas_call(
        functools.partial(gather_kernel, split, base_count, tile_rows, grid),
        out_shape=jax.ShapeDtypeStruct(
            (channels * split, base_count, FIELDS * (slots // LANES), LANES), jnp.float32
        ),
        in_specs=[vmem] * len(arrays),
        out_specs=vmem,
        scratch_shapes=[pltpu.SemaphoreType.DMA((sems,)), pltpu.SemaphoreType.DMA((sems,))],
        compiler_params=pltpu.CompilerParams(
            collective_id=0, has_side_effects=True, vmem_limit_bytes=4 * 2**20
        ),
        name="gather_fields",
    )(*arrays)


def phase(product, grid):
    half = grid // 2
    angle = ((product + half) & (grid - 1)) - half
    angle = angle.astype(jnp.float32) * (2.0 * math.pi / grid)
    return jnp.cos(angle), jnp.sin(angle)


def grid_kernel(
    grid, split, f_ref, kernel_ref, h_ref,
    fine_ref, coarse_ref, z_ref, live_ref, first_ref, second_ref, valid_ref, channel_ref
):
    channels, blocks, rows, _ = f_ref.shape
    subs = rows // FIELDS
    cols = h_ref.shape[3] // 2
    slab = grid // RADIX
    period = RADIX * GROUP
    coarse_count = grid // FINE
    piece = 2 * LANES

    left = (lax.axis_index("base") * split + lax.rem(lax.axis_index("freq"), split)) * cols
    l = left + lax.broadcasted_iota(jnp.int32, (cols, SPREAD), 0)
    c, s = phase(l * lax.broadcasted_iota(jnp.int32, (cols, SPREAD), 1), grid)
    fine = jnp.concatenate(
        [jnp.concatenate([c, s], axis=1), jnp.concatenate([-s, c], axis=1)], axis=0
    )
    fh, fl = halves_of(fine)
    fine_ref[...] = jnp.zeros_like(fine_ref)
    fine_ref[:, 0:2 * SPREAD] = fh
    fine_ref[:, 2 * SPREAD:4 * SPREAD] = fl
    fine_ref[:, 4 * SPREAD:6 * SPREAD] = fh
    l = left + lax.broadcasted_iota(jnp.int32, (cols, coarse_count), 0)
    c, s = phase(l * lax.broadcasted_iota(jnp.int32, (cols, coarse_count), 1) * FINE, grid)
    ch, cl = halves_of(jnp.concatenate([c, -s], axis=0))
    coarse_ref[:, 0:coarse_count] = ch
    coarse_ref[:, coarse_count:] = cl
    h_ref[...] = jnp.zeros_like(h_ref)
    taps_table = kernel_ref[...]

    counts = []
    for c in range(channels):
        for b in range(blocks):
            used = f_ref[c, b, 4 * subs:5 * subs, :] >= 0.0
            counts.append(jnp.sum(jnp.where(used, 1.0, 0.0)))
    for n, count in enumerate(counts):
        live_ref[n] = count.astype(jnp.int32)

    def list_block(n, carry):
        steps, open_slot, last_channel = carry
        c, b = n // blocks, n % blocks
        new_channel = c != last_channel
        steps = jnp.where(new_channel & (open_slot == 1), steps + 1, steps)
        open_slot = jnp.where(new_channel, 0, open_slot)
        count = live_ref[n]
        for sub in range(subs):
            live = count > sub * LANES
            spot = b * subs + sub

            @pl.when(live & (open_slot == 0))
            def _():
                first_ref[steps] = spot
                second_ref[steps] = spot
                valid_ref[steps] = 0
                channel_ref[steps] = c

            @pl.when(live & (open_slot == 1))
            def _():
                second_ref[steps] = spot
                valid_ref[steps] = 1

            steps = jnp.where(live & (open_slot == 1), steps + 1, steps)
            open_slot = jnp.where(live, 1 - open_slot, open_slot)
        return steps, open_slot, c

    steps, open_slot, _ = lax.fori_loop(0, channels * blocks, list_block, (0, 0, 0))
    steps = steps + open_slot

    for extra in range(2):
        first_ref[steps + extra] = 0
        second_ref[steps + extra] = 0
        valid_ref[steps + extra] = -1
        channel_ref[steps + extra] = 0

    def field(step, number):
        c = channel_ref[step]
        one, two = first_ref[step], second_ref[step]
        return jnp.concatenate(
            [
                f_ref[c, one // subs, pl.ds(number * subs + one % subs, 1), :],
                f_ref[c, two // subs, pl.ds(number * subs + two % subs, 1), :],
            ],
            axis=1,
        )

    def look_up(row):
        row = jnp.maximum(row.astype(jnp.int32), 0)
        pieces = []
        for at in range(0, piece, LANES):
            index = jnp.broadcast_to(row[:, at:at + LANES], (KW, LANES))
            pieces.append(jnp.take_along_axis(taps_table, index, axis=1))
        return jnp.concatenate(pieces, axis=1)

    lane = lax.broadcasted_iota(jnp.int32, (1, piece), 1)

    def make_z(step, slot):
        keep = lane < jnp.where(valid_ref[step] == 1, piece, jnp.where(valid_ref[step] == 0, LANES, 0))
        re = jnp.where(keep, field(step, 0), 0.0)
        im = jnp.where(keep, field(step, 1), 0.0)
        v = field(step, 3).astype(jnp.int32)
        taps_v = look_up(field(step, 5))
        offset = lax.broadcasted_iota(jnp.int32, (SPREAD, piece), 0) - (v & (FINE - 1))
        spread = jnp.zeros((SPREAD, piece), jnp.float32)
        for t in range(KW):
            spread = jnp.where(offset == t, taps_v[t:t + 1, :], spread)
        both = jnp.concatenate([spread * re, spread * im], axis=0)
        bh, bl = halves_of(both)
        pad = jnp.zeros((256 - 6 * SPREAD, piece), jnp.bfloat16)
        zb = dot(fine_ref[...], jnp.concatenate([bh, bh, bl, pad], axis=0))
        pick = lax.broadcasted_iota(jnp.int32, (2 * coarse_count, piece), 0) & (coarse_count - 1)
        onehot = jnp.where(pick == v // FINE, 1.0, 0.0).astype(jnp.bfloat16)
        e = dot(coarse_ref[...], onehot)
        zr, zi = zb[:cols], zb[cols:]
        er, ei = e[:cols], e[cols:]
        zh, zl = halves_of(zr * er - zi * ei)
        z_ref[slot, 0, 0:cols, :] = zh
        z_ref[slot, 1, 0:cols, :] = zl
        zh, zl = halves_of(zr * ei + zi * er)
        z_ref[slot, 0, cols:, :] = zh
        z_ref[slot, 1, cols:, :] = zl

    def add_rows(step, slot, firsts):
        u = field(step, 2).astype(jnp.int32)
        taps_u = look_up(field(step, 4))
        c = channel_ref[step]
        zh, zl = z_ref[slot, 0], z_ref[slot, 1]
        for first in firsts:
            residue = RADIX * lax.broadcasted_iota(jnp.int32, (GROUP, piece), 0) + first
            tap = (residue - u) & (period - 1)
            group = (u + tap - residue) // period
            r = jnp.zeros((GROUP, piece), jnp.float32)
            for t in range(KW):
                r = jnp.where(tap == t, taps_u[t:t + 1, :], r)
            rh, rl = halves_of(r)
            q = group.astype(jnp.float32).astype(jnp.bfloat16)
            zero = jnp.zeros_like(rh)
            hits = [q == jnp.bfloat16(g) for g in range(slab // GROUP)]
            wh = jnp.concatenate([jnp.where(hit, rh, zero) for hit in hits], axis=0)
            wl = jnp.concatenate([jnp.where(hit, rl, zero) for hit in hits], axis=0)
            h_ref[c, first] += dot_rows(wh, zh) + dot_rows(wh, zl) + dot_rows(wl, zh)

    make_z(0, 0)

    def two_steps(n, carry):
        step = 2 * n
        for slot in range(2):
            add_rows(step + slot, slot, (0, 1))
            make_z(step + slot + 1, 1 - slot)
            add_rows(step + slot, slot, (2, 3))
        return carry

    lax.fori_loop(0, (steps + 1) // 2, two_steps, 0)


def grid_visibilities(fields, taps_table, grid, cols, split):
    channels, blocks, rows, _ = fields.shape
    slab = grid // RADIX
    most = channels * blocks * (rows // FIELDS) + 8
    smem = lambda n: pltpu.SMEM((n,), jnp.int32)
    vmem = pl.BlockSpec(memory_space=pltpu.VMEM)
    return pl.pallas_call(
        functools.partial(grid_kernel, grid, split),
        out_shape=jax.ShapeDtypeStruct((channels, RADIX, slab, 2 * cols), jnp.float32),
        in_specs=[vmem, vmem],
        out_specs=vmem,
        scratch_shapes=[
            pltpu.VMEM((2 * cols, 256), jnp.bfloat16),
            pltpu.VMEM((2 * cols, 2 * (grid // FINE)), jnp.bfloat16),
            pltpu.VMEM((2, 2, 2 * cols, 2 * LANES), jnp.bfloat16),
            smem(channels * blocks), smem(most), smem(most), smem(most), smem(most),
        ],
        compiler_params=pltpu.CompilerParams(vmem_limit_bytes=16 * 2**20),
        name="grid_visibilities",
    )(fields, taps_table)


def power_kernel(
    grid, freq_count, base_count, split, scale, h_ref, dh_ref, dl_ref, bins_ref, share_ref, spectrum_ref,
    hh_ref, hl_ref, y_ref, power_ref, recv_ref, mask_ref, value_ref, low_ref, stage_ref, stage2_ref,
    send_sems, recv_sems, sum_send_sems, sum_recv_sems
):
    freq, base = lax.axis_index("freq"), lax.axis_index("base")
    ring = [{"freq": lax.rem(freq + d, freq_count), "base": base} for d in range(1, freq_count)]
    line = [{"freq": freq, "base": lax.rem(base + d, base_count)} for d in range(1, base_count)]
    barrier = greet(ring + line)

    channels = h_ref.shape[0]
    slab = grid // RADIX
    share_rows, width = share_ref.shape
    cols = width // split
    chunk = min(64, share_rows)
    parts = share_rows // chunk
    shares = slab // share_rows

    def split_rows(n, carry):
        high, low = halves_of(h_ref[n // RADIX, n % RADIX])
        hh_ref[n // RADIX, n % RADIX] = high
        hl_ref[n // RADIX, n % RADIX] = low
        return carry

    lax.fori_loop(0, channels * RADIX, split_rows, 0)

    def transform(n):
        top = pl.multiple_of((lax.rem(n, shares) * parts + n // shares) * chunk, chunk)
        for c in range(channels):
            for first in range(RADIX):
                dh = jnp.concatenate(
                    [dh_ref[first, pl.ds(top, chunk), :], dh_ref[first, pl.ds(slab + top, chunk), :]], axis=0
                )
                dl = jnp.concatenate(
                    [dl_ref[first, pl.ds(top, chunk), :], dl_ref[first, pl.ds(slab + top, chunk), :]], axis=0
                )
                hh, hl = hh_ref[c, first], hl_ref[c, first]
                y_ref[c % 2, first] = dot(dh, hh) + dot(dl, hh) + dot(dh, hl)
            step = min(16, chunk)
            for row in range(0, chunk, step):
                yr, yi = [], []
                for first in range(RADIX):
                    cy = y_ref[c % 2, first, row:row + step, :]
                    sy = y_ref[c % 2, first, chunk + row:chunk + row + step, :]
                    yr.append(cy[:, :cols] + sy[:, cols:])
                    yi.append(cy[:, cols:] - sy[:, :cols])
                ar, ai = yr[0] + yr[2], yi[0] + yi[2]
                br, bi = yr[0] - yr[2], yi[0] - yi[2]
                cr, ci = yr[1] + yr[3], yi[1] + yi[3]
                dr, di = yr[1] - yr[3], yi[1] - yi[3]
                outs = [
                    (ar + cr, ai + ci), (br + di, bi - dr), (ar - cr, ai - ci), (br - di, bi + dr)
                ]
                for k, (xr, xi) in enumerate(outs):
                    at = pl.ds(pl.multiple_of(k * slab + top + row, step), step)
                    value = (xr * xr + xi * xi) * scale
                    power_ref[at, :] = value if c == 0 else power_ref[at, :] + value

    def piece(n, k):
        share, part = lax.rem(n, shares), n // shares
        target = k * shares + share
        top = pl.multiple_of(target * share_rows + part * chunk, chunk)
        rows = pl.ds(pl.multiple_of(part * chunk, chunk), chunk)
        copy = pltpu.make_async_remote_copy(
            src_ref=power_ref.at[pl.ds(top, chunk), :],
            dst_ref=recv_ref.at[freq, rows, :],
            send_sem=send_sems.at[n, k], recv_sem=recv_sems.at[freq, part],
            device_id={"freq": target, "base": base}, device_id_type=MESH,
        )
        return target, top, rows, copy

    def send(n):
        for k in range(RADIX):
            target, top, rows, copy = piece(n, k)

            @pl.when(target == freq)
            def _():
                recv_ref[freq, rows, :] = power_ref[pl.ds(top, chunk), :]

            @pl.when(target != freq)
            def _():
                copy.start()

    transform(0)
    pl.semaphore_wait(barrier, len(ring) + len(line))
    send(0)

    def later(n, carry):
        transform(n)
        send(n)
        return carry

    lax.fori_loop(1, shares * parts, later, 0)

    high_count = NBINS // BIN_LOW
    lead = high_count // 4
    bins = bins_ref[...].T
    order = lax.broadcasted_iota(jnp.int32, (high_count, width), 0)
    order = lead * (order % lead) + order // lead if lead == 4 else order
    low_order = lax.broadcasted_iota(jnp.int32, (BIN_LOW, width), 0)
    for row in range(share_rows):
        at = slice(row * width, (row + 1) * width)
        bin_id = bins[row:row + 1, :]
        mask_ref[:, at] = jnp.where(order == bin_id // BIN_LOW, 1.0, 0.0).astype(jnp.bfloat16)
        low_ref[:, at] = jnp.where(low_order == bin_id % BIN_LOW, 1.0, 0.0).astype(jnp.bfloat16)
    counts = dot_rows(mask_ref[...], low_ref[...])

    totals = jnp.zeros((high_count, BIN_LOW), jnp.float32)
    for part in range(parts):
        rows = slice(part * chunk, (part + 1) * chunk)
        for d in range(1, freq_count):
            source = lax.rem(freq + d, freq_count)
            pltpu.make_async_remote_copy(
                src_ref=power_ref.at[0:chunk, :], dst_ref=recv_ref.at[source, rows, :],
                send_sem=send_sems.at[0, 0], recv_sem=recv_sems.at[source, part],
                device_id={"freq": source, "base": base}, device_id_type=MESH,
            ).wait_recv()
        for half in range(split):
            total = recv_ref[half, rows, :]
            for group in range(1, freq_count // split):
                total = total + recv_ref[group * split + half, rows, :]
            share_ref[rows, half * cols:(half + 1) * cols] = total
        for row in range(part * chunk, (part + 1) * chunk):
            at = slice(row * width, (row + 1) * width)
            out = slice((row - part * chunk) * width, (row - part * chunk + 1) * width)
            value = jnp.broadcast_to(share_ref[row:row + 1, :], (high_count, width))
            high, low = halves_of(value)
            mask = mask_ref[:, at]
            value_ref[0:high_count, out] = mask * high
            value_ref[high_count:, out] = mask * low
        span = slice(part * chunk * width, (part + 1) * chunk * width)
        sums = dot_rows(value_ref[...], low_ref[:, span])
        totals = totals + sums[:high_count] + sums[high_count:]

    def pack(x):
        return jnp.concatenate([x[lead * k:lead * (k + 1)] for k in range(4)], axis=1)

    stage_ref[freq] = jnp.concatenate([pack(totals), pack(counts)], axis=0)

    def share_out(ref, me, peers, offset):
        copies = []
        for k, peer in enumerate(peers):
            copy = pltpu.make_async_remote_copy(
                src_ref=ref.at[me], dst_ref=ref.at[me],
                send_sem=sum_send_sems.at[offset + k], recv_sem=sum_recv_sems.at[offset + k],
                device_id=peer, device_id_type=MESH,
            )
            copy.start()
            copies.append(copy)
        for copy in copies:
            copy.wait()
        total = ref[0]
        for other in range(1, ref.shape[0]):
            total = total + ref[other]
        return total

    stage2_ref[base] = share_out(stage_ref, freq, ring, 0)
    total = share_out(stage2_ref, base, line, len(ring))
    spectrum_ref[...] = total[:lead] / total[lead:]

    def finish(n, carry):
        for k in range(RADIX):
            target, _, _, copy = piece(n, k)

            @pl.when(target != freq)
            def _():
                copy.wait_send()
        return carry

    lax.fori_loop(0, shares * parts, finish, 0)


def power_and_spectrum(h, dh, dl, bins, grid, freq_count, base_count, split, width, scale):
    channels, _, slab, both = h.shape
    cols = both // 2
    share_rows = grid // freq_count
    chunk = min(64, share_rows)
    parts, shares = share_rows // chunk, slab // share_rows
    high_count = NBINS // BIN_LOW
    cells = share_rows * width
    sems = freq_count + base_count - 2
    f32, bf16 = jnp.float32, jnp.bfloat16
    vmem = pl.BlockSpec(memory_space=pltpu.VMEM)
    return pl.pallas_call(
        functools.partial(power_kernel, grid, freq_count, base_count, split, scale),
        out_shape=(
            jax.ShapeDtypeStruct((share_rows, width), f32),
            jax.ShapeDtypeStruct((4, 4 * BIN_LOW), f32),
        ),
        in_specs=[vmem] * 4,
        out_specs=(vmem, vmem),
        scratch_shapes=[
            pltpu.VMEM(h.shape, bf16),
            pltpu.VMEM(h.shape, bf16),
            pltpu.VMEM((2, RADIX, 2 * chunk, both), f32),
            pltpu.VMEM((grid, cols), f32),
            pltpu.VMEM((freq_count, share_rows, cols), f32),
            pltpu.VMEM((high_count, cells), bf16),
            pltpu.VMEM((2 * high_count, chunk * width), bf16),
            pltpu.VMEM((BIN_LOW, cells), bf16),
            pltpu.VMEM((freq_count, 8, 4 * BIN_LOW), f32),
            pltpu.VMEM((base_count, 8, 4 * BIN_LOW), f32),
            pltpu.SemaphoreType.DMA((shares * parts, RADIX)),
            pltpu.SemaphoreType.DMA((freq_count, parts)),
            pltpu.SemaphoreType.DMA((sems,)),
            pltpu.SemaphoreType.DMA((sems,)),
        ],
        compiler_params=pltpu.CompilerParams(
            collective_id=1, has_side_effects=True, vmem_limit_bytes=24 * 2**20
        ),
        name="power_and_spectrum",
    )(h, dh, dl, bins)


def per_device(visibility, tile_of, u_within, v_cell, kernel_index, kernel, live_count, bin_map):
    base_count = lax.axis_size("base")
    freq_count = lax.axis_size("freq")
    grid = bin_map.shape[1]
    width = grid // base_count
    split = 2 if width % (2 * LANES) == 0 and freq_count % 2 == 0 else 1
    channels_here, slots = u_within.shape
    dh, dl = transform_tables(grid)
    scale = 1.0 / (channels_here * freq_count * slots * base_count)
    fields = gather_fields(
        split, base_count, grid // base_count, grid,
        visibility, tile_of.transpose(0, 2, 1), u_within, v_cell, kernel_index, live_count.T,
    )
    h = grid_visibilities(fields, kernel.T, grid, width // split, split)
    share_rows = grid // freq_count
    bins = lax.dynamic_slice_in_dim(bin_map, lax.axis_index("freq") * share_rows, share_rows, 1)
    share, spectrum = power_and_spectrum(
        h, jnp.asarray(dh), jnp.asarray(dl), bins, grid, freq_count, base_count, split, width, scale
    )
    return share, spectrum.reshape(NBINS)


def solution(mesh):
    in_specs = (
        P(None, "freq", "base"),
        P("freq", "base", None),
        P("freq", "base"),
        P("freq", "base"),
        P(None, "freq", "base"),
        P(),
        P("freq", "base"),
        P("base", None),
    )
    out_specs = (P("freq", "base"), P())
    return jax.shard_map(
        per_device, mesh=mesh, in_specs=in_specs, out_specs=out_specs, check_vma=False
    )
```

```python
import functools
import math

import jax
import jax.numpy as jnp
import numpy as np
from jax import lax
from jax.experimental import pallas as pl
from jax.experimental.pallas import tpu as pltpu
from jax.sharding import PartitionSpec as P

NBINS = 512
BIN_LOW = 32
KW = 8
FINE = 32
SPREAD = FINE + KW
RADIX = 4
GROUP = 16
FIELDS = 6
LANES = 128
MESH = pl.DeviceIdType.MESH


def halves_of(x):
    high = x.astype(jnp.bfloat16)
    low = (x - high.astype(jnp.float32)).astype(jnp.bfloat16)
    return high, low


@functools.lru_cache(None)
def transform_tables(grid):
    slab = grid // RADIX
    u = RADIX * np.arange(slab)[None, None, :] + np.arange(RADIX)[:, None, None]
    angle = ((np.arange(slab)[None, :, None] * u) % grid) * (2.0 * math.pi / grid)
    x = np.concatenate([np.cos(angle), np.sin(angle)], axis=1).astype(np.float32)
    high = x.astype(jnp.bfloat16)
    low = (x - high.astype(np.float32)).astype(jnp.bfloat16)
    return high, low


def dot(a, b):
    return jnp.dot(a, b, preferred_element_type=jnp.float32)


def dot_rows(a, b):
    return lax.dot_general(a, b, (((1,), (1,)), ((), ())), preferred_element_type=jnp.float32)


def in_hbm(x):
    return pltpu.with_memory_space_constraint(x, pltpu.HBM)


def greet(peers):
    barrier = pltpu.get_barrier_semaphore()
    for peer in peers:
        pl.semaphore_signal(barrier, inc=1, device_id=peer, device_id_type=MESH)
    return barrier


def phase(product, grid):
    half = grid // 2
    angle = ((product + half) & (grid - 1)) - half
    angle = angle.astype(jnp.float32) * (2.0 * math.pi / grid)
    return jnp.cos(angle), jnp.sin(angle)


def column_tables(grid, split, fine_ref, coarse_ref):
    cols = fine_ref.shape[0] // 2
    coarse_count = grid // FINE
    left = (lax.axis_index("base") * split + lax.rem(lax.axis_index("freq"), split)) * cols
    l = left + lax.broadcasted_iota(jnp.int32, (cols, SPREAD), 0)
    c, s = phase(l * lax.broadcasted_iota(jnp.int32, (cols, SPREAD), 1), grid)
    fine = jnp.concatenate(
        [jnp.concatenate([c, s], axis=1), jnp.concatenate([-s, c], axis=1)], axis=0
    )
    fh, fl = halves_of(fine)
    fine_ref[...] = jnp.zeros_like(fine_ref)
    fine_ref[:, 0:2 * SPREAD] = fh
    fine_ref[:, 2 * SPREAD:4 * SPREAD] = fl
    fine_ref[:, 4 * SPREAD:6 * SPREAD] = fh
    l = left + lax.broadcasted_iota(jnp.int32, (cols, coarse_count), 0)
    c, s = phase(l * lax.broadcasted_iota(jnp.int32, (cols, coarse_count), 1) * FINE, grid)
    ch, cl = halves_of(jnp.concatenate([c, -s], axis=0))
    coarse_ref[:, 0:coarse_count] = ch
    coarse_ref[:, coarse_count:] = cl


def gather_kernel(
    split, base_count, tile_rows, grid, vis_hbm, tile_hbm, within_hbm, column_hbm, index_hbm, live_hbm,
    taps_hbm, out_ref, fine_ref, coarse_ref, taps_ref,
    vis_ref, tile_ref, within_ref, column_ref, index_ref, live_ref, load_sems, send_sems, recv_sems
):
    freq, base = lax.axis_index("freq"), lax.axis_index("base")
    part = lax.rem(freq, split)
    first = freq - part
    line = [{"freq": freq, "base": lax.rem(base + d, base_count)} for d in range(1, base_count)]
    mates = [{"freq": first + lax.rem(part + d, split), "base": base} for d in range(1, split)]
    barrier = greet(line + mates)
    loads = [
        pltpu.make_async_copy(a, b, load_sems.at[n])
        for n, (a, b) in enumerate([
            (vis_hbm, vis_ref), (tile_hbm, tile_ref), (within_hbm, within_ref), (column_hbm, column_ref),
            (index_hbm, index_ref), (live_hbm, live_ref), (taps_hbm, taps_ref),
        ])
    ]
    for load in loads:
        load.start()
    for load in loads:
        load.wait()
    channels, slots = within_ref.shape
    lane = lax.broadcasted_iota(jnp.int32, (1, slots), 1)
    for c in range(channels):
        is_live = lane < live_ref[0:1, c:c + 1]
        u = jnp.minimum(tile_ref[c] * tile_rows + within_ref[c:c + 1, :], grid - KW)
        fields = [
            jnp.where(is_live, vis_ref[0, c:c + 1, :], 0.0),
            jnp.where(is_live, vis_ref[1, c:c + 1, :], 0.0),
            u.astype(jnp.float32),
            column_ref[c:c + 1, :].astype(jnp.float32),
            jnp.where(is_live, index_ref[0, c:c + 1, :], -1).astype(jnp.float32),
            index_ref[1, c:c + 1, :].astype(jnp.float32),
        ]
        rows = [x[:, at:at + LANES] for x in fields for at in range(0, slots, LANES)]
        out_ref[part * channels + c, base] = jnp.concatenate(rows, axis=0)
    pl.semaphore_wait(barrier, len(line) + len(mates))

    def block_copy(owner, peer, k):
        block = out_ref.at[pl.ds(part * channels, channels), owner]
        return pltpu.make_async_remote_copy(
            src_ref=block, dst_ref=block, send_sem=send_sems.at[k], recv_sem=recv_sems.at[k],
            device_id=peer, device_id_type=MESH,
        )

    sent = [block_copy(base, peer, k) for k, peer in enumerate(line)]
    for copy in sent:
        copy.start()
    passed = []
    for d in range(base_count):
        if d:
            sent[d - 1].wait_recv()
        for k, mate in enumerate(mates):
            copy = block_copy(
                lax.rem(base + base_count - d, base_count), mate, len(line) + k * base_count + d
            )
            copy.start()
            passed.append(copy)
        if d == 0:
            column_tables(grid, split, fine_ref, coarse_ref)
    for copy in passed:
        copy.wait()
    for copy in sent:
        copy.wait_send()


def gather_fields(split, base_count, tile_rows, grid, cols, *arrays):
    channels, slots = arrays[2].shape
    sems = base_count - 1 + (split - 1) * base_count
    total = channels * split
    f32, bf16 = jnp.float32, jnp.bfloat16
    vmem = pl.BlockSpec(memory_space=pltpu.VMEM)
    hbm = pl.BlockSpec(memory_space=pltpu.HBM)
    return pl.pallas_call(
        functools.partial(gather_kernel, split, base_count, tile_rows, grid),
        out_shape=(
            jax.ShapeDtypeStruct((total, base_count, FIELDS * (slots // LANES), LANES), f32),
            jax.ShapeDtypeStruct((2 * cols, 256), bf16),
            jax.ShapeDtypeStruct((2 * cols, 2 * (grid // FINE)), bf16),
            jax.ShapeDtypeStruct(arrays[-1].shape, f32),
        ),
        in_specs=[hbm] * len(arrays),
        out_specs=(vmem,) * 4,
        scratch_shapes=[pltpu.VMEM(x.shape, x.dtype) for x in arrays[:-1]] + [
            pltpu.SemaphoreType.DMA((len(arrays),)),
            pltpu.SemaphoreType.DMA((sems,)), pltpu.SemaphoreType.DMA((sems,)),
        ],
        compiler_params=pltpu.CompilerParams(
            collective_id=0, has_side_effects=True, vmem_limit_bytes=12 * 2**20
        ),
        name="gather_fields",
    )(*[in_hbm(x) for x in arrays])


def grid_kernel(
    grid, f_ref, fine_ref, coarse_ref, kernel_ref, h_ref,
    z_ref, live_ref, first_ref, second_ref, valid_ref, channel_ref
):
    channels, blocks, rows, _ = f_ref.shape
    subs = rows // FIELDS
    cols = h_ref.shape[3] // 2
    slab = grid // RADIX
    period = RADIX * GROUP
    coarse_count = grid // FINE
    piece = 2 * LANES

    taps_table = kernel_ref[...]
    h_ref[...] = jnp.zeros_like(h_ref)

    counts = []
    for c in range(channels):
        for b in range(blocks):
            used = f_ref[c, b, 4 * subs:5 * subs, :] >= 0.0
            counts.append(jnp.sum(jnp.where(used, 1.0, 0.0)))
    for n, count in enumerate(counts):
        live_ref[n] = count.astype(jnp.int32)

    def list_block(n, carry):
        steps, open_slot, last_channel = carry
        c = lax.shift_right_logical(n, jnp.int32(blocks.bit_length() - 1))
        b = n & (blocks - 1)
        new_channel = c != last_channel
        steps = jnp.where(new_channel & (open_slot == 1), steps + 1, steps)
        open_slot = jnp.where(new_channel, 0, open_slot)
        count = live_ref[n]
        for sub in range(subs):
            live = count > sub * LANES
            spot = b * subs + sub

            @pl.when(live & (open_slot == 0))
            def _():
                first_ref[steps] = spot
                second_ref[steps] = spot
                valid_ref[steps] = 0
                channel_ref[steps] = c

            @pl.when(live & (open_slot == 1))
            def _():
                second_ref[steps] = spot
                valid_ref[steps] = 1

            steps = jnp.where(live & (open_slot == 1), steps + 1, steps)
            open_slot = jnp.where(live, 1 - open_slot, open_slot)
        return steps, open_slot, c

    steps, open_slot, _ = lax.fori_loop(0, channels * blocks, list_block, (0, 0, 0))
    steps = steps + open_slot

    for extra in range(2):
        first_ref[steps + extra] = 0
        second_ref[steps + extra] = 0
        valid_ref[steps + extra] = -1
        channel_ref[steps + extra] = 0

    def field(step, number):
        c = channel_ref[step]
        one, two = first_ref[step], second_ref[step]
        by = jnp.int32(subs.bit_length() - 1)
        return jnp.concatenate(
            [
                f_ref[c, lax.shift_right_logical(one, by), pl.ds(number * subs + (one & (subs - 1)), 1), :],
                f_ref[c, lax.shift_right_logical(two, by), pl.ds(number * subs + (two & (subs - 1)), 1), :],
            ],
            axis=1,
        )

    def look_up(row):
        row = jnp.maximum(row.astype(jnp.int32), 0)
        pieces = []
        for at in range(0, piece, LANES):
            index = jnp.broadcast_to(row[:, at:at + LANES], (KW, LANES))
            pieces.append(jnp.take_along_axis(taps_table, index, axis=1))
        return jnp.concatenate(pieces, axis=1)

    lane = lax.broadcasted_iota(jnp.int32, (1, piece), 1)

    def make_z(step, slot):
        keep = lane < jnp.where(valid_ref[step] == 1, piece, jnp.where(valid_ref[step] == 0, LANES, 0))
        re = jnp.where(keep, field(step, 0), 0.0)
        im = jnp.where(keep, field(step, 1), 0.0)
        v = field(step, 3).astype(jnp.int32)
        taps_v = look_up(field(step, 5))
        offset = lax.broadcasted_iota(jnp.int32, (SPREAD, piece), 0) - (v & (FINE - 1))
        spread = jnp.zeros((SPREAD, piece), jnp.float32)
        for t in range(KW):
            spread = jnp.where(offset == t, taps_v[t:t + 1, :], spread)
        both = jnp.concatenate([spread * re, spread * im], axis=0)
        bh, bl = halves_of(both)
        pad = jnp.zeros((256 - 6 * SPREAD, piece), jnp.bfloat16)
        zb = dot(fine_ref[...], jnp.concatenate([bh, bh, bl, pad], axis=0))
        pick = lax.broadcasted_iota(jnp.int32, (2 * coarse_count, piece), 0) & (coarse_count - 1)
        onehot = jnp.where(pick == v // FINE, 1.0, 0.0).astype(jnp.bfloat16)
        e = dot(coarse_ref[...], onehot)
        zr, zi = zb[:cols], zb[cols:]
        er, ei = e[:cols], e[cols:]
        zh, zl = halves_of(zr * er - zi * ei)
        z_ref[slot, 0, 0:cols, :] = zh
        z_ref[slot, 1, 0:cols, :] = zl
        zh, zl = halves_of(zr * ei + zi * er)
        z_ref[slot, 0, cols:, :] = zh
        z_ref[slot, 1, cols:, :] = zl

    def add_rows(step, slot, firsts):
        u = field(step, 2).astype(jnp.int32)
        taps_u = look_up(field(step, 4))
        c = channel_ref[step]
        zh, zl = z_ref[slot, 0], z_ref[slot, 1]
        for first in firsts:
            residue = RADIX * lax.broadcasted_iota(jnp.int32, (GROUP, piece), 0) + first
            tap = (residue - u) & (period - 1)
            group = (u + tap - residue) // period
            r = jnp.zeros((GROUP, piece), jnp.float32)
            for t in range(KW):
                r = jnp.where(tap == t, taps_u[t:t + 1, :], r)
            rh, rl = halves_of(r)
            q = group.astype(jnp.float32).astype(jnp.bfloat16)
            zero = jnp.zeros_like(rh)
            hits = [q == jnp.bfloat16(g) for g in range(slab // GROUP)]
            wh = jnp.concatenate([jnp.where(hit, rh, zero) for hit in hits], axis=0)
            wl = jnp.concatenate([jnp.where(hit, rl, zero) for hit in hits], axis=0)
            h_ref[c, first] += dot_rows(wh, zh) + dot_rows(wh, zl) + dot_rows(wl, zh)

    make_z(0, 0)

    def two_steps(n, carry):
        step = 2 * n
        for slot in range(2):
            add_rows(step + slot, slot, (0, 1))
            make_z(step + slot + 1, 1 - slot)
            add_rows(step + slot, slot, (2, 3))
        return carry

    lax.fori_loop(0, (steps + 1) // 2, two_steps, 0)


def grid_visibilities(fields, fine, coarse, taps_table, grid):
    both = fine.shape[0]
    channels, blocks, rows, _ = fields.shape
    most = channels * blocks * (rows // FIELDS) + 8
    smem = lambda n: pltpu.SMEM((n,), jnp.int32)
    vmem = pl.BlockSpec(memory_space=pltpu.VMEM)
    return pl.pallas_call(
        functools.partial(grid_kernel, grid),
        out_shape=jax.ShapeDtypeStruct((channels, RADIX, grid // RADIX, both), jnp.float32),
        in_specs=[vmem] * 4,
        out_specs=vmem,
        scratch_shapes=[
            pltpu.VMEM((2, 2, both, 2 * LANES), jnp.bfloat16),
            smem(channels * blocks), smem(most), smem(most), smem(most), smem(most),
        ],
        compiler_params=pltpu.CompilerParams(vmem_limit_bytes=16 * 2**20),
        name="grid_visibilities",
    )(fields, fine, coarse, taps_table)


def power_kernel(
    grid, freq_count, base_count, split, scale, h_ref, dh_hbm, dl_hbm, bins_hbm, share_ref, spectrum_ref,
    dh_ref, dl_ref, bins_ref, load_sems, bins_sem, hh_ref, hl_ref, y_ref, power_ref, recv_ref, mask_ref, value_ref, low_ref, stage_ref, stage2_ref,
    send_sems, recv_sems, sum_send_sems, sum_recv_sems
):
    freq, base = lax.axis_index("freq"), lax.axis_index("base")
    ring = [{"freq": lax.rem(freq + d, freq_count), "base": base} for d in range(1, freq_count)]
    line = [{"freq": freq, "base": lax.rem(base + d, base_count)} for d in range(1, base_count)]
    barrier = greet(ring + line)
    loads = []
    for n in range(RADIX):
        loads.append(pltpu.make_async_copy(dh_hbm.at[n], dh_ref.at[n], load_sems.at[0, n]))
        loads.append(pltpu.make_async_copy(dl_hbm.at[n], dl_ref.at[n], load_sems.at[1, n]))
    for load in loads:
        load.start()
    rows_here = bins_ref.shape[1]
    if bins_hbm.shape[1] != rows_here:
        here = pl.ds(pl.multiple_of(freq * rows_here, rows_here), rows_here)
        load_bins = pltpu.make_async_copy(bins_hbm.at[:, here], bins_ref, bins_sem)
    else:
        load_bins = pltpu.make_async_copy(bins_hbm, bins_ref, bins_sem)
    load_bins.start()

    channels = h_ref.shape[0]
    slab = grid // RADIX
    share_rows, width = share_ref.shape
    cols = width // split
    chunk = min(64, share_rows)
    parts = share_rows // chunk
    shares = slab // share_rows

    def split_rows(n, carry):
        high, low = halves_of(h_ref[n // RADIX, n % RADIX])
        hh_ref[n // RADIX, n % RADIX] = high
        hl_ref[n // RADIX, n % RADIX] = low
        return carry

    lax.fori_loop(0, channels * RADIX, split_rows, 0)
    for load in loads:
        load.wait()

    def transform(n):
        top = pl.multiple_of((lax.rem(n, shares) * parts + n // shares) * chunk, chunk)
        for c in range(channels):
            for first in range(RADIX):
                dh = jnp.concatenate(
                    [dh_ref[first, pl.ds(top, chunk), :], dh_ref[first, pl.ds(slab + top, chunk), :]], axis=0
                )
                dl = jnp.concatenate(
                    [dl_ref[first, pl.ds(top, chunk), :], dl_ref[first, pl.ds(slab + top, chunk), :]], axis=0
                )
                hh, hl = hh_ref[c, first], hl_ref[c, first]
                y_ref[c % 2, first] = dot(dh, hh) + dot(dl, hh) + dot(dh, hl)
            step = min(16, chunk)
            for row in range(0, chunk, step):
                yr, yi = [], []
                for first in range(RADIX):
                    cy = y_ref[c % 2, first, row:row + step, :]
                    sy = y_ref[c % 2, first, chunk + row:chunk + row + step, :]
                    yr.append(cy[:, :cols] + sy[:, cols:])
                    yi.append(cy[:, cols:] - sy[:, :cols])
                ar, ai = yr[0] + yr[2], yi[0] + yi[2]
                br, bi = yr[0] - yr[2], yi[0] - yi[2]
                cr, ci = yr[1] + yr[3], yi[1] + yi[3]
                dr, di = yr[1] - yr[3], yi[1] - yi[3]
                outs = [
                    (ar + cr, ai + ci), (br + di, bi - dr), (ar - cr, ai - ci), (br - di, bi + dr)
                ]
                for k, (xr, xi) in enumerate(outs):
                    at = pl.ds(pl.multiple_of(k * slab + top + row, step), step)
                    value = (xr * xr + xi * xi) * scale
                    power_ref[at, :] = value if c == 0 else power_ref[at, :] + value

    def piece(n, k):
        share, part = lax.rem(n, shares), n // shares
        target = k * shares + share
        top = pl.multiple_of(target * share_rows + part * chunk, chunk)
        rows = pl.ds(pl.multiple_of(part * chunk, chunk), chunk)
        copy = pltpu.make_async_remote_copy(
            src_ref=power_ref.at[pl.ds(top, chunk), :],
            dst_ref=recv_ref.at[freq, rows, :],
            send_sem=send_sems.at[n, k], recv_sem=recv_sems.at[freq, part],
            device_id={"freq": target, "base": base}, device_id_type=MESH,
        )
        return target, top, rows, copy

    def send(n):
        for k in range(RADIX):
            target, top, rows, copy = piece(n, k)

            @pl.when(target == freq)
            def _():
                recv_ref[freq, rows, :] = power_ref[pl.ds(top, chunk), :]

            @pl.when(target != freq)
            def _():
                copy.start()

    transform(0)
    pl.semaphore_wait(barrier, len(ring) + len(line))
    send(0)

    def later(n, carry):
        transform(n)
        send(n)
        return carry

    lax.fori_loop(1, shares * parts, later, 0)

    high_count = NBINS // BIN_LOW
    lead = high_count // 4
    load_bins.wait()
    bins = bins_ref[...].T
    order = lax.broadcasted_iota(jnp.int32, (high_count, width), 0)
    order = lead * (order % lead) + order // lead if lead == 4 else order
    low_order = lax.broadcasted_iota(jnp.int32, (BIN_LOW, width), 0)
    for row in range(share_rows):
        at = slice(row * width, (row + 1) * width)
        bin_id = bins[row:row + 1, :]
        mask_ref[:, at] = jnp.where(order == bin_id // BIN_LOW, 1.0, 0.0).astype(jnp.bfloat16)
        low_ref[:, at] = jnp.where(low_order == bin_id % BIN_LOW, 1.0, 0.0).astype(jnp.bfloat16)
    counts = dot_rows(mask_ref[...], low_ref[...])

    totals = jnp.zeros((high_count, BIN_LOW), jnp.float32)
    for part in range(parts):
        rows = slice(part * chunk, (part + 1) * chunk)
        for d in range(1, freq_count):
            source = lax.rem(freq + d, freq_count)
            pltpu.make_async_remote_copy(
                src_ref=power_ref.at[0:chunk, :], dst_ref=recv_ref.at[source, rows, :],
                send_sem=send_sems.at[0, 0], recv_sem=recv_sems.at[source, part],
                device_id={"freq": source, "base": base}, device_id_type=MESH,
            ).wait_recv()
        for half in range(split):
            total = recv_ref[half, rows, :]
            for group in range(1, freq_count // split):
                total = total + recv_ref[group * split + half, rows, :]
            share_ref[rows, half * cols:(half + 1) * cols] = total
        for row in range(part * chunk, (part + 1) * chunk):
            at = slice(row * width, (row + 1) * width)
            out = slice((row - part * chunk) * width, (row - part * chunk + 1) * width)
            value = jnp.broadcast_to(share_ref[row:row + 1, :], (high_count, width))
            high, low = halves_of(value)
            mask = mask_ref[:, at]
            value_ref[0:high_count, out] = mask * high
            value_ref[high_count:, out] = mask * low
        span = slice(part * chunk * width, (part + 1) * chunk * width)
        sums = dot_rows(value_ref[...], low_ref[:, span])
        totals = totals + sums[:high_count] + sums[high_count:]

    def pack(x):
        return jnp.concatenate([x[lead * k:lead * (k + 1)] for k in range(4)], axis=1)

    stage_ref[freq] = jnp.concatenate([pack(totals), pack(counts)], axis=0)

    def share_out(ref, me, peers, offset):
        copies = []
        for k, peer in enumerate(peers):
            copy = pltpu.make_async_remote_copy(
                src_ref=ref.at[me], dst_ref=ref.at[me],
                send_sem=sum_send_sems.at[offset + k], recv_sem=sum_recv_sems.at[offset + k],
                device_id=peer, device_id_type=MESH,
            )
            copy.start()
            copies.append(copy)
        for copy in copies:
            copy.wait()
        total = ref[0]
        for other in range(1, ref.shape[0]):
            total = total + ref[other]
        return total

    stage2_ref[base] = share_out(stage_ref, freq, ring, 0)
    total = share_out(stage2_ref, base, line, len(ring))
    spectrum_ref[...] = total[:lead] / total[lead:]

    def finish(n, carry):
        for k in range(RADIX):
            target, _, _, copy = piece(n, k)

            @pl.when(target != freq)
            def _():
                copy.wait_send()
        return carry

    lax.fori_loop(0, shares * parts, finish, 0)


def power_and_spectrum(h, dh, dl, bins, grid, freq_count, base_count, split, width, scale):
    channels, _, slab, both = h.shape
    cols = both // 2
    share_rows = grid // freq_count
    chunk = min(64, share_rows)
    parts, shares = share_rows // chunk, slab // share_rows
    high_count = NBINS // BIN_LOW
    cells = share_rows * width
    sems = freq_count + base_count - 2
    f32, bf16 = jnp.float32, jnp.bfloat16
    vmem = pl.BlockSpec(memory_space=pltpu.VMEM)
    hbm = pl.BlockSpec(memory_space=pltpu.HBM)
    return pl.pallas_call(
        functools.partial(power_kernel, grid, freq_count, base_count, split, scale),
        out_shape=(
            jax.ShapeDtypeStruct((share_rows, width), f32),
            jax.ShapeDtypeStruct((4, 4 * BIN_LOW), f32),
        ),
        in_specs=[vmem, hbm, hbm, hbm],
        out_specs=(vmem, vmem),
        scratch_shapes=[
            pltpu.VMEM(dh.shape, bf16),
            pltpu.VMEM(dl.shape, bf16),
            pltpu.VMEM((bins.shape[0], share_rows), jnp.int32),
            pltpu.SemaphoreType.DMA((2, RADIX)),
            pltpu.SemaphoreType.DMA,
            pltpu.VMEM(h.shape, bf16),
            pltpu.VMEM(h.shape, bf16),
            pltpu.VMEM((2, RADIX, 2 * chunk, both), f32),
            pltpu.VMEM((grid, cols), f32),
            pltpu.VMEM((freq_count, share_rows, cols), f32),
            pltpu.VMEM((high_count, cells), bf16),
            pltpu.VMEM((2 * high_count, chunk * width), bf16),
            pltpu.VMEM((BIN_LOW, cells), bf16),
            pltpu.VMEM((freq_count, 8, 4 * BIN_LOW), f32),
            pltpu.VMEM((base_count, 8, 4 * BIN_LOW), f32),
            pltpu.SemaphoreType.DMA((shares * parts, RADIX)),
            pltpu.SemaphoreType.DMA((freq_count, parts)),
            pltpu.SemaphoreType.DMA((sems,)),
            pltpu.SemaphoreType.DMA((sems,)),
        ],
        compiler_params=pltpu.CompilerParams(
            collective_id=1, has_side_effects=True, vmem_limit_bytes=24 * 2**20
        ),
        name="power_and_spectrum",
    )(h, in_hbm(dh), in_hbm(dl), in_hbm(bins))


def per_device(visibility, tile_of, u_within, v_cell, kernel_index, kernel, live_count, bin_map):
    base_count = lax.axis_size("base")
    freq_count = lax.axis_size("freq")
    grid = bin_map.shape[1]
    width = grid // base_count
    split = 2 if width % (2 * LANES) == 0 and freq_count % 2 == 0 else 1
    channels_here, slots = u_within.shape
    dh, dl = transform_tables(grid)
    scale = 1.0 / (channels_here * freq_count * slots * base_count)
    gathered = gather_fields(
        split, base_count, grid // base_count, grid, width // split,
        visibility, tile_of.transpose(0, 2, 1), u_within, v_cell, kernel_index, live_count.T, kernel.T,
    )
    h = grid_visibilities(*gathered, grid)
    share_rows = grid // freq_count
    bins = bin_map
    if share_rows % LANES:
        bins = lax.dynamic_slice_in_dim(bin_map, lax.axis_index("freq") * share_rows, share_rows, 1)
    share, spectrum = power_and_spectrum(
        h, jnp.asarray(dh), jnp.asarray(dl), bins, grid, freq_count, base_count, split, width, scale
    )
    return share, spectrum.reshape(NBINS)


def solution(mesh):
    in_specs = (
        P(None, "freq", "base"),
        P("freq", "base", None),
        P("freq", "base"),
        P("freq", "base"),
        P(None, "freq", "base"),
        P(),
        P("freq", "base"),
        P("base", None),
    )
    out_specs = (P("freq", "base"), P())
    return jax.shard_map(
        per_device, mesh=mesh, in_specs=in_specs, out_specs=out_specs, check_vma=False
    )
```

```python
import functools
import math

import jax
import jax.numpy as jnp
import numpy as np
from jax import lax
from jax.experimental import pallas as pl
from jax.experimental.pallas import tpu as pltpu
from jax.sharding import PartitionSpec as P

NBINS = 512
BIN_LOW = 32
KW = 8
FINE = 32
SPREAD = FINE + KW
RADIX = 4
GROUP = 16
FIELDS = 6
LANES = 128
MESH = pl.DeviceIdType.MESH


def halves_of(x):
    high = x.astype(jnp.bfloat16)
    low = (x - high.astype(jnp.float32)).astype(jnp.bfloat16)
    return high, low


@functools.lru_cache(None)
def transform_tables(grid):
    slab = grid // RADIX
    order = np.arange(slab)
    u = 2 * RADIX * (order % (slab // 2)) + RADIX * (order // (slab // 2))
    u = u[None, None, :] + np.arange(RADIX)[:, None, None]
    angle = ((np.arange(slab)[None, :, None] * u) % grid) * (2.0 * math.pi / grid)
    x = np.concatenate([np.cos(angle), np.sin(angle)], axis=1).astype(np.float32)
    high = x.astype(jnp.bfloat16)
    low = (x - high.astype(np.float32)).astype(jnp.bfloat16)
    return high, low


def dot(a, b):
    return jnp.dot(a, b, preferred_element_type=jnp.float32)


def dot_rows(a, b):
    return lax.dot_general(a, b, (((1,), (1,)), ((), ())), preferred_element_type=jnp.float32)


def in_hbm(x):
    return pltpu.with_memory_space_constraint(x, pltpu.HBM)


def greet(peers):
    barrier = pltpu.get_barrier_semaphore()
    for peer in peers:
        pl.semaphore_signal(barrier, inc=1, device_id=peer, device_id_type=MESH)
    return barrier


def phase(product, grid):
    half = grid // 2
    angle = ((product + half) & (grid - 1)) - half
    angle = angle.astype(jnp.float32) * (2.0 * math.pi / grid)
    return jnp.cos(angle), jnp.sin(angle)


def column_tables(grid, split, fine_ref, coarse_ref):
    cols = fine_ref.shape[0] // 2
    coarse_count = grid // FINE
    left = (lax.axis_index("base") * split + lax.rem(lax.axis_index("freq"), split)) * cols
    l = left + lax.broadcasted_iota(jnp.int32, (cols, SPREAD), 0)
    c, s = phase(l * lax.broadcasted_iota(jnp.int32, (cols, SPREAD), 1), grid)
    fine = jnp.concatenate(
        [jnp.concatenate([c, s], axis=1), jnp.concatenate([-s, c], axis=1)], axis=0
    )
    fh, fl = halves_of(fine)
    fine_ref[...] = jnp.zeros_like(fine_ref)
    fine_ref[:, 0:2 * SPREAD] = fh
    fine_ref[:, 2 * SPREAD:4 * SPREAD] = fl
    fine_ref[:, 4 * SPREAD:6 * SPREAD] = fh
    l = lax.broadcasted_iota(jnp.int32, (coarse_count, coarse_count), 0)
    c, s = phase(l * lax.broadcasted_iota(jnp.int32, (coarse_count, coarse_count), 1) * FINE, grid)
    ch, cl = halves_of(jnp.concatenate([c, -s], axis=0))
    coarse_ref[:, 0:coarse_count] = ch
    coarse_ref[:, coarse_count:] = cl


def gather_kernel(
    split, base_count, tile_rows, grid, vis_hbm, tile_hbm, within_hbm, column_hbm, index_hbm, live_hbm,
    taps_hbm, out_ref, fine_ref, coarse_ref, taps_ref,
    vis_ref, tile_ref, within_ref, column_ref, index_ref, live_ref, load_sems, send_sems, recv_sems
):
    freq, base = lax.axis_index("freq"), lax.axis_index("base")
    part = lax.rem(freq, split)
    first = freq - part
    line = [{"freq": freq, "base": lax.rem(base + d, base_count)} for d in range(1, base_count)]
    mates = [{"freq": first + lax.rem(part + d, split), "base": base} for d in range(1, split)]
    barrier = greet(line + mates)
    loads = [
        pltpu.make_async_copy(a, b, load_sems.at[n])
        for n, (a, b) in enumerate([
            (vis_hbm, vis_ref), (tile_hbm, tile_ref), (within_hbm, within_ref), (column_hbm, column_ref),
            (index_hbm, index_ref), (live_hbm, live_ref), (taps_hbm, taps_ref),
        ])
    ]
    for load in loads:
        load.start()
    for load in loads:
        load.wait()
    channels, slots = within_ref.shape
    lane = lax.broadcasted_iota(jnp.int32, (1, slots), 1)
    for c in range(channels):
        is_live = lane < live_ref[0:1, c:c + 1]
        u = jnp.minimum(tile_ref[c] * tile_rows + within_ref[c:c + 1, :], grid - KW)
        fields = [
            jnp.where(is_live, vis_ref[0, c:c + 1, :], 0.0),
            jnp.where(is_live, vis_ref[1, c:c + 1, :], 0.0),
            u.astype(jnp.float32),
            column_ref[c:c + 1, :].astype(jnp.float32),
            jnp.where(is_live, index_ref[0, c:c + 1, :], -1).astype(jnp.float32),
            index_ref[1, c:c + 1, :].astype(jnp.float32),
        ]
        rows = [x[:, at:at + LANES] for x in fields for at in range(0, slots, LANES)]
        out_ref[part * channels + c, base] = jnp.concatenate(rows, axis=0)
    column_tables(grid, split, fine_ref, coarse_ref)
    pl.semaphore_wait(barrier, len(line) + len(mates))

    def block_copy(owner, peer, k):
        block = out_ref.at[pl.ds(part * channels, channels), owner]
        return pltpu.make_async_remote_copy(
            src_ref=block, dst_ref=block, send_sem=send_sems.at[k], recv_sem=recv_sems.at[k],
            device_id=peer, device_id_type=MESH,
        )

    sent = [block_copy(base, peer, k) for k, peer in enumerate(line)]
    for copy in sent:
        copy.start()
    passed = []
    for d in range(base_count):
        if d:
            sent[d - 1].wait_recv()
        for k, mate in enumerate(mates):
            copy = block_copy(
                lax.rem(base + base_count - d, base_count), mate, len(line) + k * base_count + d
            )
            copy.start()
            passed.append(copy)
    for copy in passed:
        copy.wait()
    for copy in sent:
        copy.wait_send()


def gather_fields(split, base_count, tile_rows, grid, cols, *arrays):
    channels, slots = arrays[2].shape
    sems = base_count - 1 + (split - 1) * base_count
    total = channels * split
    f32, bf16 = jnp.float32, jnp.bfloat16
    vmem = pl.BlockSpec(memory_space=pltpu.VMEM)
    hbm = pl.BlockSpec(memory_space=pltpu.HBM)
    return pl.pallas_call(
        functools.partial(gather_kernel, split, base_count, tile_rows, grid),
        out_shape=(
            jax.ShapeDtypeStruct((total, base_count, FIELDS * (slots // LANES), LANES), f32),
            jax.ShapeDtypeStruct((2 * cols, 256), bf16),
            jax.ShapeDtypeStruct((2 * (grid // FINE), 2 * (grid // FINE)), bf16),
            jax.ShapeDtypeStruct(arrays[-1].shape, f32),
        ),
        in_specs=[hbm] * len(arrays),
        out_specs=(vmem,) * 4,
        scratch_shapes=[pltpu.VMEM(x.shape, x.dtype) for x in arrays[:-1]] + [
            pltpu.SemaphoreType.DMA((len(arrays),)),
            pltpu.SemaphoreType.DMA((sems,)), pltpu.SemaphoreType.DMA((sems,)),
        ],
        compiler_params=pltpu.CompilerParams(
            collective_id=0, has_side_effects=True, vmem_limit_bytes=12 * 2**20
        ),
        name="gather_fields",
    )(*[in_hbm(x) for x in arrays])


def grid_kernel(
    grid, f_ref, fine_ref, coarse_ref, kernel_ref, h_ref,
    spread_ref, pick_ref, z_ref, tap_ref, spot_ref, channel_ref
):
    channels, blocks, rows, _ = f_ref.shape
    subs = rows // FIELDS
    cols = h_ref.shape[3] // 2
    half = grid // (2 * RADIX)
    coarse_count = grid // FINE
    piece = 2 * LANES
    tap_table = kernel_ref[...]
    h_ref[...] = jnp.zeros_like(h_ref)

    counts = []
    for c in range(channels):
        for b in range(blocks):
            used = f_ref[c, b, 4 * subs:5 * subs, :] >= 0.0
            counts.append(jnp.sum(jnp.where(used, 1.0, 0.0)))
    filled = jnp.int32(0)
    for c in range(channels):
        for b in range(blocks):
            for sub in range(subs):
                spot_ref[filled + sub] = b * subs + sub
            for ahead in range(subs // 2 + 1):
                channel_ref[lax.shift_right_logical(filled, jnp.int32(1)) + ahead] = c
            count = counts[c * blocks + b].astype(jnp.int32)
            filled = filled + lax.shift_right_logical(count + (LANES - 1), jnp.int32(LANES.bit_length() - 1))
        spot_ref[filled] = -1
        filled = (filled + 1) & -2
    steps = lax.shift_right_logical(filled, jnp.int32(1))
    for ahead in range(8):
        spot_ref[filled + ahead] = -1
    for ahead in range(4):
        channel_ref[steps + ahead] = 0

    def field(step, number):
        c = channel_ref[step]
        one, two = jnp.maximum(spot_ref[2 * step], 0), jnp.maximum(spot_ref[2 * step + 1], 0)
        by = jnp.int32(subs.bit_length() - 1)
        return jnp.concatenate(
            [
                f_ref[c, lax.shift_right_logical(one, by), pl.ds(number * subs + (one & (subs - 1)), 1), :],
                f_ref[c, lax.shift_right_logical(two, by), pl.ds(number * subs + (two & (subs - 1)), 1), :],
            ],
            axis=1,
        )

    def look_up(table, row):
        row = jnp.maximum(row.astype(jnp.int32), 0)
        pieces = []
        for at in range(0, piece, LANES):
            index = jnp.broadcast_to(row[:, at:at + LANES], (KW, LANES))
            pieces.append(jnp.take_along_axis(table, index, axis=1))
        return jnp.concatenate(pieces, axis=1)

    lane = lax.broadcasted_iota(jnp.int32, (1, piece), 1)

    def make_spread(step, slot):
        keep = lane < jnp.where(
            spot_ref[2 * step + 1] >= 0, piece, jnp.where(spot_ref[2 * step] >= 0, LANES, 0)
        )
        re = jnp.where(keep, field(step, 0), 0.0)
        im = jnp.where(keep, field(step, 1), 0.0)
        v = field(step, 3).astype(jnp.int32)
        taps_v = look_up(tap_table, field(step, 5))
        offset = lax.broadcasted_iota(jnp.int32, (SPREAD, piece), 0) - (v & (FINE - 1))
        spread = jnp.zeros((SPREAD, piece), jnp.float32)
        for t in range(KW):
            spread = jnp.where(offset == t, taps_v[t:t + 1, :], spread)
        both = jnp.concatenate([spread * re, spread * im], axis=0)
        bh, bl = halves_of(both)
        pad = jnp.zeros((256 - 6 * SPREAD, piece), jnp.bfloat16)
        spread_ref[slot] = jnp.concatenate([bh, bh, bl, pad], axis=0)
        pick = lax.broadcasted_iota(jnp.int32, (2 * coarse_count, piece), 0) & (coarse_count - 1)
        pick_ref[slot] = jnp.where(pick == v // FINE, 1.0, 0.0).astype(jnp.bfloat16)

    def make_z(step, slot):
        zb = dot(fine_ref[...], spread_ref[slot])
        e = dot(coarse_ref[...], pick_ref[slot])
        er, ei = e[:coarse_count], e[coarse_count:]
        re, im = [], []
        for at in range(0, cols, coarse_count):
            zr, zi = zb[at:at + coarse_count], zb[cols + at:cols + at + coarse_count]
            re.append(zr * er - zi * ei)
            im.append(zr * ei + zi * er)
        for n, parts in enumerate((re, im)):
            zh, zl = halves_of(jnp.concatenate(parts, axis=0).T)
            z_ref[slot, 0, :, n * cols:(n + 1) * cols] = zh
            z_ref[slot, 1, :, n * cols:(n + 1) * cols] = zl

        u = field(step, 2).astype(jnp.int32)
        taps_u = look_up(tap_table, field(step, 4))
        residue = lax.broadcasted_iota(jnp.int32, (2 * RADIX, piece), 0)
        tap = (residue - u) & (2 * RADIX - 1)
        row = lax.shift_right_logical(u + tap, jnp.int32((2 * RADIX).bit_length() - 1))
        weight = jnp.zeros((2 * RADIX, piece), jnp.float32)
        for t in range(KW):
            weight = jnp.where(tap == t, taps_u[t:t + 1, :], weight)
        high = weight.astype(jnp.bfloat16).astype(jnp.float32)
        tap_ref[slot, 0] = row.astype(jnp.float32)
        tap_ref[slot, 1] = high
        tap_ref[slot, 2] = weight - high

    def add_rows(step, slot):
        c = channel_ref[step]
        rows16 = lax.broadcasted_iota(jnp.int32, (GROUP, piece), 0).astype(jnp.float32)
        spots = [(rows16 + float(at)).astype(jnp.bfloat16) for at in range(0, half, GROUP)]

        def wide(kind, residue):
            x = tap_ref[slot, kind, residue:residue + 1, :]
            return jnp.broadcast_to(x, (GROUP, piece)).astype(jnp.bfloat16)

        for first in range(RADIX):
            highs, lows = [], []
            for residue in (first, first + RADIX):
                row, high, low = (wide(kind, residue) for kind in range(3))
                zero = jnp.zeros_like(high)
                for spot in spots:
                    hit = row == spot
                    highs.append(jnp.where(hit, high, zero))
                    lows.append(jnp.where(hit, low, zero))
            wh, wl = jnp.concatenate(highs, axis=0), jnp.concatenate(lows, axis=0)
            zh, zl = z_ref[slot, 0], z_ref[slot, 1]
            h_ref[c, first] += dot(wh, zh) + dot(wh, zl) + dot(wl, zh)

    make_spread(0, 0)
    make_z(0, 0)
    make_spread(1, 1)

    def two_steps(n, carry):
        for slot in range(2):
            step = 2 * n + slot
            make_z(step + 1, 1 - slot)
            add_rows(step, slot)
            make_spread(step + 2, slot)
        return carry

    lax.fori_loop(0, (steps + 1) // 2, two_steps, 0)


def grid_visibilities(fields, fine, coarse, taps_table, grid):
    both = fine.shape[0]
    channels, blocks, rows, _ = fields.shape
    most = channels * (blocks * (rows // FIELDS) + 1)
    smem = lambda n: pltpu.SMEM((n,), jnp.int32)
    vmem = pl.BlockSpec(memory_space=pltpu.VMEM)
    return pl.pallas_call(
        functools.partial(grid_kernel, grid),
        out_shape=jax.ShapeDtypeStruct((channels, RADIX, grid // RADIX, both), jnp.float32),
        in_specs=[vmem] * 4,
        out_specs=vmem,
        scratch_shapes=[
            pltpu.VMEM((2, 256, 2 * LANES), jnp.bfloat16),
            pltpu.VMEM((2, 2 * (grid // FINE), 2 * LANES), jnp.bfloat16),
            pltpu.VMEM((2, 2, 2 * LANES, both), jnp.bfloat16),
            pltpu.VMEM((2, 3, 2 * RADIX, 2 * LANES), jnp.float32),
            smem(most + 16), smem(most // 2 + 16),
        ],
        compiler_params=pltpu.CompilerParams(vmem_limit_bytes=16 * 2**20),
        name="grid_visibilities",
    )(fields, fine, coarse, taps_table)


def power_kernel(
    grid, freq_count, base_count, split, scale, h_ref, dh_hbm, dl_hbm, bins_hbm, share_ref, spectrum_ref,
    dh_ref, dl_ref, bins_ref, load_sems, bins_sem, hh_ref, hl_ref, y_ref, power_ref, recv_ref, mask_ref, value_ref, low_ref, stage_ref, stage2_ref,
    send_sems, recv_sems, sum_send_sems, sum_recv_sems
):
    freq, base = lax.axis_index("freq"), lax.axis_index("base")
    ring = [{"freq": lax.rem(freq + d, freq_count), "base": base} for d in range(1, freq_count)]
    line = [{"freq": freq, "base": lax.rem(base + d, base_count)} for d in range(1, base_count)]
    barrier = greet(ring + line)
    loads = []
    for n in range(RADIX):
        loads.append(pltpu.make_async_copy(dh_hbm.at[n], dh_ref.at[n], load_sems.at[0, n]))
        loads.append(pltpu.make_async_copy(dl_hbm.at[n], dl_ref.at[n], load_sems.at[1, n]))
    for load in loads:
        load.start()
    rows_here = bins_ref.shape[1]
    if bins_hbm.shape[1] != rows_here:
        here = pl.ds(pl.multiple_of(freq * rows_here, rows_here), rows_here)
        load_bins = pltpu.make_async_copy(bins_hbm.at[:, here], bins_ref, bins_sem)
    else:
        load_bins = pltpu.make_async_copy(bins_hbm, bins_ref, bins_sem)
    load_bins.start()

    channels = h_ref.shape[0]
    slab = grid // RADIX
    share_rows, width = share_ref.shape
    cols = width // split
    chunk = min(64, share_rows)
    parts = share_rows // chunk
    shares = slab // share_rows

    def split_rows(n, carry):
        high, low = halves_of(h_ref[n // RADIX, n % RADIX])
        hh_ref[n // RADIX, n % RADIX] = high
        hl_ref[n // RADIX, n % RADIX] = low
        return carry

    lax.fori_loop(0, channels * RADIX, split_rows, 0)
    for load in loads:
        load.wait()

    def transform(n):
        top = pl.multiple_of((lax.rem(n, shares) * parts + n // shares) * chunk, chunk)
        for c in range(channels):
            for first in range(RADIX):
                dh = jnp.concatenate(
                    [dh_ref[first, pl.ds(top, chunk), :], dh_ref[first, pl.ds(slab + top, chunk), :]], axis=0
                )
                dl = jnp.concatenate(
                    [dl_ref[first, pl.ds(top, chunk), :], dl_ref[first, pl.ds(slab + top, chunk), :]], axis=0
                )
                hh, hl = hh_ref[c, first], hl_ref[c, first]
                y_ref[c % 2, first] = dot(dh, hh) + dot(dl, hh) + dot(dh, hl)
            step = min(16, chunk)
            for row in range(0, chunk, step):
                yr, yi = [], []
                for first in range(RADIX):
                    cy = y_ref[c % 2, first, row:row + step, :]
                    sy = y_ref[c % 2, first, chunk + row:chunk + row + step, :]
                    yr.append(cy[:, :cols] + sy[:, cols:])
                    yi.append(cy[:, cols:] - sy[:, :cols])
                ar, ai = yr[0] + yr[2], yi[0] + yi[2]
                br, bi = yr[0] - yr[2], yi[0] - yi[2]
                cr, ci = yr[1] + yr[3], yi[1] + yi[3]
                dr, di = yr[1] - yr[3], yi[1] - yi[3]
                outs = [
                    (ar + cr, ai + ci), (br + di, bi - dr), (ar - cr, ai - ci), (br - di, bi + dr)
                ]
                for k, (xr, xi) in enumerate(outs):
                    at = pl.ds(pl.multiple_of(k * slab + top + row, step), step)
                    value = (xr * xr + xi * xi) * scale
                    power_ref[at, :] = value if c == 0 else power_ref[at, :] + value

    def piece(n, k):
        share, part = lax.rem(n, shares), n // shares
        target = k * shares + share
        top = pl.multiple_of(target * share_rows + part * chunk, chunk)
        rows = pl.ds(pl.multiple_of(part * chunk, chunk), chunk)
        copy = pltpu.make_async_remote_copy(
            src_ref=power_ref.at[pl.ds(top, chunk), :],
            dst_ref=recv_ref.at[freq, rows, :],
            send_sem=send_sems.at[n, k], recv_sem=recv_sems.at[freq, part],
            device_id={"freq": target, "base": base}, device_id_type=MESH,
        )
        return target, top, rows, copy

    def send(n):
        for k in range(RADIX):
            target, top, rows, copy = piece(n, k)

            @pl.when(target == freq)
            def _():
                recv_ref[freq, rows, :] = power_ref[pl.ds(top, chunk), :]

            @pl.when(target != freq)
            def _():
                copy.start()

    transform(0)
    pl.semaphore_wait(barrier, len(ring) + len(line))
    send(0)

    def later(n, carry):
        transform(n)
        send(n)
        return carry

    lax.fori_loop(1, shares * parts, later, 0)

    high_count = NBINS // BIN_LOW
    lead = high_count // 4
    load_bins.wait()
    bins = bins_ref[...].T
    order = lax.broadcasted_iota(jnp.int32, (high_count, width), 0)
    order = lead * (order % lead) + order // lead if lead == 4 else order
    low_order = lax.broadcasted_iota(jnp.int32, (BIN_LOW, width), 0)
    for row in range(share_rows):
        at = slice(row * width, (row + 1) * width)
        bin_id = bins[row:row + 1, :]
        mask_ref[:, at] = jnp.where(order == bin_id // BIN_LOW, 1.0, 0.0).astype(jnp.bfloat16)
        low_ref[:, at] = jnp.where(low_order == bin_id % BIN_LOW, 1.0, 0.0).astype(jnp.bfloat16)
    counts = dot_rows(mask_ref[...], low_ref[...])

    totals = jnp.zeros((high_count, BIN_LOW), jnp.float32)
    for part in range(parts):
        rows = slice(part * chunk, (part + 1) * chunk)
        for d in range(1, freq_count):
            source = lax.rem(freq + d, freq_count)
            pltpu.make_async_remote_copy(
                src_ref=power_ref.at[0:chunk, :], dst_ref=recv_ref.at[source, rows, :],
                send_sem=send_sems.at[0, 0], recv_sem=recv_sems.at[source, part],
                device_id={"freq": source, "base": base}, device_id_type=MESH,
            ).wait_recv()
        for half in range(split):
            total = recv_ref[half, rows, :]
            for group in range(1, freq_count // split):
                total = total + recv_ref[group * split + half, rows, :]
            share_ref[rows, half * cols:(half + 1) * cols] = total
        for row in range(part * chunk, (part + 1) * chunk):
            at = slice(row * width, (row + 1) * width)
            out = slice((row - part * chunk) * width, (row - part * chunk + 1) * width)
            value = jnp.broadcast_to(share_ref[row:row + 1, :], (high_count, width))
            high, low = halves_of(value)
            mask = mask_ref[:, at]
            value_ref[0:high_count, out] = mask * high
            value_ref[high_count:, out] = mask * low
        span = slice(part * chunk * width, (part + 1) * chunk * width)
        sums = dot_rows(value_ref[...], low_ref[:, span])
        totals = totals + sums[:high_count] + sums[high_count:]

    def pack(x):
        return jnp.concatenate([x[lead * k:lead * (k + 1)] for k in range(4)], axis=1)

    stage_ref[freq] = jnp.concatenate([pack(totals), pack(counts)], axis=0)

    def share_out(ref, me, peers, offset):
        copies = []
        for k, peer in enumerate(peers):
            copy = pltpu.make_async_remote_copy(
                src_ref=ref.at[me], dst_ref=ref.at[me],
                send_sem=sum_send_sems.at[offset + k], recv_sem=sum_recv_sems.at[offset + k],
                device_id=peer, device_id_type=MESH,
            )
            copy.start()
            copies.append(copy)
        for copy in copies:
            copy.wait()
        total = ref[0]
        for other in range(1, ref.shape[0]):
            total = total + ref[other]
        return total

    stage2_ref[base] = share_out(stage_ref, freq, ring, 0)
    total = share_out(stage2_ref, base, line, len(ring))
    spectrum_ref[...] = total[:lead] / total[lead:]

    def finish(n, carry):
        for k in range(RADIX):
            target, _, _, copy = piece(n, k)

            @pl.when(target != freq)
            def _():
                copy.wait_send()
        return carry

    lax.fori_loop(0, shares * parts, finish, 0)


def power_and_spectrum(h, dh, dl, bins, grid, freq_count, base_count, split, width, scale):
    channels, _, slab, both = h.shape
    cols = both // 2
    share_rows = grid // freq_count
    chunk = min(64, share_rows)
    parts, shares = share_rows // chunk, slab // share_rows
    high_count = NBINS // BIN_LOW
    cells = share_rows * width
    sems = freq_count + base_count - 2
    f32, bf16 = jnp.float32, jnp.bfloat16
    vmem = pl.BlockSpec(memory_space=pltpu.VMEM)
    hbm = pl.BlockSpec(memory_space=pltpu.HBM)
    return pl.pallas_call(
        functools.partial(power_kernel, grid, freq_count, base_count, split, scale),
        out_shape=(
            jax.ShapeDtypeStruct((share_rows, width), f32),
            jax.ShapeDtypeStruct((4, 4 * BIN_LOW), f32),
        ),
        in_specs=[vmem, hbm, hbm, hbm],
        out_specs=(vmem, vmem),
        scratch_shapes=[
            pltpu.VMEM(dh.shape, bf16),
            pltpu.VMEM(dl.shape, bf16),
            pltpu.VMEM((bins.shape[0], share_rows), jnp.int32),
            pltpu.SemaphoreType.DMA((2, RADIX)),
            pltpu.SemaphoreType.DMA,
            pltpu.VMEM(h.shape, bf16),
            pltpu.VMEM(h.shape, bf16),
            pltpu.VMEM((2, RADIX, 2 * chunk, both), f32),
            pltpu.VMEM((grid, cols), f32),
            pltpu.VMEM((freq_count, share_rows, cols), f32),
            pltpu.VMEM((high_count, cells), bf16),
            pltpu.VMEM((2 * high_count, chunk * width), bf16),
            pltpu.VMEM((BIN_LOW, cells), bf16),
            pltpu.VMEM((freq_count, 8, 4 * BIN_LOW), f32),
            pltpu.VMEM((base_count, 8, 4 * BIN_LOW), f32),
            pltpu.SemaphoreType.DMA((shares * parts, RADIX)),
            pltpu.SemaphoreType.DMA((freq_count, parts)),
            pltpu.SemaphoreType.DMA((sems,)),
            pltpu.SemaphoreType.DMA((sems,)),
        ],
        compiler_params=pltpu.CompilerParams(
            collective_id=1, has_side_effects=True, vmem_limit_bytes=24 * 2**20
        ),
        name="power_and_spectrum",
    )(h, in_hbm(dh), in_hbm(dl), in_hbm(bins))


def per_device(visibility, tile_of, u_within, v_cell, kernel_index, kernel, live_count, bin_map):
    base_count = lax.axis_size("base")
    freq_count = lax.axis_size("freq")
    grid = bin_map.shape[1]
    width = grid // base_count
    split = 2 if width % (2 * LANES) == 0 and freq_count % 2 == 0 else 1
    channels_here, slots = u_within.shape
    dh, dl = transform_tables(grid)
    scale = 1.0 / (channels_here * freq_count * slots * base_count)
    gathered = gather_fields(
        split, base_count, grid // base_count, grid, width // split,
        visibility, tile_of.transpose(0, 2, 1), u_within, v_cell, kernel_index, live_count.T, kernel.T,
    )
    h = grid_visibilities(*gathered, grid)
    share_rows = grid // freq_count
    bins = bin_map
    if share_rows % LANES:
        bins = lax.dynamic_slice_in_dim(bin_map, lax.axis_index("freq") * share_rows, share_rows, 1)
    share, spectrum = power_and_spectrum(
        h, jnp.asarray(dh), jnp.asarray(dl), bins, grid, freq_count, base_count, split, width, scale
    )
    return share, spectrum.reshape(NBINS)


def solution(mesh):
    in_specs = (
        P(None, "freq", "base"),
        P("freq", "base", None),
        P("freq", "base"),
        P("freq", "base"),
        P(None, "freq", "base"),
        P(),
        P("freq", "base"),
        P("base", None),
    )
    out_specs = (P("freq", "base"), P())
    return jax.shard_map(
        per_device, mesh=mesh, in_specs=in_specs, out_specs=out_specs, check_vma=False
    )
```

```python
import functools
import math

import jax
import jax.numpy as jnp
import numpy as np
from jax import lax
from jax.experimental import pallas as pl
from jax.experimental.pallas import tpu as pltpu
from jax.sharding import PartitionSpec as P

NBINS = 512
BIN_LOW = 32
KW = 8
FINE = 32
SPREAD = FINE + KW
RADIX = 4
GROUP = 16
FIELDS = 6
LANES = 128
MESH = pl.DeviceIdType.MESH


def halves_of(x):
    high = x.astype(jnp.bfloat16)
    low = (x - high.astype(jnp.float32)).astype(jnp.bfloat16)
    return high, low


@functools.lru_cache(None)
def transform_tables(grid):
    slab = grid // RADIX
    order = np.arange(slab)
    u = 2 * RADIX * (order % (slab // 2)) + RADIX * (order // (slab // 2))
    u = u[None, None, :] + np.arange(RADIX)[:, None, None]
    angle = ((np.arange(slab)[None, :, None] * u) % grid) * (2.0 * math.pi / grid)
    x = np.concatenate([np.cos(angle), np.sin(angle)], axis=1).astype(np.float32)
    high = x.astype(jnp.bfloat16)
    low = (x - high.astype(np.float32)).astype(jnp.bfloat16)
    return high, low


def dot(a, b):
    return jnp.dot(a, b, preferred_element_type=jnp.float32)


def dot_rows(a, b):
    return lax.dot_general(a, b, (((1,), (1,)), ((), ())), preferred_element_type=jnp.float32)


def in_hbm(x):
    return pltpu.with_memory_space_constraint(x, pltpu.HBM)


def greet(peers):
    barrier = pltpu.get_barrier_semaphore()
    for peer in peers:
        pl.semaphore_signal(barrier, inc=1, device_id=peer, device_id_type=MESH)
    return barrier


def phase(product, grid):
    half = grid // 2
    angle = ((product + half) & (grid - 1)) - half
    angle = angle.astype(jnp.float32) * (2.0 * math.pi / grid)
    return jnp.cos(angle), jnp.sin(angle)


def column_tables(grid, split, fine_ref, coarse_ref):
    cols = fine_ref.shape[0] // 2
    coarse_count = grid // FINE
    left = (lax.axis_index("base") * split + lax.rem(lax.axis_index("freq"), split)) * cols
    l = left + lax.broadcasted_iota(jnp.int32, (cols, SPREAD), 0)
    c, s = phase(l * lax.broadcasted_iota(jnp.int32, (cols, SPREAD), 1), grid)
    fine = jnp.concatenate(
        [jnp.concatenate([c, s], axis=1), jnp.concatenate([-s, c], axis=1)], axis=0
    )
    fh, fl = halves_of(fine)
    fine_ref[...] = jnp.zeros_like(fine_ref)
    fine_ref[:, 0:2 * SPREAD] = fh
    fine_ref[:, 2 * SPREAD:4 * SPREAD] = fl
    fine_ref[:, 4 * SPREAD:6 * SPREAD] = fh
    l = lax.broadcasted_iota(jnp.int32, (coarse_count, coarse_count), 0)
    c, s = phase(l * lax.broadcasted_iota(jnp.int32, (coarse_count, coarse_count), 1) * FINE, grid)
    ch, cl = halves_of(jnp.concatenate([c, -s], axis=0))
    coarse_ref[:, 0:coarse_count] = ch
    coarse_ref[:, coarse_count:] = cl


def look_up(table, row):
    row = jnp.maximum(row.astype(jnp.int32), 0)
    pieces = []
    for at in range(0, row.shape[1], LANES):
        index = jnp.broadcast_to(row[:, at:at + LANES], (KW, LANES))
        pieces.append(jnp.take_along_axis(table, index, axis=1))
    return jnp.concatenate(pieces, axis=1)


def store_spread(grid, table, field, keep, slot, spread_ref, pick_ref):
    re, im = field(0), field(1)
    if keep is not None:
        re, im = jnp.where(keep, re, 0.0), jnp.where(keep, im, 0.0)
    piece = re.shape[1]
    coarse_count = grid // FINE
    v = field(3).astype(jnp.int32)
    taps_v = look_up(table, field(5))
    offset = lax.broadcasted_iota(jnp.int32, (SPREAD, piece), 0) - (v & (FINE - 1))
    spread = jnp.zeros((SPREAD, piece), jnp.float32)
    for t in range(KW):
        spread = jnp.where(offset == t, taps_v[t:t + 1, :], spread)
    both = jnp.concatenate([spread * re, spread * im], axis=0)
    bh, bl = halves_of(both)
    pad = jnp.zeros((256 - 6 * SPREAD, piece), jnp.bfloat16)
    spread_ref[slot] = jnp.concatenate([bh, bh, bl, pad], axis=0)
    pick = lax.broadcasted_iota(jnp.int32, (2 * coarse_count, piece), 0) & (coarse_count - 1)
    pick_ref[slot] = jnp.where(pick == v // FINE, 1.0, 0.0).astype(jnp.bfloat16)


def store_z(grid, table, field, slot, fine_ref, coarse_ref, spread_ref, pick_ref, z_ref, tap_ref):
    cols = fine_ref.shape[0] // 2
    coarse_count = grid // FINE
    zb = dot(fine_ref[...], spread_ref[slot])
    e = dot(coarse_ref[...], pick_ref[slot])
    er, ei = e[:coarse_count], e[coarse_count:]
    re, im = [], []
    for at in range(0, cols, coarse_count):
        zr, zi = zb[at:at + coarse_count], zb[cols + at:cols + at + coarse_count]
        re.append(zr * er - zi * ei)
        im.append(zr * ei + zi * er)
    for n, parts in enumerate((re, im)):
        zh, zl = halves_of(jnp.concatenate(parts, axis=0).T)
        z_ref[slot, 0, :, n * cols:(n + 1) * cols] = zh
        z_ref[slot, 1, :, n * cols:(n + 1) * cols] = zl

    u = field(2).astype(jnp.int32)
    taps_u = look_up(table, field(4))
    residue = lax.broadcasted_iota(jnp.int32, (2 * RADIX, u.shape[1]), 0)
    tap = (residue - u) & (2 * RADIX - 1)
    row = lax.shift_right_logical(u + tap, jnp.int32((2 * RADIX).bit_length() - 1))
    weight = jnp.zeros(tap.shape, jnp.float32)
    for t in range(KW):
        weight = jnp.where(tap == t, taps_u[t:t + 1, :], weight)
    high = weight.astype(jnp.bfloat16).astype(jnp.float32)
    tap_ref[slot, 0] = row.astype(jnp.float32)
    tap_ref[slot, 1] = high
    tap_ref[slot, 2] = weight - high


def slab_of(grid, first, slot, z_ref, tap_ref):
    half = grid // (2 * RADIX)
    piece = tap_ref.shape[3]
    rows16 = lax.broadcasted_iota(jnp.int32, (GROUP, piece), 0).astype(jnp.float32)
    spots = [(rows16 + float(at)).astype(jnp.bfloat16) for at in range(0, half, GROUP)]

    def wide(kind, residue):
        x = tap_ref[slot, kind, residue:residue + 1, :]
        return jnp.broadcast_to(x, (GROUP, piece)).astype(jnp.bfloat16)

    highs, lows = [], []
    for residue in (first, first + RADIX):
        row, high, low = (wide(kind, residue) for kind in range(3))
        zero = jnp.zeros_like(high)
        for spot in spots:
            hit = row == spot
            highs.append(jnp.where(hit, high, zero))
            lows.append(jnp.where(hit, low, zero))
    wh, wl = jnp.concatenate(highs, axis=0), jnp.concatenate(lows, axis=0)
    zh, zl = z_ref[slot, 0], z_ref[slot, 1]
    return dot(wh, zh) + dot(wh, zl) + dot(wl, zh)


def step_scratch(grid, both):
    bf16, f32 = jnp.bfloat16, jnp.float32
    piece = 2 * LANES
    return [
        pltpu.VMEM((2, 256, piece), bf16),
        pltpu.VMEM((2, 2 * (grid // FINE), piece), bf16),
        pltpu.VMEM((2, 2, piece, both), bf16),
        pltpu.VMEM((2, 3, 2 * RADIX, piece), f32),
    ]


def gather_kernel(
    split, base_count, tile_rows, grid, vis_hbm, tile_hbm, within_hbm, column_hbm, index_hbm, live_hbm,
    taps_hbm, out_ref, fine_ref, coarse_ref, taps_ref, h_ref,
    vis_ref, tile_ref, within_ref, column_ref, index_ref, live_ref, load_sems, send_sems, recv_sems,
    spread_ref, pick_ref, z_ref, tap_ref
):
    freq, base = lax.axis_index("freq"), lax.axis_index("base")
    part = lax.rem(freq, split)
    first = freq - part
    line = [{"freq": freq, "base": lax.rem(base + d, base_count)} for d in range(1, base_count)]
    mates = [{"freq": first + lax.rem(part + d, split), "base": base} for d in range(1, split)]
    barrier = greet(line + mates)
    loads = [
        pltpu.make_async_copy(a, b, load_sems.at[n])
        for n, (a, b) in enumerate([
            (vis_hbm, vis_ref), (tile_hbm, tile_ref), (within_hbm, within_ref), (column_hbm, column_ref),
            (index_hbm, index_ref), (live_hbm, live_ref), (taps_hbm, taps_ref),
        ])
    ]
    for load in loads:
        load.start()
    for load in loads:
        load.wait()
    channels, slots = within_ref.shape
    lane = lax.broadcasted_iota(jnp.int32, (1, slots), 1)
    for c in range(channels):
        is_live = lane < live_ref[0:1, c:c + 1]
        u = jnp.minimum(tile_ref[c] * tile_rows + within_ref[c:c + 1, :], grid - KW)
        fields = [
            jnp.where(is_live, vis_ref[0, c:c + 1, :], 0.0),
            jnp.where(is_live, vis_ref[1, c:c + 1, :], 0.0),
            u.astype(jnp.float32),
            column_ref[c:c + 1, :].astype(jnp.float32),
            jnp.where(is_live, index_ref[0, c:c + 1, :], -1).astype(jnp.float32),
            index_ref[1, c:c + 1, :].astype(jnp.float32),
        ]
        rows = [x[:, at:at + LANES] for x in fields for at in range(0, slots, LANES)]
        out_ref[part * channels + c, base] = jnp.concatenate(rows, axis=0)
    column_tables(grid, split, fine_ref, coarse_ref)
    pl.semaphore_wait(barrier, len(line) + len(mates))

    def block_copy(owner, peer, k):
        block = out_ref.at[pl.ds(part * channels, channels), owner]
        return pltpu.make_async_remote_copy(
            src_ref=block, dst_ref=block, send_sem=send_sems.at[k], recv_sem=recv_sems.at[k],
            device_id=peer, device_id_type=MESH,
        )

    sent = [block_copy(base, peer, k) for k, peer in enumerate(line)]
    for copy in sent:
        copy.start()
    passed = [[] for _ in mates]

    def pass_on(d):
        owner = lax.rem(base + base_count - d, base_count)
        for k, mate in enumerate(mates):
            copy = block_copy(owner, mate, len(line) + k * base_count + d)
            copy.start()
            passed[k].append(copy)

    pass_on(0)
    subs = slots // LANES
    table = taps_ref[...]
    for d in range(split):
        if d:
            passed[split - 1 - d][0].wait_recv()
        group = lax.rem(part + d, split) * channels

        def field_of(c):
            def field(number):
                rows = [out_ref[group + c, base, pl.ds(number * subs + n, 1), :] for n in range(2)]
                return jnp.concatenate(rows, axis=1)
            return field

        for c in range(channels):
            store_spread(grid, table, field_of(c), None, c % 2, spread_ref, pick_ref)
            store_z(grid, table, field_of(c), c % 2, fine_ref, coarse_ref, spread_ref, pick_ref, z_ref, tap_ref)
            for residue in range(RADIX):
                h_ref[group + c, residue] = slab_of(grid, residue, c % 2, z_ref, tap_ref)
    for d in range(1, base_count):
        sent[d - 1].wait_recv()
        pass_on(d)
    for k in range(len(mates)):
        for d, copy in enumerate(passed[k]):
            copy.wait_send()
            if d:
                copy.wait_recv()
    for copy in sent:
        copy.wait_send()


def gather_fields(split, base_count, tile_rows, grid, cols, *arrays):
    channels, slots = arrays[2].shape
    sems = base_count - 1 + (split - 1) * base_count
    total = channels * split
    f32, bf16 = jnp.float32, jnp.bfloat16
    vmem = pl.BlockSpec(memory_space=pltpu.VMEM)
    hbm = pl.BlockSpec(memory_space=pltpu.HBM)
    return pl.pallas_call(
        functools.partial(gather_kernel, split, base_count, tile_rows, grid),
        out_shape=(
            jax.ShapeDtypeStruct((total, base_count, FIELDS * (slots // LANES), LANES), f32),
            jax.ShapeDtypeStruct((2 * cols, 256), bf16),
            jax.ShapeDtypeStruct((2 * (grid // FINE), 2 * (grid // FINE)), bf16),
            jax.ShapeDtypeStruct(arrays[-1].shape, f32),
            jax.ShapeDtypeStruct((total, RADIX, grid // RADIX, 2 * cols), f32),
        ),
        in_specs=[hbm] * len(arrays),
        out_specs=(vmem,) * 5,
        scratch_shapes=[pltpu.VMEM(x.shape, x.dtype) for x in arrays[:-1]] + [
            pltpu.SemaphoreType.DMA((len(arrays),)),
            pltpu.SemaphoreType.DMA((sems,)), pltpu.SemaphoreType.DMA((sems,)),
        ] + step_scratch(grid, 2 * cols),
        compiler_params=pltpu.CompilerParams(
            collective_id=0, has_side_effects=True, vmem_limit_bytes=12 * 2**20
        ),
        name="gather_fields",
    )(*[in_hbm(x) for x in arrays])


def grid_kernel(
    grid, f_ref, fine_ref, coarse_ref, kernel_ref, start_ref, h_ref,
    spread_ref, pick_ref, z_ref, tap_ref, spot_ref, channel_ref
):
    channels, blocks, rows, _ = f_ref.shape
    subs = rows // FIELDS
    piece = 2 * LANES
    tap_table = kernel_ref[...]
    base = lax.axis_index("base")

    counts = []
    for c in range(channels):
        for b in range(blocks):
            used = f_ref[c, b, 4 * subs:5 * subs, :] >= 0.0
            counts.append(jnp.sum(jnp.where(used, 1.0, 0.0)))
    filled = jnp.int32(0)
    for c in range(channels):
        for b in range(blocks):
            done = jnp.where(base == b, 2, 0)
            for sub in range(subs):
                spot_ref[filled + sub] = b * subs + sub + done
            for ahead in range(subs // 2 + 1):
                channel_ref[lax.shift_right_logical(filled, jnp.int32(1)) + ahead] = c
            count = counts[c * blocks + b].astype(jnp.int32)
            live = lax.shift_right_logical(count + (LANES - 1), jnp.int32(LANES.bit_length() - 1))
            filled = filled + jnp.maximum(live - done, 0)
        spot_ref[filled] = -1
        filled = (filled + 1) & -2
    steps = lax.shift_right_logical(filled, jnp.int32(1))
    for ahead in range(8):
        spot_ref[filled + ahead] = -1
    for ahead in range(4):
        channel_ref[steps + ahead] = 0

    def field(step, number):
        c = channel_ref[step]
        one, two = jnp.maximum(spot_ref[2 * step], 0), jnp.maximum(spot_ref[2 * step + 1], 0)
        by = jnp.int32(subs.bit_length() - 1)
        return jnp.concatenate(
            [
                f_ref[c, lax.shift_right_logical(one, by), pl.ds(number * subs + (one & (subs - 1)), 1), :],
                f_ref[c, lax.shift_right_logical(two, by), pl.ds(number * subs + (two & (subs - 1)), 1), :],
            ],
            axis=1,
        )

    lane = lax.broadcasted_iota(jnp.int32, (1, piece), 1)

    def make_spread(step, slot):
        keep = lane < jnp.where(
            spot_ref[2 * step + 1] >= 0, piece, jnp.where(spot_ref[2 * step] >= 0, LANES, 0)
        )
        store_spread(grid, tap_table, lambda n: field(step, n), keep, slot, spread_ref, pick_ref)

    def make_z(step, slot):
        store_z(
            grid, tap_table, lambda n: field(step, n), slot,
            fine_ref, coarse_ref, spread_ref, pick_ref, z_ref, tap_ref,
        )

    def add_rows(step, slot):
        c = channel_ref[step]
        for first in range(RADIX):
            h_ref[c, first] += slab_of(grid, first, slot, z_ref, tap_ref)

    make_spread(0, 0)
    make_z(0, 0)
    make_spread(1, 1)

    def two_steps(n, carry):
        for slot in range(2):
            step = 2 * n + slot
            make_z(step + 1, 1 - slot)
            add_rows(step, slot)
            make_spread(step + 2, slot)
        return carry

    lax.fori_loop(0, (steps + 1) // 2, two_steps, 0)


def grid_visibilities(fields, fine, coarse, taps_table, start, grid):
    channels, blocks, rows, _ = fields.shape
    most = channels * (blocks * (rows // FIELDS) + 1)
    smem = lambda n: pltpu.SMEM((n,), jnp.int32)
    vmem = pl.BlockSpec(memory_space=pltpu.VMEM)
    return pl.pallas_call(
        functools.partial(grid_kernel, grid),
        out_shape=jax.ShapeDtypeStruct(start.shape, jnp.float32),
        in_specs=[vmem] * 5,
        out_specs=vmem,
        scratch_shapes=step_scratch(grid, start.shape[3]) + [smem(most + 16), smem(most // 2 + 16)],
        input_output_aliases={4: 0},
        compiler_params=pltpu.CompilerParams(vmem_limit_bytes=16 * 2**20),
        name="grid_visibilities",
    )(fields, fine, coarse, taps_table, start)


def power_kernel(
    grid, freq_count, base_count, split, scale, h_ref, dh_hbm, dl_hbm, bins_hbm, share_ref, spectrum_ref,
    dh_ref, dl_ref, bins_ref, load_sems, bins_sem, hh_ref, hl_ref, y_ref, power_ref, recv_ref, mask_ref, value_ref, low_ref, stage_ref, stage2_ref,
    send_sems, recv_sems, sum_send_sems, sum_recv_sems
):
    freq, base = lax.axis_index("freq"), lax.axis_index("base")
    ring = [{"freq": lax.rem(freq + d, freq_count), "base": base} for d in range(1, freq_count)]
    line = [{"freq": freq, "base": lax.rem(base + d, base_count)} for d in range(1, base_count)]
    barrier = greet(ring + line)
    loads = []
    for n in range(RADIX):
        loads.append(pltpu.make_async_copy(dh_hbm.at[n], dh_ref.at[n], load_sems.at[0, n]))
        loads.append(pltpu.make_async_copy(dl_hbm.at[n], dl_ref.at[n], load_sems.at[1, n]))
    for load in loads:
        load.start()
    rows_here = bins_ref.shape[1]
    if bins_hbm.shape[1] != rows_here:
        here = pl.ds(pl.multiple_of(freq * rows_here, rows_here), rows_here)
        load_bins = pltpu.make_async_copy(bins_hbm.at[:, here], bins_ref, bins_sem)
    else:
        load_bins = pltpu.make_async_copy(bins_hbm, bins_ref, bins_sem)
    load_bins.start()

    channels = h_ref.shape[0]
    slab = grid // RADIX
    share_rows, width = share_ref.shape
    cols = width // split
    chunk = min(64, share_rows)
    parts = share_rows // chunk
    shares = slab // share_rows

    def split_rows(n, carry):
        high, low = halves_of(h_ref[n // RADIX, n % RADIX])
        hh_ref[n // RADIX, n % RADIX] = high
        hl_ref[n // RADIX, n % RADIX] = low
        return carry

    lax.fori_loop(0, channels * RADIX, split_rows, 0)
    for load in loads:
        load.wait()

    def transform(n):
        top = pl.multiple_of((lax.rem(n, shares) * parts + n // shares) * chunk, chunk)
        for c in range(channels):
            for first in range(RADIX):
                dh = jnp.concatenate(
                    [dh_ref[first, pl.ds(top, chunk), :], dh_ref[first, pl.ds(slab + top, chunk), :]], axis=0
                )
                dl = jnp.concatenate(
                    [dl_ref[first, pl.ds(top, chunk), :], dl_ref[first, pl.ds(slab + top, chunk), :]], axis=0
                )
                hh, hl = hh_ref[c, first], hl_ref[c, first]
                y_ref[c % 2, first] = dot(dh, hh) + dot(dl, hh) + dot(dh, hl)
            step = min(16, chunk)
            for row in range(0, chunk, step):
                yr, yi = [], []
                for first in range(RADIX):
                    cy = y_ref[c % 2, first, row:row + step, :]
                    sy = y_ref[c % 2, first, chunk + row:chunk + row + step, :]
                    yr.append(cy[:, :cols] + sy[:, cols:])
                    yi.append(cy[:, cols:] - sy[:, :cols])
                ar, ai = yr[0] + yr[2], yi[0] + yi[2]
                br, bi = yr[0] - yr[2], yi[0] - yi[2]
                cr, ci = yr[1] + yr[3], yi[1] + yi[3]
                dr, di = yr[1] - yr[3], yi[1] - yi[3]
                outs = [
                    (ar + cr, ai + ci), (br + di, bi - dr), (ar - cr, ai - ci), (br - di, bi + dr)
                ]
                for k, (xr, xi) in enumerate(outs):
                    at = pl.ds(pl.multiple_of(k * slab + top + row, step), step)
                    value = (xr * xr + xi * xi) * scale
                    power_ref[at, :] = value if c == 0 else power_ref[at, :] + value

    def piece(n, k):
        share, part = lax.rem(n, shares), n // shares
        target = k * shares + share
        top = pl.multiple_of(target * share_rows + part * chunk, chunk)
        rows = pl.ds(pl.multiple_of(part * chunk, chunk), chunk)
        copy = pltpu.make_async_remote_copy(
            src_ref=power_ref.at[pl.ds(top, chunk), :],
            dst_ref=recv_ref.at[freq, rows, :],
            send_sem=send_sems.at[n, k], recv_sem=recv_sems.at[freq, part],
            device_id={"freq": target, "base": base}, device_id_type=MESH,
        )
        return target, top, rows, copy

    def send(n):
        for k in range(RADIX):
            target, top, rows, copy = piece(n, k)

            @pl.when(target == freq)
            def _():
                recv_ref[freq, rows, :] = power_ref[pl.ds(top, chunk), :]

            @pl.when(target != freq)
            def _():
                copy.start()

    transform(0)
    pl.semaphore_wait(barrier, len(ring) + len(line))
    send(0)

    def later(n, carry):
        transform(n)
        send(n)
        return carry

    lax.fori_loop(1, shares * parts, later, 0)

    high_count = NBINS // BIN_LOW
    lead = high_count // 4
    load_bins.wait()
    bins = bins_ref[...].T
    order = lax.broadcasted_iota(jnp.int32, (high_count, width), 0)
    order = lead * (order % lead) + order // lead if lead == 4 else order
    low_order = lax.broadcasted_iota(jnp.int32, (BIN_LOW, width), 0)
    for row in range(share_rows):
        at = slice(row * width, (row + 1) * width)
        bin_id = bins[row:row + 1, :]
        mask_ref[:, at] = jnp.where(order == bin_id // BIN_LOW, 1.0, 0.0).astype(jnp.bfloat16)
        low_ref[:, at] = jnp.where(low_order == bin_id % BIN_LOW, 1.0, 0.0).astype(jnp.bfloat16)
    counts = dot_rows(mask_ref[...], low_ref[...])

    totals = jnp.zeros((high_count, BIN_LOW), jnp.float32)
    for part in range(parts):
        rows = slice(part * chunk, (part + 1) * chunk)
        for d in range(1, freq_count):
            source = lax.rem(freq + d, freq_count)
            pltpu.make_async_remote_copy(
                src_ref=power_ref.at[0:chunk, :], dst_ref=recv_ref.at[source, rows, :],
                send_sem=send_sems.at[0, 0], recv_sem=recv_sems.at[source, part],
                device_id={"freq": source, "base": base}, device_id_type=MESH,
            ).wait_recv()
        for half in range(split):
            total = recv_ref[half, rows, :]
            for group in range(1, freq_count // split):
                total = total + recv_ref[group * split + half, rows, :]
            share_ref[rows, half * cols:(half + 1) * cols] = total
        for row in range(part * chunk, (part + 1) * chunk):
            at = slice(row * width, (row + 1) * width)
            out = slice((row - part * chunk) * width, (row - part * chunk + 1) * width)
            value = jnp.broadcast_to(share_ref[row:row + 1, :], (high_count, width))
            high, low = halves_of(value)
            mask = mask_ref[:, at]
            value_ref[0:high_count, out] = mask * high
            value_ref[high_count:, out] = mask * low
        span = slice(part * chunk * width, (part + 1) * chunk * width)
        sums = dot_rows(value_ref[...], low_ref[:, span])
        totals = totals + sums[:high_count] + sums[high_count:]

    def pack(x):
        return jnp.concatenate([x[lead * k:lead * (k + 1)] for k in range(4)], axis=1)

    stage_ref[freq] = jnp.concatenate([pack(totals), pack(counts)], axis=0)

    def share_out(ref, me, peers, offset):
        copies = []
        for k, peer in enumerate(peers):
            copy = pltpu.make_async_remote_copy(
                src_ref=ref.at[me], dst_ref=ref.at[me],
                send_sem=sum_send_sems.at[offset + k], recv_sem=sum_recv_sems.at[offset + k],
                device_id=peer, device_id_type=MESH,
            )
            copy.start()
            copies.append(copy)
        for copy in copies:
            copy.wait()
        total = ref[0]
        for other in range(1, ref.shape[0]):
            total = total + ref[other]
        return total

    stage2_ref[base] = share_out(stage_ref, freq, ring, 0)
    total = share_out(stage2_ref, base, line, len(ring))
    spectrum_ref[...] = total

    def finish(n, carry):
        for k in range(RADIX):
            target, _, _, copy = piece(n, k)

            @pl.when(target != freq)
            def _():
                copy.wait_send()
        return carry

    lax.fori_loop(0, shares * parts, finish, 0)


def power_and_spectrum(h, dh, dl, bins, grid, freq_count, base_count, split, width, scale):
    channels, _, slab, both = h.shape
    cols = both // 2
    share_rows = grid // freq_count
    chunk = min(64, share_rows)
    parts, shares = share_rows // chunk, slab // share_rows
    high_count = NBINS // BIN_LOW
    cells = share_rows * width
    sems = freq_count + base_count - 2
    f32, bf16 = jnp.float32, jnp.bfloat16
    vmem = pl.BlockSpec(memory_space=pltpu.VMEM)
    hbm = pl.BlockSpec(memory_space=pltpu.HBM)
    return pl.pallas_call(
        functools.partial(power_kernel, grid, freq_count, base_count, split, scale),
        out_shape=(
            jax.ShapeDtypeStruct((share_rows, width), f32),
            jax.ShapeDtypeStruct((8, 4 * BIN_LOW), f32),
        ),
        in_specs=[vmem, hbm, hbm, hbm],
        out_specs=(vmem, vmem),
        scratch_shapes=[
            pltpu.VMEM(dh.shape, bf16),
            pltpu.VMEM(dl.shape, bf16),
            pltpu.VMEM((bins.shape[0], share_rows), jnp.int32),
            pltpu.SemaphoreType.DMA((2, RADIX)),
            pltpu.SemaphoreType.DMA,
            pltpu.VMEM(h.shape, bf16),
            pltpu.VMEM(h.shape, bf16),
            pltpu.VMEM((2, RADIX, 2 * chunk, both), f32),
            pltpu.VMEM((grid, cols), f32),
            pltpu.VMEM((freq_count, share_rows, cols), f32),
            pltpu.VMEM((high_count, cells), bf16),
            pltpu.VMEM((2 * high_count, chunk * width), bf16),
            pltpu.VMEM((BIN_LOW, cells), bf16),
            pltpu.VMEM((freq_count, 8, 4 * BIN_LOW), f32),
            pltpu.VMEM((base_count, 8, 4 * BIN_LOW), f32),
            pltpu.SemaphoreType.DMA((shares * parts, RADIX)),
            pltpu.SemaphoreType.DMA((freq_count, parts)),
            pltpu.SemaphoreType.DMA((sems,)),
            pltpu.SemaphoreType.DMA((sems,)),
        ],
        compiler_params=pltpu.CompilerParams(
            collective_id=1, has_side_effects=True, vmem_limit_bytes=24 * 2**20
        ),
        name="power_and_spectrum",
    )(h, in_hbm(dh), in_hbm(dl), in_hbm(bins))


def finish_kernel(share_ref, sums_ref, power_ref, spectrum_ref):
    power_ref[...] = share_ref[...]
    mean = sums_ref[0:4, :] / sums_ref[4:8, :]
    width = mean.shape[1]
    for n in range(4):
        spectrum_ref[n * width:(n + 1) * width] = mean[n]


def finish(share, sums):
    vmem = pl.BlockSpec(memory_space=pltpu.VMEM)
    return pl.pallas_call(
        finish_kernel,
        out_shape=(
            jax.ShapeDtypeStruct(share.shape, share.dtype), jax.ShapeDtypeStruct((NBINS,), jnp.float32)
        ),
        in_specs=[vmem, vmem],
        out_specs=(vmem, vmem),
        compiler_params=pltpu.CompilerParams(vmem_limit_bytes=4 * 2**20),
        name="finish",
    )(share, sums)


def per_device(visibility, tile_of, u_within, v_cell, kernel_index, kernel, live_count, bin_map):
    base_count = lax.axis_size("base")
    freq_count = lax.axis_size("freq")
    grid = bin_map.shape[1]
    width = grid // base_count
    split = 2 if width % (2 * LANES) == 0 and freq_count % 2 == 0 else 1
    channels_here, slots = u_within.shape
    dh, dl = transform_tables(grid)
    scale = 1.0 / (channels_here * freq_count * slots * base_count)
    gathered = gather_fields(
        split, base_count, grid // base_count, grid, width // split,
        visibility, tile_of.transpose(0, 2, 1), u_within, v_cell, kernel_index, live_count.T, kernel.T,
    )
    h = grid_visibilities(*gathered, grid)
    share_rows = grid // freq_count
    bins = bin_map
    if share_rows % LANES:
        bins = lax.dynamic_slice_in_dim(bin_map, lax.axis_index("freq") * share_rows, share_rows, 1)
    share, sums = power_and_spectrum(
        h, jnp.asarray(dh), jnp.asarray(dl), bins, grid, freq_count, base_count, split, width, scale
    )
    return finish(share, sums)


def solution(mesh):
    in_specs = (
        P(None, "freq", "base"),
        P("freq", "base", None),
        P("freq", "base"),
        P("freq", "base"),
        P(None, "freq", "base"),
        P(),
        P("freq", "base"),
        P("base", None),
    )
    out_specs = (P("freq", "base"), P())
    return jax.shard_map(
        per_device, mesh=mesh, in_specs=in_specs, out_specs=out_specs, check_vma=False
    )
```

```python
import functools
import math

import jax
import jax.numpy as jnp
import numpy as np
from jax import lax
from jax.experimental import pallas as pl
from jax.experimental.pallas import tpu as pltpu
from jax.sharding import PartitionSpec as P

NBINS = 512
BIN_LOW = 32
KW = 8
FINE = 32
SPREAD = FINE + KW
RADIX = 4
GROUP = 16
FIELDS = 6
LANES = 128
MESH = pl.DeviceIdType.MESH


def halves_of(x):
    high = x.astype(jnp.bfloat16)
    low = (x - high.astype(jnp.float32)).astype(jnp.bfloat16)
    return high, low


@functools.lru_cache(None)
def transform_tables(grid):
    slab = grid // RADIX
    order = np.arange(slab)
    u = 2 * RADIX * (order % (slab // 2)) + RADIX * (order // (slab // 2))
    u = u[None, None, :] + np.arange(RADIX)[:, None, None]
    angle = ((np.arange(slab)[None, :, None] * u) % grid) * (2.0 * math.pi / grid)
    x = np.concatenate([np.cos(angle), np.sin(angle)], axis=1).astype(np.float32)
    high = x.astype(jnp.bfloat16)
    low = (x - high.astype(np.float32)).astype(jnp.bfloat16)
    return high, low


def dot(a, b):
    return jnp.dot(a, b, preferred_element_type=jnp.float32)


def dot_rows(a, b):
    return lax.dot_general(a, b, (((1,), (1,)), ((), ())), preferred_element_type=jnp.float32)


def in_hbm(x):
    return pltpu.with_memory_space_constraint(x, pltpu.HBM)


def greet(peers):
    barrier = pltpu.get_barrier_semaphore()
    for peer in peers:
        pl.semaphore_signal(barrier, inc=1, device_id=peer, device_id_type=MESH)
    return barrier


def phase(product, grid):
    half = grid // 2
    angle = ((product + half) & (grid - 1)) - half
    angle = angle.astype(jnp.float32) * (2.0 * math.pi / grid)
    return jnp.cos(angle), jnp.sin(angle)


def column_tables(grid, split, fine_ref, coarse_ref):
    cols = fine_ref.shape[0] // 2
    coarse_count = grid // FINE
    left = (lax.axis_index("base") * split + lax.rem(lax.axis_index("freq"), split)) * cols
    l = left + lax.broadcasted_iota(jnp.int32, (cols, SPREAD), 0)
    c, s = phase(l * lax.broadcasted_iota(jnp.int32, (cols, SPREAD), 1), grid)
    fine = jnp.concatenate(
        [jnp.concatenate([c, s], axis=1), jnp.concatenate([-s, c], axis=1)], axis=0
    )
    fh, fl = halves_of(fine)
    fine_ref[...] = jnp.zeros_like(fine_ref)
    fine_ref[:, 0:2 * SPREAD] = fh
    fine_ref[:, 2 * SPREAD:4 * SPREAD] = fl
    fine_ref[:, 4 * SPREAD:6 * SPREAD] = fh
    l = lax.broadcasted_iota(jnp.int32, (coarse_count, coarse_count), 0)
    c, s = phase(l * lax.broadcasted_iota(jnp.int32, (coarse_count, coarse_count), 1) * FINE, grid)
    ch, cl = halves_of(jnp.concatenate([c, -s], axis=0))
    coarse_ref[:, 0:coarse_count] = ch
    coarse_ref[:, coarse_count:] = cl


def look_up(table, row):
    row = jnp.maximum(row.astype(jnp.int32), 0)
    pieces = []
    for at in range(0, row.shape[1], LANES):
        index = jnp.broadcast_to(row[:, at:at + LANES], (KW, LANES))
        pieces.append(jnp.take_along_axis(table, index, axis=1))
    return jnp.concatenate(pieces, axis=1)


def store_spread(grid, table, field, keep, slot, spread_ref, pick_ref):
    re, im = field(0), field(1)
    if keep is not None:
        re, im = jnp.where(keep, re, 0.0), jnp.where(keep, im, 0.0)
    piece = re.shape[1]
    coarse_count = grid // FINE
    v = field(3).astype(jnp.int32)
    taps_v = look_up(table, field(5))
    offset = lax.broadcasted_iota(jnp.int32, (SPREAD, piece), 0) - (v & (FINE - 1))
    spread = jnp.zeros((SPREAD, piece), jnp.float32)
    for t in range(KW):
        spread = jnp.where(offset == t, taps_v[t:t + 1, :], spread)
    both = jnp.concatenate([spread * re, spread * im], axis=0)
    bh, bl = halves_of(both)
    pad = jnp.zeros((256 - 6 * SPREAD, piece), jnp.bfloat16)
    spread_ref[slot] = jnp.concatenate([bh, bh, bl, pad], axis=0)
    pick = lax.broadcasted_iota(jnp.int32, (2 * coarse_count, piece), 0) & (coarse_count - 1)
    pick_ref[slot] = jnp.where(pick == v // FINE, 1.0, 0.0).astype(jnp.bfloat16)


def store_z(grid, table, field, slot, fine_ref, coarse_ref, spread_ref, pick_ref, z_ref, tap_ref):
    cols = fine_ref.shape[0] // 2
    coarse_count = grid // FINE
    zb = dot(fine_ref[...], spread_ref[slot])
    e = dot(coarse_ref[...], pick_ref[slot])
    er, ei = e[:coarse_count], e[coarse_count:]
    re, im = [], []
    for at in range(0, cols, coarse_count):
        zr, zi = zb[at:at + coarse_count], zb[cols + at:cols + at + coarse_count]
        re.append(zr * er - zi * ei)
        im.append(zr * ei + zi * er)
    for n, parts in enumerate((re, im)):
        zh, zl = halves_of(jnp.concatenate(parts, axis=0).T)
        z_ref[slot, 0, :, n * cols:(n + 1) * cols] = zh
        z_ref[slot, 1, :, n * cols:(n + 1) * cols] = zl

    u = field(2).astype(jnp.int32)
    taps_u = look_up(table, field(4))
    residue = lax.broadcasted_iota(jnp.int32, (2 * RADIX, u.shape[1]), 0)
    tap = (residue - u) & (2 * RADIX - 1)
    row = lax.shift_right_logical(u + tap, jnp.int32((2 * RADIX).bit_length() - 1))
    weight = jnp.zeros(tap.shape, jnp.float32)
    for t in range(KW):
        weight = jnp.where(tap == t, taps_u[t:t + 1, :], weight)
    high = weight.astype(jnp.bfloat16).astype(jnp.float32)
    tap_ref[slot, 0] = row.astype(jnp.float32)
    tap_ref[slot, 1] = high
    tap_ref[slot, 2] = weight - high


def slab_of(grid, first, slot, z_ref, tap_ref):
    half = grid // (2 * RADIX)
    piece = tap_ref.shape[3]
    rows16 = lax.broadcasted_iota(jnp.int32, (GROUP, piece), 0).astype(jnp.float32)
    spots = [(rows16 + float(at)).astype(jnp.bfloat16) for at in range(0, half, GROUP)]

    def wide(kind, residue):
        x = tap_ref[slot, kind, residue:residue + 1, :]
        return jnp.broadcast_to(x, (GROUP, piece)).astype(jnp.bfloat16)

    highs, lows = [], []
    for residue in (first, first + RADIX):
        row, high, low = (wide(kind, residue) for kind in range(3))
        zero = jnp.zeros_like(high)
        for spot in spots:
            hit = row == spot
            highs.append(jnp.where(hit, high, zero))
            lows.append(jnp.where(hit, low, zero))
    wh, wl = jnp.concatenate(highs, axis=0), jnp.concatenate(lows, axis=0)
    zh, zl = z_ref[slot, 0], z_ref[slot, 1]
    return dot(wh, zh) + dot(wh, zl) + dot(wl, zh)


def step_scratch(grid, both):
    bf16, f32 = jnp.bfloat16, jnp.float32
    piece = 2 * LANES
    return [
        pltpu.VMEM((2, 256, piece), bf16),
        pltpu.VMEM((2, 2 * (grid // FINE), piece), bf16),
        pltpu.VMEM((2, 2, piece, both), bf16),
        pltpu.VMEM((2, 3, 2 * RADIX, piece), f32),
    ]


def second_pair(base, subs):
    if subs < 4:
        return lax.rem(base + lax.axis_size("base") - 1, lax.axis_size("base")), 0
    return jnp.maximum(base - 1, 0), jnp.where(base == 0, 2, 0)


def gather_kernel(
    split, base_count, tile_rows, grid, vis_hbm, tile_hbm, within_hbm, column_hbm, index_hbm, live_hbm,
    taps_hbm, out_ref, fine_ref, coarse_ref, taps_ref, h_ref,
    vis_ref, tile_ref, within_ref, column_ref, index_ref, live_ref, load_sems, send_sems, recv_sems,
    spread_ref, pick_ref, z_ref, tap_ref
):
    freq, base = lax.axis_index("freq"), lax.axis_index("base")
    part = lax.rem(freq, split)
    first = freq - part
    line = [{"freq": freq, "base": lax.rem(base + d, base_count)} for d in range(1, base_count)]
    mates = [{"freq": first + lax.rem(part + d, split), "base": base} for d in range(1, split)]
    barrier = greet(line + mates)
    loads = [
        pltpu.make_async_copy(a, b, load_sems.at[n])
        for n, (a, b) in enumerate([
            (vis_hbm, vis_ref), (tile_hbm, tile_ref), (within_hbm, within_ref), (column_hbm, column_ref),
            (index_hbm, index_ref), (live_hbm, live_ref), (taps_hbm, taps_ref),
        ])
    ]
    for load in loads:
        load.start()
    for load in loads:
        load.wait()
    channels, slots = within_ref.shape
    lane = lax.broadcasted_iota(jnp.int32, (1, slots), 1)
    for c in range(channels):
        is_live = lane < live_ref[0:1, c:c + 1]
        u = jnp.minimum(tile_ref[c] * tile_rows + within_ref[c:c + 1, :], grid - KW)
        fields = [
            jnp.where(is_live, vis_ref[0, c:c + 1, :], 0.0),
            jnp.where(is_live, vis_ref[1, c:c + 1, :], 0.0),
            u.astype(jnp.float32),
            column_ref[c:c + 1, :].astype(jnp.float32),
            jnp.where(is_live, index_ref[0, c:c + 1, :], -1).astype(jnp.float32),
            index_ref[1, c:c + 1, :].astype(jnp.float32),
        ]
        rows = [x[:, at:at + LANES] for x in fields for at in range(0, slots, LANES)]
        out_ref[part * channels + c, base] = jnp.concatenate(rows, axis=0)
    column_tables(grid, split, fine_ref, coarse_ref)
    pl.semaphore_wait(barrier, len(line) + len(mates))

    def block_copy(owner, peer, k):
        block = out_ref.at[pl.ds(part * channels, channels), owner]
        return pltpu.make_async_remote_copy(
            src_ref=block, dst_ref=block, send_sem=send_sems.at[k], recv_sem=recv_sems.at[k],
            device_id=peer, device_id_type=MESH,
        )

    sent = [block_copy(base, peer, k) for k, peer in enumerate(line)]
    for copy in sent:
        copy.start()
    passed = [[] for _ in mates]

    def pass_on(d):
        owner = lax.rem(base + base_count - d, base_count)
        for k, mate in enumerate(mates):
            copy = block_copy(owner, mate, len(line) + k * base_count + d)
            copy.start()
            passed[k].append(copy)

    pass_on(0)
    subs = slots // LANES
    table = taps_ref[...]

    def grid_group(d, owner, sub, begin):
        group = lax.rem(part + d, split) * channels

        def field_of(c):
            def field(number):
                rows = [out_ref[group + c, owner, pl.ds(number * subs + sub + n, 1), :] for n in range(2)]
                return jnp.concatenate(rows, axis=1)
            return field

        for c in range(channels):
            store_spread(grid, table, field_of(c), None, c % 2, spread_ref, pick_ref)
            store_z(grid, table, field_of(c), c % 2, fine_ref, coarse_ref, spread_ref, pick_ref, z_ref, tap_ref)
            for residue in range(RADIX):
                rows = slab_of(grid, residue, c % 2, z_ref, tap_ref)
                h_ref[group + c, residue] = rows if begin else h_ref[group + c, residue] + rows

    grid_group(0, base, 0, True)
    for d in range(1, split):
        passed[split - 1 - d][0].wait_recv()
        grid_group(d, base, 0, True)
    below, sub = second_pair(base, subs)
    for d in range(1, base_count):
        if d == base_count - 1 and d > 1:
            grid_group(0, below, sub, False)
        sent[d - 1].wait_recv()
        pass_on(d)
    if base_count < 3:
        grid_group(0, below, sub, False)
    for d in range(1, split):
        passed[split - 1 - d][1].wait_recv()
        grid_group(d, below, sub, False)
    for k in range(len(mates)):
        for d, copy in enumerate(passed[k]):
            copy.wait_send()
            if d > 1:
                copy.wait_recv()
    for copy in sent:
        copy.wait_send()


def gather_fields(split, base_count, tile_rows, grid, cols, *arrays):
    channels, slots = arrays[2].shape
    sems = base_count - 1 + (split - 1) * base_count
    total = channels * split
    f32, bf16 = jnp.float32, jnp.bfloat16
    vmem = pl.BlockSpec(memory_space=pltpu.VMEM)
    hbm = pl.BlockSpec(memory_space=pltpu.HBM)
    return pl.pallas_call(
        functools.partial(gather_kernel, split, base_count, tile_rows, grid),
        out_shape=(
            jax.ShapeDtypeStruct((total, base_count, FIELDS * (slots // LANES), LANES), f32),
            jax.ShapeDtypeStruct((2 * cols, 256), bf16),
            jax.ShapeDtypeStruct((2 * (grid // FINE), 2 * (grid // FINE)), bf16),
            jax.ShapeDtypeStruct(arrays[-1].shape, f32),
            jax.ShapeDtypeStruct((total, RADIX, grid // RADIX, 2 * cols), f32),
        ),
        in_specs=[hbm] * len(arrays),
        out_specs=(vmem,) * 5,
        scratch_shapes=[pltpu.VMEM(x.shape, x.dtype) for x in arrays[:-1]] + [
            pltpu.SemaphoreType.DMA((len(arrays),)),
            pltpu.SemaphoreType.DMA((sems,)), pltpu.SemaphoreType.DMA((sems,)),
        ] + step_scratch(grid, 2 * cols),
        compiler_params=pltpu.CompilerParams(
            collective_id=0, has_side_effects=True, vmem_limit_bytes=12 * 2**20
        ),
        name="gather_fields",
    )(*[in_hbm(x) for x in arrays])


def grid_kernel(
    grid, f_ref, fine_ref, coarse_ref, kernel_ref, start_ref, h_ref,
    spread_ref, pick_ref, z_ref, tap_ref, spot_ref, channel_ref
):
    channels, blocks, rows, _ = f_ref.shape
    subs = rows // FIELDS
    piece = 2 * LANES
    tap_table = kernel_ref[...]
    base = lax.axis_index("base")
    below, _ = second_pair(base, subs)

    counts = []
    for c in range(channels):
        for b in range(blocks):
            used = f_ref[c, b, 4 * subs:5 * subs, :] >= 0.0
            counts.append(jnp.sum(jnp.where(used, 1.0, 0.0)))
    filled = jnp.int32(0)
    for c in range(channels):
        for b in range(blocks):
            done = jnp.where(base == b, 2, 0) + jnp.where(below == b, 2, 0)
            for sub in range(subs):
                spot_ref[filled + sub] = b * subs + sub + done
            for ahead in range(subs // 2 + 1):
                channel_ref[lax.shift_right_logical(filled, jnp.int32(1)) + ahead] = c
            count = counts[c * blocks + b].astype(jnp.int32)
            live = lax.shift_right_logical(count + (LANES - 1), jnp.int32(LANES.bit_length() - 1))
            filled = filled + jnp.maximum(live - done, 0)
        spot_ref[filled] = -1
        filled = (filled + 1) & -2
    steps = lax.shift_right_logical(filled, jnp.int32(1))
    for ahead in range(8):
        spot_ref[filled + ahead] = -1
    for ahead in range(4):
        channel_ref[steps + ahead] = 0

    def field(step, number):
        c = channel_ref[step]
        one, two = jnp.maximum(spot_ref[2 * step], 0), jnp.maximum(spot_ref[2 * step + 1], 0)
        by = jnp.int32(subs.bit_length() - 1)
        return jnp.concatenate(
            [
                f_ref[c, lax.shift_right_logical(one, by), pl.ds(number * subs + (one & (subs - 1)), 1), :],
                f_ref[c, lax.shift_right_logical(two, by), pl.ds(number * subs + (two & (subs - 1)), 1), :],
            ],
            axis=1,
        )

    lane = lax.broadcasted_iota(jnp.int32, (1, piece), 1)

    def make_spread(step, slot):
        keep = lane < jnp.where(
            spot_ref[2 * step + 1] >= 0, piece, jnp.where(spot_ref[2 * step] >= 0, LANES, 0)
        )
        store_spread(grid, tap_table, lambda n: field(step, n), keep, slot, spread_ref, pick_ref)

    def make_z(step, slot):
        store_z(
            grid, tap_table, lambda n: field(step, n), slot,
            fine_ref, coarse_ref, spread_ref, pick_ref, z_ref, tap_ref,
        )

    def add_rows(step, slot):
        c = channel_ref[step]
        for first in range(RADIX):
            h_ref[c, first] += slab_of(grid, first, slot, z_ref, tap_ref)

    make_spread(0, 0)
    make_z(0, 0)
    make_spread(1, 1)

    def two_steps(n, carry):
        for slot in range(2):
            step = 2 * n + slot
            make_z(step + 1, 1 - slot)
            add_rows(step, slot)
            make_spread(step + 2, slot)
        return carry

    lax.fori_loop(0, (steps + 1) // 2, two_steps, 0)


def grid_visibilities(fields, fine, coarse, taps_table, start, grid):
    channels, blocks, rows, _ = fields.shape
    most = channels * (blocks * (rows // FIELDS) + 1)
    smem = lambda n: pltpu.SMEM((n,), jnp.int32)
    vmem = pl.BlockSpec(memory_space=pltpu.VMEM)
    return pl.pallas_call(
        functools.partial(grid_kernel, grid),
        out_shape=jax.ShapeDtypeStruct(start.shape, jnp.float32),
        in_specs=[vmem] * 5,
        out_specs=vmem,
        scratch_shapes=step_scratch(grid, start.shape[3]) + [smem(most + 16), smem(most // 2 + 16)],
        input_output_aliases={4: 0},
        compiler_params=pltpu.CompilerParams(vmem_limit_bytes=16 * 2**20),
        name="grid_visibilities",
    )(fields, fine, coarse, taps_table, start)


def power_kernel(
    grid, freq_count, base_count, split, scale, h_ref, dh_hbm, dl_hbm, bins_hbm, share_ref, spectrum_ref,
    dh_ref, dl_ref, bins_ref, load_sems, bins_sem, hh_ref, hl_ref, y_ref, power_ref, recv_ref, mask_ref, value_ref, low_ref, stage_ref, stage2_ref,
    send_sems, recv_sems, sum_send_sems, sum_recv_sems
):
    freq, base = lax.axis_index("freq"), lax.axis_index("base")
    ring = [{"freq": lax.rem(freq + d, freq_count), "base": base} for d in range(1, freq_count)]
    line = [{"freq": freq, "base": lax.rem(base + d, base_count)} for d in range(1, base_count)]
    barrier = greet(ring + line)
    loads = []
    for n in range(RADIX):
        loads.append(pltpu.make_async_copy(dh_hbm.at[n], dh_ref.at[n], load_sems.at[0, n]))
        loads.append(pltpu.make_async_copy(dl_hbm.at[n], dl_ref.at[n], load_sems.at[1, n]))
    for load in loads:
        load.start()
    rows_here = bins_ref.shape[1]
    if bins_hbm.shape[1] != rows_here:
        here = pl.ds(pl.multiple_of(freq * rows_here, rows_here), rows_here)
        load_bins = pltpu.make_async_copy(bins_hbm.at[:, here], bins_ref, bins_sem)
    else:
        load_bins = pltpu.make_async_copy(bins_hbm, bins_ref, bins_sem)
    load_bins.start()

    channels = h_ref.shape[0]
    slab = grid // RADIX
    share_rows, width = share_ref.shape
    cols = width // split
    chunk = min(64, share_rows)
    parts = share_rows // chunk
    shares = slab // share_rows

    def split_rows(n, carry):
        high, low = halves_of(h_ref[n // RADIX, n % RADIX])
        hh_ref[n // RADIX, n % RADIX] = high
        hl_ref[n // RADIX, n % RADIX] = low
        return carry

    lax.fori_loop(0, channels * RADIX, split_rows, 0)
    for load in loads:
        load.wait()

    def transform(n):
        top = pl.multiple_of((lax.rem(n, shares) * parts + n // shares) * chunk, chunk)
        for c in range(channels):
            for first in range(RADIX):
                dh = jnp.concatenate(
                    [dh_ref[first, pl.ds(top, chunk), :], dh_ref[first, pl.ds(slab + top, chunk), :]], axis=0
                )
                dl = jnp.concatenate(
                    [dl_ref[first, pl.ds(top, chunk), :], dl_ref[first, pl.ds(slab + top, chunk), :]], axis=0
                )
                hh, hl = hh_ref[c, first], hl_ref[c, first]
                y_ref[c % 2, first] = dot(dh, hh) + dot(dl, hh) + dot(dh, hl)
            step = min(16, chunk)
            for row in range(0, chunk, step):
                yr, yi = [], []
                for first in range(RADIX):
                    cy = y_ref[c % 2, first, row:row + step, :]
                    sy = y_ref[c % 2, first, chunk + row:chunk + row + step, :]
                    yr.append(cy[:, :cols] + sy[:, cols:])
                    yi.append(cy[:, cols:] - sy[:, :cols])
                ar, ai = yr[0] + yr[2], yi[0] + yi[2]
                br, bi = yr[0] - yr[2], yi[0] - yi[2]
                cr, ci = yr[1] + yr[3], yi[1] + yi[3]
                dr, di = yr[1] - yr[3], yi[1] - yi[3]
                outs = [
                    (ar + cr, ai + ci), (br + di, bi - dr), (ar - cr, ai - ci), (br - di, bi + dr)
                ]
                for k, (xr, xi) in enumerate(outs):
                    at = pl.ds(pl.multiple_of(k * slab + top + row, step), step)
                    value = (xr * xr + xi * xi) * scale
                    power_ref[at, :] = value if c == 0 else power_ref[at, :] + value

    def piece(n, k):
        share, part = lax.rem(n, shares), n // shares
        target = k * shares + share
        top = pl.multiple_of(target * share_rows + part * chunk, chunk)
        rows = pl.ds(pl.multiple_of(part * chunk, chunk), chunk)
        copy = pltpu.make_async_remote_copy(
            src_ref=power_ref.at[pl.ds(top, chunk), :],
            dst_ref=recv_ref.at[freq, rows, :],
            send_sem=send_sems.at[n, k], recv_sem=recv_sems.at[freq, part],
            device_id={"freq": target, "base": base}, device_id_type=MESH,
        )
        return target, top, rows, copy

    def send(n):
        for k in range(RADIX):
            target, top, rows, copy = piece(n, k)

            @pl.when(target == freq)
            def _():
                recv_ref[freq, rows, :] = power_ref[pl.ds(top, chunk), :]

            @pl.when(target != freq)
            def _():
                copy.start()

    transform(0)
    pl.semaphore_wait(barrier, len(ring) + len(line))
    send(0)

    def later(n, carry):
        transform(n)
        send(n)
        return carry

    lax.fori_loop(1, shares * parts, later, 0)

    high_count = NBINS // BIN_LOW
    lead = high_count // 4
    load_bins.wait()
    bins = bins_ref[...].T
    order = lax.broadcasted_iota(jnp.int32, (high_count, width), 0)
    order = lead * (order % lead) + order // lead if lead == 4 else order
    low_order = lax.broadcasted_iota(jnp.int32, (BIN_LOW, width), 0)
    for row in range(share_rows):
        at = slice(row * width, (row + 1) * width)
        bin_id = bins[row:row + 1, :]
        mask_ref[:, at] = jnp.where(order == bin_id // BIN_LOW, 1.0, 0.0).astype(jnp.bfloat16)
        low_ref[:, at] = jnp.where(low_order == bin_id % BIN_LOW, 1.0, 0.0).astype(jnp.bfloat16)
    counts = dot_rows(mask_ref[...], low_ref[...])

    totals = jnp.zeros((high_count, BIN_LOW), jnp.float32)
    for part in range(parts):
        rows = slice(part * chunk, (part + 1) * chunk)
        for d in range(1, freq_count):
            source = lax.rem(freq + d, freq_count)
            pltpu.make_async_remote_copy(
                src_ref=power_ref.at[0:chunk, :], dst_ref=recv_ref.at[source, rows, :],
                send_sem=send_sems.at[0, 0], recv_sem=recv_sems.at[source, part],
                device_id={"freq": source, "base": base}, device_id_type=MESH,
            ).wait_recv()
        for half in range(split):
            total = recv_ref[half, rows, :]
            for group in range(1, freq_count // split):
                total = total + recv_ref[group * split + half, rows, :]
            share_ref[rows, half * cols:(half + 1) * cols] = total
        for row in range(part * chunk, (part + 1) * chunk):
            at = slice(row * width, (row + 1) * width)
            out = slice((row - part * chunk) * width, (row - part * chunk + 1) * width)
            value = jnp.broadcast_to(share_ref[row:row + 1, :], (high_count, width))
            high, low = halves_of(value)
            mask = mask_ref[:, at]
            value_ref[0:high_count, out] = mask * high
            value_ref[high_count:, out] = mask * low
        span = slice(part * chunk * width, (part + 1) * chunk * width)
        sums = dot_rows(value_ref[...], low_ref[:, span])
        totals = totals + sums[:high_count] + sums[high_count:]

    def pack(x):
        return jnp.concatenate([x[lead * k:lead * (k + 1)] for k in range(4)], axis=1)

    stage_ref[freq] = jnp.concatenate([pack(totals), pack(counts)], axis=0)

    def share_out(ref, me, peers, offset):
        copies = []
        for k, peer in enumerate(peers):
            copy = pltpu.make_async_remote_copy(
                src_ref=ref.at[me], dst_ref=ref.at[me],
                send_sem=sum_send_sems.at[offset + k], recv_sem=sum_recv_sems.at[offset + k],
                device_id=peer, device_id_type=MESH,
            )
            copy.start()
            copies.append(copy)
        for copy in copies:
            copy.wait()
        total = ref[0]
        for other in range(1, ref.shape[0]):
            total = total + ref[other]
        return total

    stage2_ref[base] = share_out(stage_ref, freq, ring, 0)
    total = share_out(stage2_ref, base, line, len(ring))
    spectrum_ref[...] = total

    def finish(n, carry):
        for k in range(RADIX):
            target, _, _, copy = piece(n, k)

            @pl.when(target != freq)
            def _():
                copy.wait_send()
        return carry

    lax.fori_loop(0, shares * parts, finish, 0)


def power_and_spectrum(h, dh, dl, bins, grid, freq_count, base_count, split, width, scale):
    channels, _, slab, both = h.shape
    cols = both // 2
    share_rows = grid // freq_count
    chunk = min(64, share_rows)
    parts, shares = share_rows // chunk, slab // share_rows
    high_count = NBINS // BIN_LOW
    cells = share_rows * width
    sems = freq_count + base_count - 2
    f32, bf16 = jnp.float32, jnp.bfloat16
    vmem = pl.BlockSpec(memory_space=pltpu.VMEM)
    hbm = pl.BlockSpec(memory_space=pltpu.HBM)
    return pl.pallas_call(
        functools.partial(power_kernel, grid, freq_count, base_count, split, scale),
        out_shape=(
            jax.ShapeDtypeStruct((share_rows, width), f32),
            jax.ShapeDtypeStruct((8, 4 * BIN_LOW), f32),
        ),
        in_specs=[vmem, hbm, hbm, hbm],
        out_specs=(vmem, vmem),
        scratch_shapes=[
            pltpu.VMEM(dh.shape, bf16),
            pltpu.VMEM(dl.shape, bf16),
            pltpu.VMEM((bins.shape[0], share_rows), jnp.int32),
            pltpu.SemaphoreType.DMA((2, RADIX)),
            pltpu.SemaphoreType.DMA,
            pltpu.VMEM(h.shape, bf16),
            pltpu.VMEM(h.shape, bf16),
            pltpu.VMEM((2, RADIX, 2 * chunk, both), f32),
            pltpu.VMEM((grid, cols), f32),
            pltpu.VMEM((freq_count, share_rows, cols), f32),
            pltpu.VMEM((high_count, cells), bf16),
            pltpu.VMEM((2 * high_count, chunk * width), bf16),
            pltpu.VMEM((BIN_LOW, cells), bf16),
            pltpu.VMEM((freq_count, 8, 4 * BIN_LOW), f32),
            pltpu.VMEM((base_count, 8, 4 * BIN_LOW), f32),
            pltpu.SemaphoreType.DMA((shares * parts, RADIX)),
            pltpu.SemaphoreType.DMA((freq_count, parts)),
            pltpu.SemaphoreType.DMA((sems,)),
            pltpu.SemaphoreType.DMA((sems,)),
        ],
        compiler_params=pltpu.CompilerParams(
            collective_id=1, has_side_effects=True, vmem_limit_bytes=24 * 2**20
        ),
        name="power_and_spectrum",
    )(h, in_hbm(dh), in_hbm(dl), in_hbm(bins))


def finish_kernel(share_ref, sums_ref, power_ref, spectrum_ref):
    power_ref[...] = share_ref[...]
    mean = sums_ref[0:4, :] / sums_ref[4:8, :]
    width = mean.shape[1]
    for n in range(4):
        spectrum_ref[n * width:(n + 1) * width] = mean[n]


def finish(share, sums):
    vmem = pl.BlockSpec(memory_space=pltpu.VMEM)
    return pl.pallas_call(
        finish_kernel,
        out_shape=(
            jax.ShapeDtypeStruct(share.shape, share.dtype), jax.ShapeDtypeStruct((NBINS,), jnp.float32)
        ),
        in_specs=[vmem, vmem],
        out_specs=(vmem, vmem),
        compiler_params=pltpu.CompilerParams(vmem_limit_bytes=4 * 2**20),
        name="finish",
    )(share, sums)


def per_device(visibility, tile_of, u_within, v_cell, kernel_index, kernel, live_count, bin_map):
    base_count = lax.axis_size("base")
    freq_count = lax.axis_size("freq")
    grid = bin_map.shape[1]
    width = grid // base_count
    split = 2 if width % (2 * LANES) == 0 and freq_count % 2 == 0 else 1
    channels_here, slots = u_within.shape
    dh, dl = transform_tables(grid)
    scale = 1.0 / (channels_here * freq_count * slots * base_count)
    gathered = gather_fields(
        split, base_count, grid // base_count, grid, width // split,
        visibility, tile_of.transpose(0, 2, 1), u_within, v_cell, kernel_index, live_count.T, kernel.T,
    )
    h = grid_visibilities(*gathered, grid)
    share_rows = grid // freq_count
    bins = bin_map
    if share_rows % LANES:
        bins = lax.dynamic_slice_in_dim(bin_map, lax.axis_index("freq") * share_rows, share_rows, 1)
    share, sums = power_and_spectrum(
        h, jnp.asarray(dh), jnp.asarray(dl), bins, grid, freq_count, base_count, split, width, scale
    )
    return finish(share, sums)


def solution(mesh):
    in_specs = (
        P(None, "freq", "base"),
        P("freq", "base", None),
        P("freq", "base"),
        P("freq", "base"),
        P(None, "freq", "base"),
        P(),
        P("freq", "base"),
        P("base", None),
    )
    out_specs = (P("freq", "base"), P())
    return jax.shard_map(
        per_device, mesh=mesh, in_specs=in_specs, out_specs=out_specs, check_vma=False
    )
```

```python
import functools
import math

import jax
import jax.numpy as jnp
import numpy as np
from jax import lax
from jax.experimental import pallas as pl
from jax.experimental.pallas import tpu as pltpu
from jax.sharding import PartitionSpec as P

NBINS = 512
BIN_LOW = 32
KW = 8
FINE = 32
SPREAD = FINE + KW
RADIX = 4
GROUP = 16
FIELDS = 6
LANES = 128
F8 = jnp.float8_e5m2
Z_SCALE = 2.0 ** 9
W_SCALE = 2.0 ** 12
MESH = pl.DeviceIdType.MESH


def halves_of(x):
    high = x.astype(jnp.bfloat16)
    low = (x - high.astype(jnp.float32)).astype(jnp.bfloat16)
    return high, low


@functools.lru_cache(None)
def transform_tables(grid):
    slab = grid // RADIX
    order = np.arange(slab)
    u = 2 * RADIX * (order % (slab // 2)) + RADIX * (order // (slab // 2))
    u = u[None, None, :] + np.arange(RADIX)[:, None, None]
    angle = ((np.arange(slab)[None, :, None] * u) % grid) * (2.0 * math.pi / grid)
    x = np.concatenate([np.cos(angle), np.sin(angle)], axis=1).astype(np.float32)
    high = x.astype(jnp.bfloat16)
    low = (x - high.astype(np.float32)).astype(jnp.bfloat16)
    return high, low


def dot(a, b):
    return jnp.dot(a, b, preferred_element_type=jnp.float32)


def dot_rows(a, b):
    return lax.dot_general(a, b, (((1,), (1,)), ((), ())), preferred_element_type=jnp.float32)


def in_hbm(x):
    return pltpu.with_memory_space_constraint(x, pltpu.HBM)


def greet(peers):
    barrier = pltpu.get_barrier_semaphore()
    for peer in peers:
        pl.semaphore_signal(barrier, inc=1, device_id=peer, device_id_type=MESH)
    return barrier


def phase(product, grid):
    half = grid // 2
    angle = ((product + half) & (grid - 1)) - half
    angle = angle.astype(jnp.float32) * (2.0 * math.pi / grid)
    return jnp.cos(angle), jnp.sin(angle)


def column_tables(grid, split, fine_ref, coarse_ref):
    cols = fine_ref.shape[0] // 2
    coarse_count = grid // FINE
    left = (lax.axis_index("base") * split + lax.rem(lax.axis_index("freq"), split)) * cols
    l = left + lax.broadcasted_iota(jnp.int32, (cols, SPREAD), 0)
    c, s = phase(l * lax.broadcasted_iota(jnp.int32, (cols, SPREAD), 1), grid)
    fine = jnp.concatenate(
        [jnp.concatenate([c, s], axis=1), jnp.concatenate([-s, c], axis=1)], axis=0
    )
    fh, fl = halves_of(fine)
    fine_ref[...] = jnp.zeros_like(fine_ref)
    fine_ref[:, 0:2 * SPREAD] = fh
    fine_ref[:, 2 * SPREAD:4 * SPREAD] = fl
    fine_ref[:, 4 * SPREAD:6 * SPREAD] = fh
    l = lax.broadcasted_iota(jnp.int32, (coarse_count, coarse_count), 0)
    c, s = phase(l * lax.broadcasted_iota(jnp.int32, (coarse_count, coarse_count), 1) * FINE, grid)
    ch, cl = halves_of(jnp.concatenate([c, -s], axis=0))
    coarse_ref[:, 0:coarse_count] = ch
    coarse_ref[:, coarse_count:] = cl


def look_up(table, row):
    row = jnp.maximum(row.astype(jnp.int32), 0)
    pieces = []
    for at in range(0, row.shape[1], LANES):
        index = jnp.broadcast_to(row[:, at:at + LANES], (KW, LANES))
        pieces.append(jnp.take_along_axis(table, index, axis=1))
    return jnp.concatenate(pieces, axis=1)


def store_spread(grid, table, field, keep, slot, spread_ref, pick_ref):
    re, im = field(0), field(1)
    if keep is not None:
        re, im = jnp.where(keep, re, 0.0), jnp.where(keep, im, 0.0)
    piece = re.shape[1]
    coarse_count = grid // FINE
    v = field(3).astype(jnp.int32)
    taps_v = look_up(table, field(5))
    offset = lax.broadcasted_iota(jnp.int32, (SPREAD, piece), 0) - (v & (FINE - 1))
    spread = jnp.zeros((SPREAD, piece), jnp.float32)
    for t in range(KW):
        spread = jnp.where(offset == t, taps_v[t:t + 1, :], spread)
    re, im = re * Z_SCALE, im * Z_SCALE
    both = jnp.concatenate([spread * re, spread * im], axis=0)
    bh, bl = halves_of(both)
    pad = jnp.zeros((256 - 6 * SPREAD, piece), jnp.bfloat16)
    spread_ref[slot] = jnp.concatenate([bh, bh, bl, pad], axis=0)
    pick = lax.broadcasted_iota(jnp.int32, (2 * coarse_count, piece), 0) & (coarse_count - 1)
    pick_ref[slot] = jnp.where(pick == v // FINE, 1.0, 0.0).astype(jnp.bfloat16)


def store_z(grid, table, field, slot, fine_ref, coarse_ref, spread_ref, pick_ref, z_ref, z8_ref, tap_ref):
    cols = fine_ref.shape[0] // 2
    coarse_count = grid // FINE
    zb = dot(fine_ref[...], spread_ref[slot])
    e = dot(coarse_ref[...], pick_ref[slot])
    er, ei = e[:coarse_count], e[coarse_count:]
    re, im = [], []
    for at in range(0, cols, coarse_count):
        zr, zi = zb[at:at + coarse_count], zb[cols + at:cols + at + coarse_count]
        re.append(zr * er - zi * ei)
        im.append(zr * ei + zi * er)
    for n, parts in enumerate((re, im)):
        turned = jnp.concatenate(parts, axis=0).T
        zh, zl = halves_of(turned)
        z_ref[slot, 0, :, n * cols:(n + 1) * cols] = zh
        z_ref[slot, 1, :, n * cols:(n + 1) * cols] = zl
        z8_ref[slot, :, n * cols:(n + 1) * cols] = turned.astype(F8)

    u = field(2).astype(jnp.int32)
    taps_u = look_up(table, field(4))
    residue = lax.broadcasted_iota(jnp.int32, (2 * RADIX, u.shape[1]), 0)
    tap = (residue - u) & (2 * RADIX - 1)
    row = lax.shift_right_logical(u + tap, jnp.int32((2 * RADIX).bit_length() - 1))
    weight = jnp.zeros(tap.shape, jnp.float32)
    for t in range(KW):
        weight = jnp.where(tap == t, taps_u[t:t + 1, :], weight)
    weight = weight * W_SCALE
    high = weight.astype(jnp.bfloat16).astype(jnp.float32)
    tap_ref[slot, 0] = row.astype(jnp.float32)
    tap_ref[slot, 1] = high
    tap_ref[slot, 2] = weight - high


def slab_of(grid, first, slot, z_ref, z8_ref, tap_ref):
    half = grid // (2 * RADIX)
    piece = tap_ref.shape[3]
    rows16 = lax.broadcasted_iota(jnp.int32, (GROUP, piece), 0).astype(jnp.float32)
    spots = [(rows16 + float(at)).astype(jnp.bfloat16) for at in range(0, half, GROUP)]

    def wide(kind, residue):
        x = tap_ref[slot, kind, residue:residue + 1, :]
        return jnp.broadcast_to(x, (GROUP, piece)).astype(jnp.bfloat16)

    highs, lows = [], []
    for residue in (first, first + RADIX):
        row, high, low = (wide(kind, residue) for kind in range(3))
        zero = jnp.zeros_like(high)
        for spot in spots:
            hit = row == spot
            highs.append(jnp.where(hit, high, zero))
            lows.append(jnp.where(hit, low, zero))
    wh, wl = jnp.concatenate(highs, axis=0), jnp.concatenate(lows, axis=0)
    zh, zl = z_ref[slot, 0], z_ref[slot, 1]
    return dot(wh, zh) + dot(wh, zl) + dot(wl.astype(F8), z8_ref[slot])


def step_scratch(grid, both):
    bf16, f32 = jnp.bfloat16, jnp.float32
    piece = 2 * LANES
    return [
        pltpu.VMEM((2, 256, piece), bf16),
        pltpu.VMEM((2, 2 * (grid // FINE), piece), bf16),
        pltpu.VMEM((2, 2, piece, both), bf16),
        pltpu.VMEM((2, piece, both), F8),
        pltpu.VMEM((2, 3, 2 * RADIX, piece), f32),
    ]


def second_pair(base, subs):
    if subs < 4:
        return lax.rem(base + lax.axis_size("base") - 1, lax.axis_size("base")), 0
    return jnp.maximum(base - 1, 0), jnp.where(base == 0, 2, 0)


def gather_kernel(
    split, base_count, tile_rows, grid, vis_hbm, tile_hbm, within_hbm, column_hbm, index_hbm, live_hbm,
    taps_hbm, out_ref, fine_ref, coarse_ref, taps_ref, h_ref,
    vis_ref, tile_ref, within_ref, column_ref, index_ref, live_ref, load_sems, send_sems, recv_sems,
    spread_ref, pick_ref, z_ref, z8_ref, tap_ref
):
    freq, base = lax.axis_index("freq"), lax.axis_index("base")
    part = lax.rem(freq, split)
    first = freq - part
    line = [{"freq": freq, "base": lax.rem(base + d, base_count)} for d in range(1, base_count)]
    mates = [{"freq": first + lax.rem(part + d, split), "base": base} for d in range(1, split)]
    barrier = greet(line + mates)
    loads = [
        pltpu.make_async_copy(a, b, load_sems.at[n])
        for n, (a, b) in enumerate([
            (vis_hbm, vis_ref), (tile_hbm, tile_ref), (within_hbm, within_ref), (column_hbm, column_ref),
            (index_hbm, index_ref), (live_hbm, live_ref), (taps_hbm, taps_ref),
        ])
    ]
    for load in loads:
        load.start()
    for load in loads:
        load.wait()
    channels, slots = within_ref.shape
    lane = lax.broadcasted_iota(jnp.int32, (1, slots), 1)
    for c in range(channels):
        is_live = lane < live_ref[0:1, c:c + 1]
        u = jnp.minimum(tile_ref[c] * tile_rows + within_ref[c:c + 1, :], grid - KW)
        fields = [
            jnp.where(is_live, vis_ref[0, c:c + 1, :], 0.0),
            jnp.where(is_live, vis_ref[1, c:c + 1, :], 0.0),
            u.astype(jnp.float32),
            column_ref[c:c + 1, :].astype(jnp.float32),
            jnp.where(is_live, index_ref[0, c:c + 1, :], -1).astype(jnp.float32),
            index_ref[1, c:c + 1, :].astype(jnp.float32),
        ]
        rows = [x[:, at:at + LANES] for x in fields for at in range(0, slots, LANES)]
        out_ref[part * channels + c, base] = jnp.concatenate(rows, axis=0)
    column_tables(grid, split, fine_ref, coarse_ref)
    pl.semaphore_wait(barrier, len(line) + len(mates))

    def block_copy(owner, peer, k):
        block = out_ref.at[pl.ds(part * channels, channels), owner]
        return pltpu.make_async_remote_copy(
            src_ref=block, dst_ref=block, send_sem=send_sems.at[k], recv_sem=recv_sems.at[k],
            device_id=peer, device_id_type=MESH,
        )

    sent = [block_copy(base, peer, k) for k, peer in enumerate(line)]
    for copy in sent:
        copy.start()
    passed = [[] for _ in mates]

    def pass_on(d):
        owner = lax.rem(base + base_count - d, base_count)
        for k, mate in enumerate(mates):
            copy = block_copy(owner, mate, len(line) + k * base_count + d)
            copy.start()
            passed[k].append(copy)

    pass_on(0)
    subs = slots // LANES
    table = taps_ref[...]

    def grid_group(d, owner, sub, begin):
        group = lax.rem(part + d, split) * channels

        def field_of(c):
            def field(number):
                rows = [out_ref[group + c, owner, pl.ds(number * subs + sub + n, 1), :] for n in range(2)]
                return jnp.concatenate(rows, axis=1)
            return field

        for c in range(channels):
            store_spread(grid, table, field_of(c), None, c % 2, spread_ref, pick_ref)
            store_z(grid, table, field_of(c), c % 2, fine_ref, coarse_ref, spread_ref, pick_ref, z_ref, z8_ref, tap_ref)
            for residue in range(RADIX):
                rows = slab_of(grid, residue, c % 2, z_ref, z8_ref, tap_ref)
                h_ref[group + c, residue] = rows if begin else h_ref[group + c, residue] + rows

    grid_group(0, base, 0, True)
    for d in range(1, split):
        passed[split - 1 - d][0].wait_recv()
        grid_group(d, base, 0, True)
    below, sub = second_pair(base, subs)
    for d in range(1, base_count):
        if d == base_count - 1 and d > 1:
            grid_group(0, below, sub, False)
        sent[d - 1].wait_recv()
        pass_on(d)
    if base_count < 3:
        grid_group(0, below, sub, False)
    for d in range(1, split):
        passed[split - 1 - d][1].wait_recv()
        grid_group(d, below, sub, False)
    for k in range(len(mates)):
        for d, copy in enumerate(passed[k]):
            copy.wait_send()
            if d > 1:
                copy.wait_recv()
    for copy in sent:
        copy.wait_send()


def gather_fields(split, base_count, tile_rows, grid, cols, *arrays):
    channels, slots = arrays[2].shape
    sems = base_count - 1 + (split - 1) * base_count
    total = channels * split
    f32, bf16 = jnp.float32, jnp.bfloat16
    vmem = pl.BlockSpec(memory_space=pltpu.VMEM)
    hbm = pl.BlockSpec(memory_space=pltpu.HBM)
    return pl.pallas_call(
        functools.partial(gather_kernel, split, base_count, tile_rows, grid),
        out_shape=(
            jax.ShapeDtypeStruct((total, base_count, FIELDS * (slots // LANES), LANES), f32),
            jax.ShapeDtypeStruct((2 * cols, 256), bf16),
            jax.ShapeDtypeStruct((2 * (grid // FINE), 2 * (grid // FINE)), bf16),
            jax.ShapeDtypeStruct(arrays[-1].shape, f32),
            jax.ShapeDtypeStruct((total, RADIX, grid // RADIX, 2 * cols), f32),
        ),
        in_specs=[hbm] * len(arrays),
        out_specs=(vmem,) * 5,
        scratch_shapes=[pltpu.VMEM(x.shape, x.dtype) for x in arrays[:-1]] + [
            pltpu.SemaphoreType.DMA((len(arrays),)),
            pltpu.SemaphoreType.DMA((sems,)), pltpu.SemaphoreType.DMA((sems,)),
        ] + step_scratch(grid, 2 * cols),
        compiler_params=pltpu.CompilerParams(
            collective_id=0, has_side_effects=True, vmem_limit_bytes=12 * 2**20
        ),
        name="gather_fields",
    )(*[in_hbm(x) for x in arrays])


def grid_kernel(
    grid, f_ref, fine_ref, coarse_ref, kernel_ref, start_ref, dh_hbm, dl_hbm, h_ref, dh_ref, dl_ref,
    spread_ref, pick_ref, z_ref, z8_ref, tap_ref, spot_ref, channel_ref, load_sems
):
    loads = []
    for n in range(RADIX):
        loads.append(pltpu.make_async_copy(dh_hbm.at[n], dh_ref.at[n], load_sems.at[0, n]))
        loads.append(pltpu.make_async_copy(dl_hbm.at[n], dl_ref.at[n], load_sems.at[1, n]))
    for load in loads:
        load.start()
    channels, blocks, rows, _ = f_ref.shape
    subs = rows // FIELDS
    piece = 2 * LANES
    tap_table = kernel_ref[...]
    base = lax.axis_index("base")
    below, _ = second_pair(base, subs)

    counts = []
    for c in range(channels):
        for b in range(blocks):
            used = f_ref[c, b, 4 * subs:5 * subs, :] >= 0.0
            counts.append(jnp.sum(jnp.where(used, 1.0, 0.0)))
    filled = jnp.int32(0)
    for c in range(channels):
        for b in range(blocks):
            done = jnp.where(base == b, 2, 0) + jnp.where(below == b, 2, 0)
            for sub in range(subs):
                spot_ref[filled + sub] = b * subs + sub + done
            for ahead in range(subs // 2 + 1):
                channel_ref[lax.shift_right_logical(filled, jnp.int32(1)) + ahead] = c
            count = counts[c * blocks + b].astype(jnp.int32)
            live = lax.shift_right_logical(count + (LANES - 1), jnp.int32(LANES.bit_length() - 1))
            filled = filled + jnp.maximum(live - done, 0)
        spot_ref[filled] = -1
        filled = (filled + 1) & -2
    steps = lax.shift_right_logical(filled, jnp.int32(1))
    for ahead in range(8):
        spot_ref[filled + ahead] = -1
    for ahead in range(4):
        channel_ref[steps + ahead] = 0

    def field(step, number):
        c = channel_ref[step]
        one, two = jnp.maximum(spot_ref[2 * step], 0), jnp.maximum(spot_ref[2 * step + 1], 0)
        by = jnp.int32(subs.bit_length() - 1)
        return jnp.concatenate(
            [
                f_ref[c, lax.shift_right_logical(one, by), pl.ds(number * subs + (one & (subs - 1)), 1), :],
                f_ref[c, lax.shift_right_logical(two, by), pl.ds(number * subs + (two & (subs - 1)), 1), :],
            ],
            axis=1,
        )

    lane = lax.broadcasted_iota(jnp.int32, (1, piece), 1)

    def make_spread(step, slot):
        keep = lane < jnp.where(
            spot_ref[2 * step + 1] >= 0, piece, jnp.where(spot_ref[2 * step] >= 0, LANES, 0)
        )
        store_spread(grid, tap_table, lambda n: field(step, n), keep, slot, spread_ref, pick_ref)

    def make_z(step, slot):
        store_z(
            grid, tap_table, lambda n: field(step, n), slot,
            fine_ref, coarse_ref, spread_ref, pick_ref, z_ref, z8_ref, tap_ref,
        )

    def add_rows(step, slot):
        c = channel_ref[step]
        for first in range(RADIX):
            h_ref[c, first] += slab_of(grid, first, slot, z_ref, z8_ref, tap_ref)

    make_spread(0, 0)
    make_z(0, 0)
    make_spread(1, 1)

    def two_steps(n, carry):
        for slot in range(2):
            step = 2 * n + slot
            make_z(step + 1, 1 - slot)
            make_spread(step + 2, slot)
            add_rows(step, slot)
        return carry

    lax.fori_loop(0, (steps + 1) // 2, two_steps, 0)
    for load in loads:
        load.wait()


def grid_visibilities(fields, fine, coarse, taps_table, start, dh, dl, grid):
    channels, blocks, rows, _ = fields.shape
    most = channels * (blocks * (rows // FIELDS) + 1)
    smem = lambda n: pltpu.SMEM((n,), jnp.int32)
    vmem = pl.BlockSpec(memory_space=pltpu.VMEM)
    hbm = pl.BlockSpec(memory_space=pltpu.HBM)
    return pl.pallas_call(
        functools.partial(grid_kernel, grid),
        out_shape=(
            jax.ShapeDtypeStruct(start.shape, jnp.float32),
            jax.ShapeDtypeStruct(dh.shape, jnp.bfloat16),
            jax.ShapeDtypeStruct(dl.shape, jnp.bfloat16),
        ),
        in_specs=[vmem] * 5 + [hbm] * 2,
        out_specs=(vmem,) * 3,
        scratch_shapes=step_scratch(grid, start.shape[3]) + [
            smem(most + 16), smem(most // 2 + 16), pltpu.SemaphoreType.DMA((2, RADIX)),
        ],
        input_output_aliases={4: 0},
        compiler_params=pltpu.CompilerParams(vmem_limit_bytes=16 * 2**20),
        name="grid_visibilities",
    )(fields, fine, coarse, taps_table, start, in_hbm(dh), in_hbm(dl))


def power_kernel(
    grid, freq_count, base_count, split, scale, h_ref, dh_ref, dl_ref, bins_hbm, share_ref, spectrum_ref,
    bins_ref, bins_sem, hh_ref, hl_ref, y_ref, power_ref, recv_ref, mask_ref, value_ref, low_ref, stage_ref, stage2_ref,
    send_sems, recv_sems, sum_send_sems, sum_recv_sems
):
    freq, base = lax.axis_index("freq"), lax.axis_index("base")
    ring = [{"freq": lax.rem(freq + d, freq_count), "base": base} for d in range(1, freq_count)]
    line = [{"freq": freq, "base": lax.rem(base + d, base_count)} for d in range(1, base_count)]
    barrier = greet(ring + line)
    rows_here = bins_ref.shape[1]
    if bins_hbm.shape[1] != rows_here:
        here = pl.ds(pl.multiple_of(freq * rows_here, rows_here), rows_here)
        load_bins = pltpu.make_async_copy(bins_hbm.at[:, here], bins_ref, bins_sem)
    else:
        load_bins = pltpu.make_async_copy(bins_hbm, bins_ref, bins_sem)
    load_bins.start()

    channels = h_ref.shape[0]
    slab = grid // RADIX
    share_rows, width = share_ref.shape
    cols = width // split
    chunk = min(64, share_rows)
    parts = share_rows // chunk
    shares = slab // share_rows

    def transform(n, begin=False):
        top = pl.multiple_of((lax.rem(n, shares) * parts + n // shares) * chunk, chunk)
        for c in range(channels):
            for first in range(RADIX):
                dh = jnp.concatenate(
                    [dh_ref[first, pl.ds(top, chunk), :], dh_ref[first, pl.ds(slab + top, chunk), :]], axis=0
                )
                dl = jnp.concatenate(
                    [dl_ref[first, pl.ds(top, chunk), :], dl_ref[first, pl.ds(slab + top, chunk), :]], axis=0
                )
                if begin:
                    hh, hl = halves_of(h_ref[c, first])
                    hh_ref[c, first] = hh
                    hl_ref[c, first] = hl
                else:
                    hh, hl = hh_ref[c, first], hl_ref[c, first]
                y_ref[c % 2, first] = dot(dh, hh) + dot(dl, hh) + dot(dh, hl)
            step = min(16, chunk)
            for row in range(0, chunk, step):
                yr, yi = [], []
                for first in range(RADIX):
                    cy = y_ref[c % 2, first, row:row + step, :]
                    sy = y_ref[c % 2, first, chunk + row:chunk + row + step, :]
                    yr.append(cy[:, :cols] + sy[:, cols:])
                    yi.append(cy[:, cols:] - sy[:, :cols])
                ar, ai = yr[0] + yr[2], yi[0] + yi[2]
                br, bi = yr[0] - yr[2], yi[0] - yi[2]
                cr, ci = yr[1] + yr[3], yi[1] + yi[3]
                dr, di = yr[1] - yr[3], yi[1] - yi[3]
                outs = [
                    (ar + cr, ai + ci), (br + di, bi - dr), (ar - cr, ai - ci), (br - di, bi + dr)
                ]
                for k, (xr, xi) in enumerate(outs):
                    at = pl.ds(pl.multiple_of(k * slab + top + row, step), step)
                    value = (xr * xr + xi * xi) * scale
                    power_ref[at, :] = value if c == 0 else power_ref[at, :] + value

    def piece(n, k):
        share, part = lax.rem(n, shares), n // shares
        target = k * shares + share
        top = pl.multiple_of(target * share_rows + part * chunk, chunk)
        rows = pl.ds(pl.multiple_of(part * chunk, chunk), chunk)
        copy = pltpu.make_async_remote_copy(
            src_ref=power_ref.at[pl.ds(top, chunk), :],
            dst_ref=recv_ref.at[freq, rows, :],
            send_sem=send_sems.at[n, k], recv_sem=recv_sems.at[freq, part],
            device_id={"freq": target, "base": base}, device_id_type=MESH,
        )
        return target, top, rows, copy

    def send(n):
        for k in range(RADIX):
            target, top, rows, copy = piece(n, k)

            @pl.when(target == freq)
            def _():
                recv_ref[freq, rows, :] = power_ref[pl.ds(top, chunk), :]

            @pl.when(target != freq)
            def _():
                copy.start()

    transform(0, True)
    pl.semaphore_wait(barrier, len(ring) + len(line))
    send(0)

    def later(n, carry):
        transform(n)
        send(n)
        return carry

    lax.fori_loop(1, shares * parts, later, 0)

    high_count = NBINS // BIN_LOW
    lead = high_count // 4
    load_bins.wait()
    bins = bins_ref[...].T
    order = lax.broadcasted_iota(jnp.int32, (high_count, width), 0)
    order = lead * (order % lead) + order // lead if lead == 4 else order
    low_order = lax.broadcasted_iota(jnp.int32, (BIN_LOW, width), 0)
    for row in range(share_rows):
        at = slice(row * width, (row + 1) * width)
        bin_id = bins[row:row + 1, :]
        mask_ref[:, at] = jnp.where(order == bin_id // BIN_LOW, 1.0, 0.0).astype(jnp.bfloat16)
        low_ref[:, at] = jnp.where(low_order == bin_id % BIN_LOW, 1.0, 0.0).astype(jnp.bfloat16)
    counts = dot_rows(mask_ref[...], low_ref[...])

    totals = jnp.zeros((high_count, BIN_LOW), jnp.float32)
    for part in range(parts):
        rows = slice(part * chunk, (part + 1) * chunk)
        for d in range(1, freq_count):
            source = lax.rem(freq + d, freq_count)
            pltpu.make_async_remote_copy(
                src_ref=power_ref.at[0:chunk, :], dst_ref=recv_ref.at[source, rows, :],
                send_sem=send_sems.at[0, 0], recv_sem=recv_sems.at[source, part],
                device_id={"freq": source, "base": base}, device_id_type=MESH,
            ).wait_recv()
        for half in range(split):
            total = recv_ref[half, rows, :]
            for group in range(1, freq_count // split):
                total = total + recv_ref[group * split + half, rows, :]
            share_ref[rows, half * cols:(half + 1) * cols] = total
        for row in range(part * chunk, (part + 1) * chunk):
            at = slice(row * width, (row + 1) * width)
            out = slice((row - part * chunk) * width, (row - part * chunk + 1) * width)
            value = jnp.broadcast_to(share_ref[row:row + 1, :], (high_count, width))
            high, low = halves_of(value)
            mask = mask_ref[:, at]
            value_ref[0:high_count, out] = mask * high
            value_ref[high_count:, out] = mask * low
        span = slice(part * chunk * width, (part + 1) * chunk * width)
        sums = dot_rows(value_ref[...], low_ref[:, span])
        totals = totals + sums[:high_count] + sums[high_count:]

    def pack(x):
        return jnp.concatenate([x[lead * k:lead * (k + 1)] for k in range(4)], axis=1)

    stage_ref[freq] = jnp.concatenate([pack(totals), pack(counts)], axis=0)

    def share_out(ref, me, peers, offset):
        copies = []
        for k, peer in enumerate(peers):
            copy = pltpu.make_async_remote_copy(
                src_ref=ref.at[me], dst_ref=ref.at[me],
                send_sem=sum_send_sems.at[offset + k], recv_sem=sum_recv_sems.at[offset + k],
                device_id=peer, device_id_type=MESH,
            )
            copy.start()
            copies.append(copy)
        for copy in copies:
            copy.wait()
        total = ref[0]
        for other in range(1, ref.shape[0]):
            total = total + ref[other]
        return total

    stage2_ref[base] = share_out(stage_ref, freq, ring, 0)
    total = share_out(stage2_ref, base, line, len(ring))
    spectrum_ref[...] = total

    def finish(n, carry):
        for k in range(RADIX):
            target, _, _, copy = piece(n, k)

            @pl.when(target != freq)
            def _():
                copy.wait_send()
        return carry

    lax.fori_loop(0, shares * parts, finish, 0)


def power_and_spectrum(h, dh, dl, bins, grid, freq_count, base_count, split, width, scale):
    channels, _, slab, both = h.shape
    cols = both // 2
    share_rows = grid // freq_count
    chunk = min(64, share_rows)
    parts, shares = share_rows // chunk, slab // share_rows
    high_count = NBINS // BIN_LOW
    cells = share_rows * width
    sems = freq_count + base_count - 2
    f32, bf16 = jnp.float32, jnp.bfloat16
    vmem = pl.BlockSpec(memory_space=pltpu.VMEM)
    hbm = pl.BlockSpec(memory_space=pltpu.HBM)
    return pl.pallas_call(
        functools.partial(power_kernel, grid, freq_count, base_count, split, scale),
        out_shape=(
            jax.ShapeDtypeStruct((share_rows, width), f32),
            jax.ShapeDtypeStruct((8, 4 * BIN_LOW), f32),
        ),
        in_specs=[vmem, vmem, vmem, hbm],
        out_specs=(vmem, vmem),
        scratch_shapes=[
            pltpu.VMEM((bins.shape[0], share_rows), jnp.int32),
            pltpu.SemaphoreType.DMA,
            pltpu.VMEM(h.shape, bf16),
            pltpu.VMEM(h.shape, bf16),
            pltpu.VMEM((2, RADIX, 2 * chunk, both), f32),
            pltpu.VMEM((grid, cols), f32),
            pltpu.VMEM((freq_count, share_rows, cols), f32),
            pltpu.VMEM((high_count, cells), bf16),
            pltpu.VMEM((2 * high_count, chunk * width), bf16),
            pltpu.VMEM((BIN_LOW, cells), bf16),
            pltpu.VMEM((freq_count, 8, 4 * BIN_LOW), f32),
            pltpu.VMEM((base_count, 8, 4 * BIN_LOW), f32),
            pltpu.SemaphoreType.DMA((shares * parts, RADIX)),
            pltpu.SemaphoreType.DMA((freq_count, parts)),
            pltpu.SemaphoreType.DMA((sems,)),
            pltpu.SemaphoreType.DMA((sems,)),
        ],
        compiler_params=pltpu.CompilerParams(
            collective_id=1, has_side_effects=True, vmem_limit_bytes=24 * 2**20
        ),
        name="power_and_spectrum",
    )(h, dh, dl, in_hbm(bins))


def finish_kernel(share_ref, sums_ref, power_ref, spectrum_ref):
    power_ref[...] = share_ref[...]
    mean = sums_ref[0:4, :] / sums_ref[4:8, :]
    width = mean.shape[1]
    for n in range(4):
        spectrum_ref[n * width:(n + 1) * width] = mean[n]


def finish(share, sums):
    vmem = pl.BlockSpec(memory_space=pltpu.VMEM)
    return pl.pallas_call(
        finish_kernel,
        out_shape=(
            jax.ShapeDtypeStruct(share.shape, share.dtype), jax.ShapeDtypeStruct((NBINS,), jnp.float32)
        ),
        in_specs=[vmem, vmem],
        out_specs=(vmem, vmem),
        compiler_params=pltpu.CompilerParams(vmem_limit_bytes=4 * 2**20),
        name="finish",
    )(share, sums)


def per_device(visibility, tile_of, u_within, v_cell, kernel_index, kernel, live_count, bin_map):
    base_count = lax.axis_size("base")
    freq_count = lax.axis_size("freq")
    grid = bin_map.shape[1]
    width = grid // base_count
    split = 2 if width % (2 * LANES) == 0 and freq_count % 2 == 0 else 1
    channels_here, slots = u_within.shape
    dh, dl = transform_tables(grid)
    scale = 1.0 / (channels_here * freq_count * slots * base_count) / (Z_SCALE * W_SCALE) ** 2
    gathered = gather_fields(
        split, base_count, grid // base_count, grid, width // split,
        visibility, tile_of.transpose(0, 2, 1), u_within, v_cell, kernel_index, live_count.T, kernel.T,
    )
    h, dh, dl = grid_visibilities(*gathered, jnp.asarray(dh), jnp.asarray(dl), grid)
    share_rows = grid // freq_count
    bins = bin_map
    if share_rows % LANES:
        bins = lax.dynamic_slice_in_dim(bin_map, lax.axis_index("freq") * share_rows, share_rows, 1)
    share, sums = power_and_spectrum(
        h, dh, dl, bins, grid, freq_count, base_count, split, width, scale
    )
    return finish(share, sums)


def solution(mesh):
    in_specs = (
        P(None, "freq", "base"),
        P("freq", "base", None),
        P("freq", "base"),
        P("freq", "base"),
        P(None, "freq", "base"),
        P(),
        P("freq", "base"),
        P("base", None),
    )
    out_specs = (P("freq", "base"), P())
    return jax.shard_map(
        per_device, mesh=mesh, in_specs=in_specs, out_specs=out_specs, check_vma=False
    )
```

```python
import functools
import math

import jax
import jax.numpy as jnp
import numpy as np
from jax import lax
from jax.experimental import pallas as pl
from jax.experimental.pallas import tpu as pltpu
from jax.sharding import PartitionSpec as P

NBINS = 512
BIN_LOW = 32
KW = 8
FINE = 32
SPREAD = FINE + KW
RADIX = 4
GROUP = 16
FIELDS = 6
LANES = 128
F8 = jnp.float8_e5m2
F8W = jnp.float8_e4m3fn
Z_SCALE = 2.0 ** 9
W_SCALE = 2.0 ** 12
LIFT = 2.0 ** 9
MESH = pl.DeviceIdType.MESH


def halves_of(x):
    high = x.astype(jnp.bfloat16)
    low = (x - high.astype(jnp.float32)).astype(jnp.bfloat16)
    return high, low


@functools.lru_cache(None)
def transform_tables(grid):
    slab = grid // RADIX
    order = np.arange(slab)
    u = 2 * RADIX * (order % (slab // 2)) + RADIX * (order // (slab // 2))
    u = u[None, None, :] + np.arange(RADIX)[:, None, None]
    angle = ((np.arange(slab)[None, :, None] * u) % grid) * (2.0 * math.pi / grid)
    x = np.concatenate([np.cos(angle), np.sin(angle)], axis=1).astype(np.float32)
    high = x.astype(jnp.bfloat16)
    low = (x - high.astype(np.float32)).astype(jnp.bfloat16)
    return high, low


def dot(a, b):
    return jnp.dot(a, b, preferred_element_type=jnp.float32)


def dot_rows(a, b):
    return lax.dot_general(a, b, (((1,), (1,)), ((), ())), preferred_element_type=jnp.float32)


def in_hbm(x):
    return pltpu.with_memory_space_constraint(x, pltpu.HBM)


def greet(peers):
    barrier = pltpu.get_barrier_semaphore()
    for peer in peers:
        pl.semaphore_signal(barrier, inc=1, device_id=peer, device_id_type=MESH)
    return barrier


def phase(product, grid):
    half = grid // 2
    angle = ((product + half) & (grid - 1)) - half
    angle = angle.astype(jnp.float32) * (2.0 * math.pi / grid)
    return jnp.cos(angle), jnp.sin(angle)


def column_tables(grid, split, fine_ref, coarse_ref):
    cols = fine_ref.shape[0] // 2
    coarse_count = grid // FINE
    left = (lax.axis_index("base") * split + lax.rem(lax.axis_index("freq"), split)) * cols
    l = left + lax.broadcasted_iota(jnp.int32, (cols, SPREAD), 0)
    c, s = phase(l * lax.broadcasted_iota(jnp.int32, (cols, SPREAD), 1), grid)
    fine = jnp.concatenate(
        [jnp.concatenate([c, s], axis=1), jnp.concatenate([-s, c], axis=1)], axis=0
    )
    fh, fl = halves_of(fine)
    fine_ref[...] = jnp.zeros_like(fine_ref)
    fine_ref[:, 0:2 * SPREAD] = fh
    fine_ref[:, 2 * SPREAD:4 * SPREAD] = fl
    fine_ref[:, 4 * SPREAD:6 * SPREAD] = fh
    l = lax.broadcasted_iota(jnp.int32, (coarse_count, coarse_count), 0)
    c, s = phase(l * lax.broadcasted_iota(jnp.int32, (coarse_count, coarse_count), 1) * FINE, grid)
    ch, cl = halves_of(jnp.concatenate([c, -s], axis=0))
    coarse_ref[:, 0:coarse_count] = ch
    coarse_ref[:, coarse_count:] = cl


def look_up(table, row):
    row = jnp.maximum(row.astype(jnp.int32), 0)
    pieces = []
    for at in range(0, row.shape[1], LANES):
        index = jnp.broadcast_to(row[:, at:at + LANES], (KW, LANES))
        pieces.append(jnp.take_along_axis(table, index, axis=1))
    return jnp.concatenate(pieces, axis=1)


def store_spread(grid, table, field, keep, slot, spread_ref, pick_ref):
    re, im = field(0), field(1)
    if keep is not None:
        re, im = jnp.where(keep, re, 0.0), jnp.where(keep, im, 0.0)
    piece = re.shape[1]
    coarse_count = grid // FINE
    v = field(3).astype(jnp.int32)
    taps_v = look_up(table, field(5))
    offset = lax.broadcasted_iota(jnp.int32, (SPREAD, piece), 0) - (v & (FINE - 1))
    spread = jnp.zeros((SPREAD, piece), jnp.float32)
    for t in range(KW):
        spread = jnp.where(offset == t, taps_v[t:t + 1, :], spread)
    re, im = re * Z_SCALE, im * Z_SCALE
    both = jnp.concatenate([spread * re, spread * im], axis=0)
    bh, bl = halves_of(both)
    pad = jnp.zeros((256 - 6 * SPREAD, piece), jnp.bfloat16)
    spread_ref[slot] = jnp.concatenate([bh, bh, bl, pad], axis=0)
    pick = lax.broadcasted_iota(jnp.int32, (2 * coarse_count, piece), 0) & (coarse_count - 1)
    pick_ref[slot] = jnp.where(pick == v // FINE, 1.0, 0.0).astype(jnp.bfloat16)


def store_z(grid, table, field, slot, fine_ref, coarse_ref, spread_ref, pick_ref, z_ref, z8_ref, tap_ref):
    cols = fine_ref.shape[0] // 2
    coarse_count = grid // FINE
    piece = z_ref.shape[1]
    zb = dot(fine_ref[...], spread_ref[slot])
    e = dot(coarse_ref[...], pick_ref[slot])
    er, ei = e[:coarse_count], e[coarse_count:]
    re, im = [], []
    for at in range(0, cols, coarse_count):
        zr, zi = zb[at:at + coarse_count], zb[cols + at:cols + at + coarse_count]
        re.append(zr * er - zi * ei)
        im.append(zr * ei + zi * er)
    for n, parts in enumerate((re, im)):
        turned = jnp.concatenate(parts, axis=0).T
        zh = turned.astype(jnp.bfloat16)
        zl = turned - zh.astype(jnp.float32)
        z_ref[slot, :, n * cols:(n + 1) * cols] = zh
        z8_ref[slot, 0:piece, n * cols:(n + 1) * cols] = turned.astype(F8)
        z8_ref[slot, piece:, n * cols:(n + 1) * cols] = (zl * LIFT).astype(F8)

    u = field(2).astype(jnp.int32)
    taps_u = look_up(table, field(4))
    residue = lax.broadcasted_iota(jnp.int32, (2 * RADIX, u.shape[1]), 0)
    tap = (residue - u) & (2 * RADIX - 1)
    row = lax.shift_right_logical(u + tap, jnp.int32((2 * RADIX).bit_length() - 1))
    weight = jnp.zeros(tap.shape, jnp.float32)
    for t in range(KW):
        weight = jnp.where(tap == t, taps_u[t:t + 1, :], weight)
    weight = weight * W_SCALE
    high = weight.astype(jnp.bfloat16).astype(jnp.float32)
    tap_ref[slot, 0] = row.astype(jnp.float32)
    tap_ref[slot, 1] = high
    tap_ref[slot, 2] = weight - high
    tap_ref[slot, 3] = high * (1.0 / LIFT)


def slab_of(grid, first, slot, z_ref, z8_ref, tap_ref):
    half = grid // (2 * RADIX)
    piece = tap_ref.shape[3]
    rows16 = lax.broadcasted_iota(jnp.int32, (GROUP, piece), 0).astype(jnp.float32)
    spots = [(rows16 + float(at)).astype(jnp.bfloat16) for at in range(0, half, GROUP)]

    def wide(kind, residue):
        x = tap_ref[slot, kind, residue:residue + 1, :]
        return jnp.broadcast_to(x, (GROUP, piece)).astype(jnp.bfloat16)

    highs, lows, shifts = [], [], []
    for residue in (first, first + RADIX):
        row, high, low, shift = (wide(kind, residue) for kind in range(4))
        zero = jnp.zeros_like(high)
        for spot in spots:
            hit = row == spot
            highs.append(jnp.where(hit, high, zero))
            lows.append(jnp.where(hit, low, zero))
            shifts.append(jnp.where(hit, shift, zero))
    wh = jnp.concatenate(highs, axis=0)
    small = [jnp.concatenate(x, axis=0).astype(F8W) for x in (lows, shifts)]
    return dot(wh, z_ref[slot]) + dot(jnp.concatenate(small, axis=1), z8_ref[slot])


def step_scratch(grid, both):
    bf16, f32 = jnp.bfloat16, jnp.float32
    piece = 2 * LANES
    return [
        pltpu.VMEM((2, 256, piece), bf16),
        pltpu.VMEM((2, 2 * (grid // FINE), piece), bf16),
        pltpu.VMEM((2, piece, both), bf16),
        pltpu.VMEM((2, 2 * piece, both), F8),
        pltpu.VMEM((2, 4, 2 * RADIX, piece), f32),
    ]


def second_pair(base, subs):
    if subs < 4:
        return lax.rem(base + lax.axis_size("base") - 1, lax.axis_size("base")), 0
    return jnp.maximum(base - 1, 0), jnp.where(base == 0, 2, 0)


def gather_kernel(
    split, base_count, tile_rows, grid, vis_hbm, tile_hbm, within_hbm, column_hbm, index_hbm, live_hbm,
    taps_hbm, out_ref, fine_ref, coarse_ref, taps_ref, h_ref,
    vis_ref, tile_ref, within_ref, column_ref, index_ref, live_ref, load_sems, send_sems, recv_sems,
    spread_ref, pick_ref, z_ref, z8_ref, tap_ref
):
    freq, base = lax.axis_index("freq"), lax.axis_index("base")
    part = lax.rem(freq, split)
    first = freq - part
    line = [{"freq": freq, "base": lax.rem(base + d, base_count)} for d in range(1, base_count)]
    mates = [{"freq": first + lax.rem(part + d, split), "base": base} for d in range(1, split)]
    barrier = greet(line + mates)
    loads = [
        pltpu.make_async_copy(a, b, load_sems.at[n])
        for n, (a, b) in enumerate([
            (vis_hbm, vis_ref), (tile_hbm, tile_ref), (within_hbm, within_ref), (column_hbm, column_ref),
            (index_hbm, index_ref), (live_hbm, live_ref), (taps_hbm, taps_ref),
        ])
    ]
    for load in loads:
        load.start()
    for load in loads:
        load.wait()
    channels, slots = within_ref.shape
    lane = lax.broadcasted_iota(jnp.int32, (1, slots), 1)
    for c in range(channels):
        is_live = lane < live_ref[0:1, c:c + 1]
        u = jnp.minimum(tile_ref[c] * tile_rows + within_ref[c:c + 1, :], grid - KW)
        fields = [
            jnp.where(is_live, vis_ref[0, c:c + 1, :], 0.0),
            jnp.where(is_live, vis_ref[1, c:c + 1, :], 0.0),
            u.astype(jnp.float32),
            column_ref[c:c + 1, :].astype(jnp.float32),
            jnp.where(is_live, index_ref[0, c:c + 1, :], -1).astype(jnp.float32),
            index_ref[1, c:c + 1, :].astype(jnp.float32),
        ]
        rows = [x[:, at:at + LANES] for x in fields for at in range(0, slots, LANES)]
        out_ref[part * channels + c, base] = jnp.concatenate(rows, axis=0)
    column_tables(grid, split, fine_ref, coarse_ref)
    pl.semaphore_wait(barrier, len(line) + len(mates))

    def block_copy(owner, peer, k):
        block = out_ref.at[pl.ds(part * channels, channels), owner]
        return pltpu.make_async_remote_copy(
            src_ref=block, dst_ref=block, send_sem=send_sems.at[k], recv_sem=recv_sems.at[k],
            device_id=peer, device_id_type=MESH,
        )

    sent = [block_copy(base, peer, k) for k, peer in enumerate(line)]
    for copy in sent:
        copy.start()
    passed = [[] for _ in mates]

    def pass_on(d):
        owner = lax.rem(base + base_count - d, base_count)
        for k, mate in enumerate(mates):
            copy = block_copy(owner, mate, len(line) + k * base_count + d)
            copy.start()
            passed[k].append(copy)

    pass_on(0)
    subs = slots // LANES
    table = taps_ref[...]

    def grid_group(d, owner, sub, begin):
        group = lax.rem(part + d, split) * channels

        def field_of(c):
            def field(number):
                rows = [out_ref[group + c, owner, pl.ds(number * subs + sub + n, 1), :] for n in range(2)]
                return jnp.concatenate(rows, axis=1)
            return field

        for c in range(channels):
            store_spread(grid, table, field_of(c), None, c % 2, spread_ref, pick_ref)
            store_z(grid, table, field_of(c), c % 2, fine_ref, coarse_ref, spread_ref, pick_ref, z_ref, z8_ref, tap_ref)
            for residue in range(RADIX):
                rows = slab_of(grid, residue, c % 2, z_ref, z8_ref, tap_ref)
                h_ref[group + c, residue] = rows if begin else h_ref[group + c, residue] + rows

    grid_group(0, base, 0, True)
    for d in range(1, split):
        passed[split - 1 - d][0].wait_recv()
        grid_group(d, base, 0, True)
    below, sub = second_pair(base, subs)
    for d in range(1, base_count):
        if d == base_count - 1 and d > 1:
            grid_group(0, below, sub, False)
        sent[d - 1].wait_recv()
        pass_on(d)
    if base_count < 3:
        grid_group(0, below, sub, False)
    for d in range(1, split):
        passed[split - 1 - d][1].wait_recv()
        grid_group(d, below, sub, False)
    for k in range(len(mates)):
        for d, copy in enumerate(passed[k]):
            copy.wait_send()
            if d > 1:
                copy.wait_recv()
    for copy in sent:
        copy.wait_send()


def gather_fields(split, base_count, tile_rows, grid, cols, *arrays):
    channels, slots = arrays[2].shape
    sems = base_count - 1 + (split - 1) * base_count
    total = channels * split
    f32, bf16 = jnp.float32, jnp.bfloat16
    vmem = pl.BlockSpec(memory_space=pltpu.VMEM)
    hbm = pl.BlockSpec(memory_space=pltpu.HBM)
    return pl.pallas_call(
        functools.partial(gather_kernel, split, base_count, tile_rows, grid),
        out_shape=(
            jax.ShapeDtypeStruct((total, base_count, FIELDS * (slots // LANES), LANES), f32),
            jax.ShapeDtypeStruct((2 * cols, 256), bf16),
            jax.ShapeDtypeStruct((2 * (grid // FINE), 2 * (grid // FINE)), bf16),
            jax.ShapeDtypeStruct(arrays[-1].shape, f32),
            jax.ShapeDtypeStruct((total, RADIX, grid // RADIX, 2 * cols), f32),
        ),
        in_specs=[hbm] * len(arrays),
        out_specs=(vmem,) * 5,
        scratch_shapes=[pltpu.VMEM(x.shape, x.dtype) for x in arrays[:-1]] + [
            pltpu.SemaphoreType.DMA((len(arrays),)),
            pltpu.SemaphoreType.DMA((sems,)), pltpu.SemaphoreType.DMA((sems,)),
        ] + step_scratch(grid, 2 * cols),
        compiler_params=pltpu.CompilerParams(
            collective_id=0, has_side_effects=True, vmem_limit_bytes=12 * 2**20
        ),
        name="gather_fields",
    )(*[in_hbm(x) for x in arrays])


def grid_kernel(
    grid, f_ref, fine_ref, coarse_ref, kernel_ref, start_ref, dh_hbm, dl_hbm, h_ref, dh_ref, dl_ref,
    spread_ref, pick_ref, z_ref, z8_ref, tap_ref, spot_ref, channel_ref, load_sems
):
    loads = []
    for n in range(RADIX):
        loads.append(pltpu.make_async_copy(dh_hbm.at[n], dh_ref.at[n], load_sems.at[0, n]))
        loads.append(pltpu.make_async_copy(dl_hbm.at[n], dl_ref.at[n], load_sems.at[1, n]))
    for load in loads:
        load.start()
    channels, blocks, rows, _ = f_ref.shape
    subs = rows // FIELDS
    piece = 2 * LANES
    tap_table = kernel_ref[...]
    base = lax.axis_index("base")
    below, _ = second_pair(base, subs)

    counts = []
    for c in range(channels):
        for b in range(blocks):
            used = f_ref[c, b, 4 * subs:5 * subs, :] >= 0.0
            counts.append(jnp.sum(jnp.where(used, 1.0, 0.0)))
    filled = jnp.int32(0)
    for c in range(channels):
        for b in range(blocks):
            done = jnp.where(base == b, 2, 0) + jnp.where(below == b, 2, 0)
            for sub in range(subs):
                spot_ref[filled + sub] = b * subs + sub + done
            for ahead in range(subs // 2 + 1):
                channel_ref[lax.shift_right_logical(filled, jnp.int32(1)) + ahead] = c
            count = counts[c * blocks + b].astype(jnp.int32)
            live = lax.shift_right_logical(count + (LANES - 1), jnp.int32(LANES.bit_length() - 1))
            filled = filled + jnp.maximum(live - done, 0)
        spot_ref[filled] = -1
        filled = (filled + 1) & -2
    steps = lax.shift_right_logical(filled, jnp.int32(1))
    for ahead in range(8):
        spot_ref[filled + ahead] = -1
    for ahead in range(4):
        channel_ref[steps + ahead] = 0

    def field(step, number):
        c = channel_ref[step]
        one, two = jnp.maximum(spot_ref[2 * step], 0), jnp.maximum(spot_ref[2 * step + 1], 0)
        by = jnp.int32(subs.bit_length() - 1)
        return jnp.concatenate(
            [
                f_ref[c, lax.shift_right_logical(one, by), pl.ds(number * subs + (one & (subs - 1)), 1), :],
                f_ref[c, lax.shift_right_logical(two, by), pl.ds(number * subs + (two & (subs - 1)), 1), :],
            ],
            axis=1,
        )

    lane = lax.broadcasted_iota(jnp.int32, (1, piece), 1)

    def make_spread(step, slot):
        keep = lane < jnp.where(
            spot_ref[2 * step + 1] >= 0, piece, jnp.where(spot_ref[2 * step] >= 0, LANES, 0)
        )
        store_spread(grid, tap_table, lambda n: field(step, n), keep, slot, spread_ref, pick_ref)

    def make_z(step, slot):
        store_z(
            grid, tap_table, lambda n: field(step, n), slot,
            fine_ref, coarse_ref, spread_ref, pick_ref, z_ref, z8_ref, tap_ref,
        )

    def add_rows(step, slot):
        c = channel_ref[step]
        for first in range(RADIX):
            h_ref[c, first] += slab_of(grid, first, slot, z_ref, z8_ref, tap_ref)

    make_spread(0, 0)
    make_z(0, 0)
    make_spread(1, 1)

    def two_steps(n, carry):
        for slot in range(2):
            step = 2 * n + slot
            make_z(step + 1, 1 - slot)
            make_spread(step + 2, slot)
            add_rows(step, slot)
        return carry

    lax.fori_loop(0, (steps + 1) // 2, two_steps, 0)
    for load in loads:
        load.wait()


def grid_visibilities(fields, fine, coarse, taps_table, start, dh, dl, grid):
    channels, blocks, rows, _ = fields.shape
    most = channels * (blocks * (rows // FIELDS) + 1)
    smem = lambda n: pltpu.SMEM((n,), jnp.int32)
    vmem = pl.BlockSpec(memory_space=pltpu.VMEM)
    hbm = pl.BlockSpec(memory_space=pltpu.HBM)
    return pl.pallas_call(
        functools.partial(grid_kernel, grid),
        out_shape=(
            jax.ShapeDtypeStruct(start.shape, jnp.float32),
            jax.ShapeDtypeStruct(dh.shape, jnp.bfloat16),
            jax.ShapeDtypeStruct(dl.shape, jnp.bfloat16),
        ),
        in_specs=[vmem] * 5 + [hbm] * 2,
        out_specs=(vmem,) * 3,
        scratch_shapes=step_scratch(grid, start.shape[3]) + [
            smem(most + 16), smem(most // 2 + 16), pltpu.SemaphoreType.DMA((2, RADIX)),
        ],
        input_output_aliases={4: 0},
        compiler_params=pltpu.CompilerParams(vmem_limit_bytes=16 * 2**20),
        name="grid_visibilities",
    )(fields, fine, coarse, taps_table, start, in_hbm(dh), in_hbm(dl))


def power_kernel(
    grid, freq_count, base_count, split, scale, h_ref, dh_ref, dl_ref, bins_hbm, share_ref, spectrum_ref,
    bins_ref, bins_sem, hh_ref, hl_ref, y_ref, power_ref, recv_ref, mask_ref, value_ref, low_ref, stage_ref, stage2_ref,
    send_sems, recv_sems, sum_send_sems, sum_recv_sems
):
    freq, base = lax.axis_index("freq"), lax.axis_index("base")
    ring = [{"freq": lax.rem(freq + d, freq_count), "base": base} for d in range(1, freq_count)]
    line = [{"freq": freq, "base": lax.rem(base + d, base_count)} for d in range(1, base_count)]
    barrier = greet(ring + line)
    rows_here = bins_ref.shape[1]
    if bins_hbm.shape[1] != rows_here:
        here = pl.ds(pl.multiple_of(freq * rows_here, rows_here), rows_here)
        load_bins = pltpu.make_async_copy(bins_hbm.at[:, here], bins_ref, bins_sem)
    else:
        load_bins = pltpu.make_async_copy(bins_hbm, bins_ref, bins_sem)
    load_bins.start()

    channels = h_ref.shape[0]
    slab = grid // RADIX
    share_rows, width = share_ref.shape
    cols = width // split
    chunk = min(64, share_rows)
    parts = share_rows // chunk
    shares = slab // share_rows

    def transform(n, begin=False):
        top = pl.multiple_of((lax.rem(n, shares) * parts + n // shares) * chunk, chunk)
        for c in range(channels):
            for first in range(RADIX):
                dh = jnp.concatenate(
                    [dh_ref[first, pl.ds(top, chunk), :], dh_ref[first, pl.ds(slab + top, chunk), :]], axis=0
                )
                dl = jnp.concatenate(
                    [dl_ref[first, pl.ds(top, chunk), :], dl_ref[first, pl.ds(slab + top, chunk), :]], axis=0
                )
                if begin:
                    hh, hl = halves_of(h_ref[c, first])
                    hh_ref[c, first] = hh
                    hl_ref[c, first] = hl
                else:
                    hh, hl = hh_ref[c, first], hl_ref[c, first]
                y_ref[c % 2, first] = dot(dh, hh) + dot(dl, hh) + dot(dh, hl)
            step = min(16, chunk)
            for row in range(0, chunk, step):
                yr, yi = [], []
                for first in range(RADIX):
                    cy = y_ref[c % 2, first, row:row + step, :]
                    sy = y_ref[c % 2, first, chunk + row:chunk + row + step, :]
                    yr.append(cy[:, :cols] + sy[:, cols:])
                    yi.append(cy[:, cols:] - sy[:, :cols])
                ar, ai = yr[0] + yr[2], yi[0] + yi[2]
                br, bi = yr[0] - yr[2], yi[0] - yi[2]
                cr, ci = yr[1] + yr[3], yi[1] + yi[3]
                dr, di = yr[1] - yr[3], yi[1] - yi[3]
                outs = [
                    (ar + cr, ai + ci), (br + di, bi - dr), (ar - cr, ai - ci), (br - di, bi + dr)
                ]
                for k, (xr, xi) in enumerate(outs):
                    at = pl.ds(pl.multiple_of(k * slab + top + row, step), step)
                    value = (xr * xr + xi * xi) * scale
                    power_ref[at, :] = value if c == 0 else power_ref[at, :] + value

    def piece(n, k):
        share, part = lax.rem(n, shares), n // shares
        target = k * shares + share
        top = pl.multiple_of(target * share_rows + part * chunk, chunk)
        rows = pl.ds(pl.multiple_of(part * chunk, chunk), chunk)
        copy = pltpu.make_async_remote_copy(
            src_ref=power_ref.at[pl.ds(top, chunk), :],
            dst_ref=recv_ref.at[freq, rows, :],
            send_sem=send_sems.at[n, k], recv_sem=recv_sems.at[freq, part],
            device_id={"freq": target, "base": base}, device_id_type=MESH,
        )
        return target, top, rows, copy

    def send(n):
        for k in range(RADIX):
            target, top, rows, copy = piece(n, k)

            @pl.when(target == freq)
            def _():
                recv_ref[freq, rows, :] = power_ref[pl.ds(top, chunk), :]

            @pl.when(target != freq)
            def _():
                copy.start()

    transform(0, True)
    pl.semaphore_wait(barrier, len(ring) + len(line))
    send(0)

    def later(n, carry):
        transform(n)
        send(n)
        return carry

    lax.fori_loop(1, shares * parts, later, 0)

    high_count = NBINS // BIN_LOW
    lead = high_count // 4
    load_bins.wait()
    bins = bins_ref[...].T
    order = lax.broadcasted_iota(jnp.int32, (high_count, width), 0)
    order = lead * (order % lead) + order // lead if lead == 4 else order
    low_order = lax.broadcasted_iota(jnp.int32, (BIN_LOW, width), 0)
    for row in range(share_rows):
        at = slice(row * width, (row + 1) * width)
        bin_id = bins[row:row + 1, :]
        mask_ref[:, at] = jnp.where(order == bin_id // BIN_LOW, 1.0, 0.0).astype(jnp.bfloat16)
        low_ref[:, at] = jnp.where(low_order == bin_id % BIN_LOW, 1.0, 0.0).astype(jnp.bfloat16)
    counts = dot_rows(mask_ref[...], low_ref[...])

    totals = jnp.zeros((high_count, BIN_LOW), jnp.float32)
    for part in range(parts):
        rows = slice(part * chunk, (part + 1) * chunk)
        for d in range(1, freq_count):
            source = lax.rem(freq + d, freq_count)
            pltpu.make_async_remote_copy(
                src_ref=power_ref.at[0:chunk, :], dst_ref=recv_ref.at[source, rows, :],
                send_sem=send_sems.at[0, 0], recv_sem=recv_sems.at[source, part],
                device_id={"freq": source, "base": base}, device_id_type=MESH,
            ).wait_recv()
        for half in range(split):
            total = recv_ref[half, rows, :]
            for group in range(1, freq_count // split):
                total = total + recv_ref[group * split + half, rows, :]
            share_ref[rows, half * cols:(half + 1) * cols] = total
        for row in range(part * chunk, (part + 1) * chunk):
            at = slice(row * width, (row + 1) * width)
            out = slice((row - part * chunk) * width, (row - part * chunk + 1) * width)
            value = jnp.broadcast_to(share_ref[row:row + 1, :], (high_count, width))
            high, low = halves_of(value)
            mask = mask_ref[:, at]
            value_ref[0:high_count, out] = mask * high
            value_ref[high_count:, out] = mask * low
        span = slice(part * chunk * width, (part + 1) * chunk * width)
        sums = dot_rows(value_ref[...], low_ref[:, span])
        totals = totals + sums[:high_count] + sums[high_count:]

    def pack(x):
        return jnp.concatenate([x[lead * k:lead * (k + 1)] for k in range(4)], axis=1)

    stage_ref[freq] = jnp.concatenate([pack(totals), pack(counts)], axis=0)

    def share_out(ref, me, peers, offset):
        copies = []
        for k, peer in enumerate(peers):
            copy = pltpu.make_async_remote_copy(
                src_ref=ref.at[me], dst_ref=ref.at[me],
                send_sem=sum_send_sems.at[offset + k], recv_sem=sum_recv_sems.at[offset + k],
                device_id=peer, device_id_type=MESH,
            )
            copy.start()
            copies.append(copy)
        for copy in copies:
            copy.wait()
        total = ref[0]
        for other in range(1, ref.shape[0]):
            total = total + ref[other]
        return total

    stage2_ref[base] = share_out(stage_ref, freq, ring, 0)
    total = share_out(stage2_ref, base, line, len(ring))
    spectrum_ref[...] = total

    def finish(n, carry):
        for k in range(RADIX):
            target, _, _, copy = piece(n, k)

            @pl.when(target != freq)
            def _():
                copy.wait_send()
        return carry

    lax.fori_loop(0, shares * parts, finish, 0)


def power_and_spectrum(h, dh, dl, bins, grid, freq_count, base_count, split, width, scale):
    channels, _, slab, both = h.shape
    cols = both // 2
    share_rows = grid // freq_count
    chunk = min(64, share_rows)
    parts, shares = share_rows // chunk, slab // share_rows
    high_count = NBINS // BIN_LOW
    cells = share_rows * width
    sems = freq_count + base_count - 2
    f32, bf16 = jnp.float32, jnp.bfloat16
    vmem = pl.BlockSpec(memory_space=pltpu.VMEM)
    hbm = pl.BlockSpec(memory_space=pltpu.HBM)
    return pl.pallas_call(
        functools.partial(power_kernel, grid, freq_count, base_count, split, scale),
        out_shape=(
            jax.ShapeDtypeStruct((share_rows, width), f32),
            jax.ShapeDtypeStruct((8, 4 * BIN_LOW), f32),
        ),
        in_specs=[vmem, vmem, vmem, hbm],
        out_specs=(vmem, vmem),
        scratch_shapes=[
            pltpu.VMEM((bins.shape[0], share_rows), jnp.int32),
            pltpu.SemaphoreType.DMA,
            pltpu.VMEM(h.shape, bf16),
            pltpu.VMEM(h.shape, bf16),
            pltpu.VMEM((2, RADIX, 2 * chunk, both), f32),
            pltpu.VMEM((grid, cols), f32),
            pltpu.VMEM((freq_count, share_rows, cols), f32),
            pltpu.VMEM((high_count, cells), bf16),
            pltpu.VMEM((2 * high_count, chunk * width), bf16),
            pltpu.VMEM((BIN_LOW, cells), bf16),
            pltpu.VMEM((freq_count, 8, 4 * BIN_LOW), f32),
            pltpu.VMEM((base_count, 8, 4 * BIN_LOW), f32),
            pltpu.SemaphoreType.DMA((shares * parts, RADIX)),
            pltpu.SemaphoreType.DMA((freq_count, parts)),
            pltpu.SemaphoreType.DMA((sems,)),
            pltpu.SemaphoreType.DMA((sems,)),
        ],
        compiler_params=pltpu.CompilerParams(
            collective_id=1, has_side_effects=True, vmem_limit_bytes=24 * 2**20
        ),
        name="power_and_spectrum",
    )(h, dh, dl, in_hbm(bins))


def finish_kernel(share_ref, sums_ref, power_ref, spectrum_ref):
    power_ref[...] = share_ref[...]
    mean = sums_ref[0:4, :] / sums_ref[4:8, :]
    width = mean.shape[1]
    for n in range(4):
        spectrum_ref[n * width:(n + 1) * width] = mean[n]


def finish(share, sums):
    vmem = pl.BlockSpec(memory_space=pltpu.VMEM)
    return pl.pallas_call(
        finish_kernel,
        out_shape=(
            jax.ShapeDtypeStruct(share.shape, share.dtype), jax.ShapeDtypeStruct((NBINS,), jnp.float32)
        ),
        in_specs=[vmem, vmem],
        out_specs=(vmem, vmem),
        compiler_params=pltpu.CompilerParams(vmem_limit_bytes=4 * 2**20),
        name="finish",
    )(share, sums)


def per_device(visibility, tile_of, u_within, v_cell, kernel_index, kernel, live_count, bin_map):
    base_count = lax.axis_size("base")
    freq_count = lax.axis_size("freq")
    grid = bin_map.shape[1]
    width = grid // base_count
    split = 2 if width % (2 * LANES) == 0 and freq_count % 2 == 0 else 1
    channels_here, slots = u_within.shape
    dh, dl = transform_tables(grid)
    scale = 1.0 / (channels_here * freq_count * slots * base_count) / (Z_SCALE * W_SCALE) ** 2
    gathered = gather_fields(
        split, base_count, grid // base_count, grid, width // split,
        visibility, tile_of.transpose(0, 2, 1), u_within, v_cell, kernel_index, live_count.T, kernel.T,
    )
    h, dh, dl = grid_visibilities(*gathered, jnp.asarray(dh), jnp.asarray(dl), grid)
    share_rows = grid // freq_count
    bins = bin_map
    if share_rows % LANES:
        bins = lax.dynamic_slice_in_dim(bin_map, lax.axis_index("freq") * share_rows, share_rows, 1)
    share, sums = power_and_spectrum(
        h, dh, dl, bins, grid, freq_count, base_count, split, width, scale
    )
    return finish(share, sums)


def solution(mesh):
    in_specs = (
        P(None, "freq", "base"),
        P("freq", "base", None),
        P("freq", "base"),
        P("freq", "base"),
        P(None, "freq", "base"),
        P(),
        P("freq", "base"),
        P("base", None),
    )
    out_specs = (P("freq", "base"), P())
    return jax.shard_map(
        per_device, mesh=mesh, in_specs=in_specs, out_specs=out_specs, check_vma=False
    )
```

```python
import functools
import math

import jax
import jax.numpy as jnp
import numpy as np
from jax import lax
from jax.experimental import pallas as pl
from jax.experimental.pallas import tpu as pltpu
from jax.sharding import PartitionSpec as P

NBINS = 512
BIN_LOW = 32
KW = 8
FINE = 32
SPREAD = FINE + KW
RADIX = 4
GROUP = 16
FIELDS = 6
LANES = 128
F8 = jnp.float8_e5m2
F8W = jnp.float8_e4m3fn
Z_SCALE = 2.0 ** 9
W_SCALE = 2.0 ** 12
LIFT = 2.0 ** 9
MESH = pl.DeviceIdType.MESH


def halves_of(x):
    high = x.astype(jnp.bfloat16)
    low = (x - high.astype(jnp.float32)).astype(jnp.bfloat16)
    return high, low


@functools.lru_cache(None)
def transform_tables(grid):
    slab = grid // RADIX
    order = np.arange(slab)
    u = 2 * RADIX * (order % (slab // 2)) + RADIX * (order // (slab // 2))
    u = u[None, None, :] + np.arange(RADIX)[:, None, None]
    angle = ((np.arange(slab)[None, :, None] * u) % grid) * (2.0 * math.pi / grid)
    x = np.concatenate([np.cos(angle), np.sin(angle)], axis=1).astype(np.float32)
    high = x.astype(jnp.bfloat16)
    low = (x - high.astype(np.float32)).astype(jnp.bfloat16)
    return high, low


def dot(a, b):
    return jnp.dot(a, b, preferred_element_type=jnp.float32)


def dot_rows(a, b):
    return lax.dot_general(a, b, (((1,), (1,)), ((), ())), preferred_element_type=jnp.float32)


def in_hbm(x):
    return pltpu.with_memory_space_constraint(x, pltpu.HBM)


def greet(peers):
    barrier = pltpu.get_barrier_semaphore()
    for peer in peers:
        pl.semaphore_signal(barrier, inc=1, device_id=peer, device_id_type=MESH)
    return barrier


def phase(product, grid):
    half = grid // 2
    angle = ((product + half) & (grid - 1)) - half
    angle = angle.astype(jnp.float32) * (2.0 * math.pi / grid)
    return jnp.cos(angle), jnp.sin(angle)


def column_tables(grid, split, fine_ref, coarse_ref):
    cols = fine_ref.shape[0] // 2
    coarse_count = grid // FINE
    left = (lax.axis_index("base") * split + lax.rem(lax.axis_index("freq"), split)) * cols
    l = left + lax.broadcasted_iota(jnp.int32, (SPREAD, cols), 1)
    c, s = phase(l * lax.broadcasted_iota(jnp.int32, (SPREAD, cols), 0), grid)
    c, s = c.T, s.T
    fine = jnp.concatenate(
        [jnp.concatenate([c, s], axis=1), jnp.concatenate([-s, c], axis=1)], axis=0
    )
    fh, fl = halves_of(fine)
    fine_ref[...] = jnp.zeros_like(fine_ref)
    fine_ref[:, 0:2 * SPREAD] = fh
    fine_ref[:, 2 * SPREAD:4 * SPREAD] = fl
    fine_ref[:, 4 * SPREAD:6 * SPREAD] = fh
    l = lax.broadcasted_iota(jnp.int32, (coarse_count, coarse_count), 0)
    c, s = phase(l * lax.broadcasted_iota(jnp.int32, (coarse_count, coarse_count), 1) * FINE, grid)
    ch, cl = halves_of(jnp.concatenate([c, -s], axis=0))
    coarse_ref[:, 0:coarse_count] = ch
    coarse_ref[:, coarse_count:] = cl


def look_up(table, row):
    row = jnp.maximum(row.astype(jnp.int32), 0)
    pieces = []
    for at in range(0, row.shape[1], LANES):
        index = jnp.broadcast_to(row[:, at:at + LANES], (KW, LANES))
        pieces.append(jnp.take_along_axis(table, index, axis=1))
    return jnp.concatenate(pieces, axis=1)


def store_spread(grid, table, field, keep, slot, spread_ref, pick_ref):
    re, im = field(0), field(1)
    if keep is not None:
        re, im = jnp.where(keep, re, 0.0), jnp.where(keep, im, 0.0)
    piece = re.shape[1]
    coarse_count = grid // FINE
    v = field(3).astype(jnp.int32)
    taps_v = look_up(table, field(5))
    offset = lax.broadcasted_iota(jnp.int32, (SPREAD, piece), 0) - (v & (FINE - 1))
    spread = jnp.zeros((SPREAD, piece), jnp.float32)
    for t in range(KW):
        spread = jnp.where(offset == t, taps_v[t:t + 1, :], spread)
    re, im = re * Z_SCALE, im * Z_SCALE
    both = jnp.concatenate([spread * re, spread * im], axis=0)
    bh, bl = halves_of(both)
    pad = jnp.zeros((256 - 6 * SPREAD, piece), jnp.bfloat16)
    spread_ref[slot] = jnp.concatenate([bh, bh, bl, pad], axis=0)
    pick = lax.broadcasted_iota(jnp.int32, (2 * coarse_count, piece), 0) & (coarse_count - 1)
    pick_ref[slot] = jnp.where(pick == v // FINE, 1.0, 0.0).astype(jnp.bfloat16)


def store_z(grid, table, field, slot, fine_ref, coarse_ref, spread_ref, pick_ref, z_ref, z8_ref, tap_ref):
    cols = fine_ref.shape[0] // 2
    coarse_count = grid // FINE
    piece = z_ref.shape[1]
    zb = dot(fine_ref[...], spread_ref[slot])
    e = dot(coarse_ref[...], pick_ref[slot])
    er, ei = e[:coarse_count], e[coarse_count:]
    re, im = [], []
    for at in range(0, cols, coarse_count):
        zr, zi = zb[at:at + coarse_count], zb[cols + at:cols + at + coarse_count]
        re.append(zr * er - zi * ei)
        im.append(zr * ei + zi * er)
    for n, parts in enumerate((re, im)):
        turned = jnp.concatenate(parts, axis=0).T
        zh = turned.astype(jnp.bfloat16)
        zl = turned - zh.astype(jnp.float32)
        z_ref[slot, :, n * cols:(n + 1) * cols] = zh
        z8_ref[slot, 0:piece, n * cols:(n + 1) * cols] = turned.astype(F8)
        z8_ref[slot, piece:, n * cols:(n + 1) * cols] = (zl * LIFT).astype(F8)

    u = field(2).astype(jnp.int32)
    taps_u = look_up(table, field(4))
    residue = lax.broadcasted_iota(jnp.int32, (2 * RADIX, u.shape[1]), 0)
    tap = (residue - u) & (2 * RADIX - 1)
    row = lax.shift_right_logical(u + tap, jnp.int32((2 * RADIX).bit_length() - 1))
    weight = jnp.zeros(tap.shape, jnp.float32)
    for t in range(KW):
        weight = jnp.where(tap == t, taps_u[t:t + 1, :], weight)
    weight = weight * W_SCALE
    high = weight.astype(jnp.bfloat16).astype(jnp.float32)
    tap_ref[slot, 0] = row.astype(jnp.float32)
    tap_ref[slot, 1] = high
    tap_ref[slot, 2] = weight - high
    tap_ref[slot, 3] = high * (1.0 / LIFT)


def slab_of(grid, first, slot, z_ref, z8_ref, tap_ref):
    half = grid // (2 * RADIX)
    piece = tap_ref.shape[3]
    rows16 = lax.broadcasted_iota(jnp.int32, (GROUP, piece), 0).astype(jnp.float32)
    spots = [(rows16 + float(at)).astype(jnp.bfloat16) for at in range(0, half, GROUP)]

    def wide(kind, residue):
        x = tap_ref[slot, kind, residue:residue + 1, :]
        return jnp.broadcast_to(x, (GROUP, piece)).astype(jnp.bfloat16)

    highs, lows, shifts = [], [], []
    for residue in (first, first + RADIX):
        row, high, low, shift = (wide(kind, residue) for kind in range(4))
        zero = jnp.zeros_like(high)
        for spot in spots:
            hit = row == spot
            highs.append(jnp.where(hit, high, zero))
            lows.append(jnp.where(hit, low, zero))
            shifts.append(jnp.where(hit, shift, zero))
    wh = jnp.concatenate(highs, axis=0)
    small = [jnp.concatenate(x, axis=0).astype(F8W) for x in (lows, shifts)]
    return dot(wh, z_ref[slot]) + dot(jnp.concatenate(small, axis=1), z8_ref[slot])


def step_scratch(grid, both):
    bf16, f32 = jnp.bfloat16, jnp.float32
    piece = 2 * LANES
    return [
        pltpu.VMEM((2, 256, piece), bf16),
        pltpu.VMEM((2, 2 * (grid // FINE), piece), bf16),
        pltpu.VMEM((2, piece, both), bf16),
        pltpu.VMEM((2, 2 * piece, both), F8),
        pltpu.VMEM((2, 4, 2 * RADIX, piece), f32),
    ]


def second_pair(base, subs):
    if subs < 4:
        return lax.rem(base + lax.axis_size("base") - 1, lax.axis_size("base")), 0
    return jnp.maximum(base - 1, 0), jnp.where(base == 0, 2, 0)


def gather_kernel(
    split, base_count, tile_rows, grid, vis_hbm, tile_hbm, within_hbm, column_hbm, index_hbm, live_hbm,
    taps_hbm, out_ref, fine_ref, coarse_ref, taps_ref, h_ref,
    vis_ref, tile_ref, within_ref, column_ref, index_ref, live_ref, load_sems, send_sems, recv_sems,
    spread_ref, pick_ref, z_ref, z8_ref, tap_ref
):
    freq, base = lax.axis_index("freq"), lax.axis_index("base")
    part = lax.rem(freq, split)
    first = freq - part
    line = [{"freq": freq, "base": lax.rem(base + d, base_count)} for d in range(1, base_count)]
    mates = [{"freq": first + lax.rem(part + d, split), "base": base} for d in range(1, split)]
    barrier = greet(line + mates)
    loads = [
        pltpu.make_async_copy(a, b, load_sems.at[n])
        for n, (a, b) in enumerate([
            (vis_hbm, vis_ref), (tile_hbm, tile_ref), (within_hbm, within_ref), (column_hbm, column_ref),
            (index_hbm, index_ref), (live_hbm, live_ref), (taps_hbm, taps_ref),
        ])
    ]
    for load in loads:
        load.start()
    for load in loads:
        load.wait()
    channels, slots = within_ref.shape
    lane = lax.broadcasted_iota(jnp.int32, (1, slots), 1)
    for c in range(channels):
        is_live = lane < live_ref[0:1, c:c + 1]
        u = jnp.minimum(tile_ref[c] * tile_rows + within_ref[c:c + 1, :], grid - KW)
        fields = [
            jnp.where(is_live, vis_ref[0, c:c + 1, :], 0.0),
            jnp.where(is_live, vis_ref[1, c:c + 1, :], 0.0),
            u.astype(jnp.float32),
            column_ref[c:c + 1, :].astype(jnp.float32),
            jnp.where(is_live, index_ref[0, c:c + 1, :], -1).astype(jnp.float32),
            index_ref[1, c:c + 1, :].astype(jnp.float32),
        ]
        rows = [x[:, at:at + LANES] for x in fields for at in range(0, slots, LANES)]
        out_ref[part * channels + c, base] = jnp.concatenate(rows, axis=0)
    column_tables(grid, split, fine_ref, coarse_ref)
    pl.semaphore_wait(barrier, len(line) + len(mates))

    def block_copy(owner, peer, k):
        block = out_ref.at[pl.ds(part * channels, channels), owner]
        return pltpu.make_async_remote_copy(
            src_ref=block, dst_ref=block, send_sem=send_sems.at[k], recv_sem=recv_sems.at[k],
            device_id=peer, device_id_type=MESH,
        )

    sent = [block_copy(base, peer, k) for k, peer in enumerate(line)]
    for copy in sent:
        copy.start()
    passed = [[] for _ in mates]

    def pass_on(d):
        owner = lax.rem(base + base_count - d, base_count)
        for k, mate in enumerate(mates):
            copy = block_copy(owner, mate, len(line) + k * base_count + d)
            copy.start()
            passed[k].append(copy)

    pass_on(0)
    subs = slots // LANES
    table = taps_ref[...]

    def grid_group(d, owner, sub, begin):
        group = lax.rem(part + d, split) * channels

        def field_of(c):
            def field(number):
                rows = [out_ref[group + c, owner, pl.ds(number * subs + sub + n, 1), :] for n in range(2)]
                return jnp.concatenate(rows, axis=1)
            return field

        for c in range(channels):
            store_spread(grid, table, field_of(c), None, c % 2, spread_ref, pick_ref)
            store_z(grid, table, field_of(c), c % 2, fine_ref, coarse_ref, spread_ref, pick_ref, z_ref, z8_ref, tap_ref)
            for residue in range(RADIX):
                rows = slab_of(grid, residue, c % 2, z_ref, z8_ref, tap_ref)
                h_ref[group + c, residue] = rows if begin else h_ref[group + c, residue] + rows

    grid_group(0, base, 0, True)
    for d in range(1, split):
        passed[split - 1 - d][0].wait_recv()
        grid_group(d, base, 0, True)
    below, sub = second_pair(base, subs)
    for d in range(1, base_count):
        if d == base_count - 1 and d > 1:
            grid_group(0, below, sub, False)
        sent[d - 1].wait_recv()
        pass_on(d)
    if base_count < 3:
        grid_group(0, below, sub, False)
    for d in range(1, split):
        passed[split - 1 - d][1].wait_recv()
        grid_group(d, below, sub, False)
    for k in range(len(mates)):
        for d, copy in enumerate(passed[k]):
            copy.wait_send()
            if d > 1:
                copy.wait_recv()
    for copy in sent:
        copy.wait_send()


def gather_fields(split, base_count, tile_rows, grid, cols, *arrays):
    channels, slots = arrays[2].shape
    sems = base_count - 1 + (split - 1) * base_count
    total = channels * split
    f32, bf16 = jnp.float32, jnp.bfloat16
    vmem = pl.BlockSpec(memory_space=pltpu.VMEM)
    hbm = pl.BlockSpec(memory_space=pltpu.HBM)
    return pl.pallas_call(
        functools.partial(gather_kernel, split, base_count, tile_rows, grid),
        out_shape=(
            jax.ShapeDtypeStruct((total, base_count, FIELDS * (slots // LANES), LANES), f32),
            jax.ShapeDtypeStruct((2 * cols, 256), bf16),
            jax.ShapeDtypeStruct((2 * (grid // FINE), 2 * (grid // FINE)), bf16),
            jax.ShapeDtypeStruct(arrays[-1].shape, f32),
            jax.ShapeDtypeStruct((total, RADIX, grid // RADIX, 2 * cols), f32),
        ),
        in_specs=[hbm] * len(arrays),
        out_specs=(vmem,) * 5,
        scratch_shapes=[pltpu.VMEM(x.shape, x.dtype) for x in arrays[:-1]] + [
            pltpu.SemaphoreType.DMA((len(arrays),)),
            pltpu.SemaphoreType.DMA((sems,)), pltpu.SemaphoreType.DMA((sems,)),
        ] + step_scratch(grid, 2 * cols),
        compiler_params=pltpu.CompilerParams(
            collective_id=0, has_side_effects=True, vmem_limit_bytes=12 * 2**20
        ),
        name="gather_fields",
    )(*[in_hbm(x) for x in arrays])


def grid_kernel(
    grid, f_ref, fine_ref, coarse_ref, kernel_ref, start_ref, dh_hbm, dl_hbm, h_ref, dh_ref, dl_ref,
    spread_ref, pick_ref, z_ref, z8_ref, tap_ref, spot_ref, channel_ref, load_sems
):
    loads = []
    for n in range(RADIX):
        loads.append(pltpu.make_async_copy(dh_hbm.at[n], dh_ref.at[n], load_sems.at[0, n]))
        loads.append(pltpu.make_async_copy(dl_hbm.at[n], dl_ref.at[n], load_sems.at[1, n]))
    for load in loads:
        load.start()
    channels, blocks, rows, _ = f_ref.shape
    subs = rows // FIELDS
    piece = 2 * LANES
    tap_table = kernel_ref[...]
    base = lax.axis_index("base")
    below, _ = second_pair(base, subs)

    counts = []
    for c in range(channels):
        for b in range(blocks):
            used = f_ref[c, b, 4 * subs:5 * subs, :] >= 0.0
            counts.append(jnp.sum(jnp.where(used, 1.0, 0.0)))
    filled = jnp.int32(0)
    for c in range(channels):
        for b in range(blocks):
            done = jnp.where(base == b, 2, 0) + jnp.where(below == b, 2, 0)
            for sub in range(subs):
                spot_ref[filled + sub] = b * subs + sub + done
            for ahead in range(subs // 2 + 1):
                channel_ref[lax.shift_right_logical(filled, jnp.int32(1)) + ahead] = c
            count = counts[c * blocks + b].astype(jnp.int32)
            live = lax.shift_right_logical(count + (LANES - 1), jnp.int32(LANES.bit_length() - 1))
            filled = filled + jnp.maximum(live - done, 0)
        spot_ref[filled] = -1
        filled = (filled + 1) & -2
    steps = lax.shift_right_logical(filled, jnp.int32(1))
    for ahead in range(8):
        spot_ref[filled + ahead] = -1
    for ahead in range(4):
        channel_ref[steps + ahead] = 0

    def field(step, number):
        c = channel_ref[step]
        one, two = jnp.maximum(spot_ref[2 * step], 0), jnp.maximum(spot_ref[2 * step + 1], 0)
        by = jnp.int32(subs.bit_length() - 1)
        return jnp.concatenate(
            [
                f_ref[c, lax.shift_right_logical(one, by), pl.ds(number * subs + (one & (subs - 1)), 1), :],
                f_ref[c, lax.shift_right_logical(two, by), pl.ds(number * subs + (two & (subs - 1)), 1), :],
            ],
            axis=1,
        )

    lane = lax.broadcasted_iota(jnp.int32, (1, piece), 1)

    def make_spread(step, slot):
        keep = lane < jnp.where(
            spot_ref[2 * step + 1] >= 0, piece, jnp.where(spot_ref[2 * step] >= 0, LANES, 0)
        )
        store_spread(grid, tap_table, lambda n: field(step, n), keep, slot, spread_ref, pick_ref)

    def make_z(step, slot):
        store_z(
            grid, tap_table, lambda n: field(step, n), slot,
            fine_ref, coarse_ref, spread_ref, pick_ref, z_ref, z8_ref, tap_ref,
        )

    def add_rows(step, slot):
        c = channel_ref[step]
        for first in range(RADIX):
            h_ref[c, first] += slab_of(grid, first, slot, z_ref, z8_ref, tap_ref)

    make_spread(0, 0)
    make_z(0, 0)
    make_spread(1, 1)

    def two_steps(n, carry):
        for slot in range(2):
            step = 2 * n + slot
            make_z(step + 1, 1 - slot)
            make_spread(step + 2, slot)
            add_rows(step, slot)
        return carry

    lax.fori_loop(0, lax.shift_right_logical(steps, jnp.int32(1)), two_steps, 0)

    @pl.when((steps & 1) == 1)
    def _():
        add_rows(steps - 1, 0)

    for load in loads:
        load.wait()


def grid_visibilities(fields, fine, coarse, taps_table, start, dh, dl, grid):
    channels, blocks, rows, _ = fields.shape
    most = channels * (blocks * (rows // FIELDS) + 1)
    smem = lambda n: pltpu.SMEM((n,), jnp.int32)
    vmem = pl.BlockSpec(memory_space=pltpu.VMEM)
    hbm = pl.BlockSpec(memory_space=pltpu.HBM)
    return pl.pallas_call(
        functools.partial(grid_kernel, grid),
        out_shape=(
            jax.ShapeDtypeStruct(start.shape, jnp.float32),
            jax.ShapeDtypeStruct(dh.shape, jnp.bfloat16),
            jax.ShapeDtypeStruct(dl.shape, jnp.bfloat16),
        ),
        in_specs=[vmem] * 5 + [hbm] * 2,
        out_specs=(vmem,) * 3,
        scratch_shapes=step_scratch(grid, start.shape[3]) + [
            smem(most + 16), smem(most // 2 + 16), pltpu.SemaphoreType.DMA((2, RADIX)),
        ],
        input_output_aliases={4: 0},
        compiler_params=pltpu.CompilerParams(vmem_limit_bytes=16 * 2**20),
        name="grid_visibilities",
    )(fields, fine, coarse, taps_table, start, in_hbm(dh), in_hbm(dl))


def power_kernel(
    grid, freq_count, base_count, split, scale, h_ref, dh_ref, dl_ref, bins_hbm, share_ref, spectrum_ref,
    bins_ref, bins_sem, hh_ref, hl_ref, y_ref, power_ref, recv_ref, mask_ref, value_ref, low_ref, stage_ref, stage2_ref,
    send_sems, recv_sems, sum_send_sems, sum_recv_sems
):
    freq, base = lax.axis_index("freq"), lax.axis_index("base")
    ring = [{"freq": lax.rem(freq + d, freq_count), "base": base} for d in range(1, freq_count)]
    line = [{"freq": freq, "base": lax.rem(base + d, base_count)} for d in range(1, base_count)]
    barrier = greet(ring + line)
    rows_here = bins_ref.shape[1]
    if bins_hbm.shape[1] != rows_here:
        here = pl.ds(pl.multiple_of(freq * rows_here, rows_here), rows_here)
        load_bins = pltpu.make_async_copy(bins_hbm.at[:, here], bins_ref, bins_sem)
    else:
        load_bins = pltpu.make_async_copy(bins_hbm, bins_ref, bins_sem)
    load_bins.start()

    channels = h_ref.shape[0]
    slab = grid // RADIX
    share_rows, width = share_ref.shape
    cols = width // split
    chunk = min(64, share_rows)
    parts = share_rows // chunk
    shares = slab // share_rows

    def transform(n, begin=False):
        top = pl.multiple_of((lax.rem(n, shares) * parts + n // shares) * chunk, chunk)
        for c in range(channels):
            for first in range(RADIX):
                dh = jnp.concatenate(
                    [dh_ref[first, pl.ds(top, chunk), :], dh_ref[first, pl.ds(slab + top, chunk), :]], axis=0
                )
                dl = jnp.concatenate(
                    [dl_ref[first, pl.ds(top, chunk), :], dl_ref[first, pl.ds(slab + top, chunk), :]], axis=0
                )
                if begin:
                    hh, hl = halves_of(h_ref[c, first])
                    hh_ref[c, first] = hh
                    hl_ref[c, first] = hl
                else:
                    hh, hl = hh_ref[c, first], hl_ref[c, first]
                y_ref[c % 2, first] = dot(dh, hh) + dot(dl, hh) + dot(dh, hl)
            step = min(16, chunk)
            for row in range(0, chunk, step):
                yr, yi = [], []
                for first in range(RADIX):
                    cy = y_ref[c % 2, first, row:row + step, :]
                    sy = y_ref[c % 2, first, chunk + row:chunk + row + step, :]
                    yr.append(cy[:, :cols] + sy[:, cols:])
                    yi.append(cy[:, cols:] - sy[:, :cols])
                ar, ai = yr[0] + yr[2], yi[0] + yi[2]
                br, bi = yr[0] - yr[2], yi[0] - yi[2]
                cr, ci = yr[1] + yr[3], yi[1] + yi[3]
                dr, di = yr[1] - yr[3], yi[1] - yi[3]
                outs = [
                    (ar + cr, ai + ci), (br + di, bi - dr), (ar - cr, ai - ci), (br - di, bi + dr)
                ]
                for k, (xr, xi) in enumerate(outs):
                    at = pl.ds(pl.multiple_of(k * slab + top + row, step), step)
                    value = (xr * xr + xi * xi) * scale
                    power_ref[at, :] = value if c == 0 else power_ref[at, :] + value

    def piece(n, k):
        share, part = lax.rem(n, shares), n // shares
        target = k * shares + share
        top = pl.multiple_of(target * share_rows + part * chunk, chunk)
        rows = pl.ds(pl.multiple_of(part * chunk, chunk), chunk)
        copy = pltpu.make_async_remote_copy(
            src_ref=power_ref.at[pl.ds(top, chunk), :],
            dst_ref=recv_ref.at[freq, rows, :],
            send_sem=send_sems.at[n, k], recv_sem=recv_sems.at[freq, part],
            device_id={"freq": target, "base": base}, device_id_type=MESH,
        )
        return target, top, rows, copy

    def send(n):
        for k in range(RADIX):
            target, top, rows, copy = piece(n, k)

            @pl.when(target == freq)
            def _():
                recv_ref[freq, rows, :] = power_ref[pl.ds(top, chunk), :]

            @pl.when(target != freq)
            def _():
                copy.start()

    transform(0, True)
    pl.semaphore_wait(barrier, len(ring) + len(line))
    send(0)

    def later(n, carry):
        transform(n)
        send(n)
        return carry

    lax.fori_loop(1, shares * parts, later, 0)

    high_count = NBINS // BIN_LOW
    lead = high_count // 4
    load_bins.wait()
    bins = bins_ref[...].T
    order = lax.broadcasted_iota(jnp.int32, (high_count, width), 0)
    order = lead * (order % lead) + order // lead if lead == 4 else order
    low_order = lax.broadcasted_iota(jnp.int32, (BIN_LOW, width), 0)
    for row in range(share_rows):
        at = slice(row * width, (row + 1) * width)
        bin_id = bins[row:row + 1, :]
        mask_ref[:, at] = jnp.where(order == bin_id // BIN_LOW, 1.0, 0.0).astype(jnp.bfloat16)
        low_ref[:, at] = jnp.where(low_order == bin_id % BIN_LOW, 1.0, 0.0).astype(jnp.bfloat16)
    counts = dot_rows(mask_ref[...], low_ref[...])

    totals = jnp.zeros((high_count, BIN_LOW), jnp.float32)
    for part in range(parts):
        rows = slice(part * chunk, (part + 1) * chunk)
        for d in range(1, freq_count):
            source = lax.rem(freq + d, freq_count)
            pltpu.make_async_remote_copy(
                src_ref=power_ref.at[0:chunk, :], dst_ref=recv_ref.at[source, rows, :],
                send_sem=send_sems.at[0, 0], recv_sem=recv_sems.at[source, part],
                device_id={"freq": source, "base": base}, device_id_type=MESH,
            ).wait_recv()
        for half in range(split):
            total = recv_ref[half, rows, :]
            for group in range(1, freq_count // split):
                total = total + recv_ref[group * split + half, rows, :]
            share_ref[rows, half * cols:(half + 1) * cols] = total
        for row in range(part * chunk, (part + 1) * chunk):
            at = slice(row * width, (row + 1) * width)
            out = slice((row - part * chunk) * width, (row - part * chunk + 1) * width)
            value = jnp.broadcast_to(share_ref[row:row + 1, :], (high_count, width))
            high, low = halves_of(value)
            mask = mask_ref[:, at]
            value_ref[0:high_count, out] = mask * high
            value_ref[high_count:, out] = mask * low
        span = slice(part * chunk * width, (part + 1) * chunk * width)
        sums = dot_rows(value_ref[...], low_ref[:, span])
        totals = totals + sums[:high_count] + sums[high_count:]

    def pack(x):
        return jnp.concatenate([x[lead * k:lead * (k + 1)] for k in range(4)], axis=1)

    stage_ref[freq] = jnp.concatenate([pack(totals), pack(counts)], axis=0)

    def share_out(ref, me, peers, offset):
        copies = []
        for k, peer in enumerate(peers):
            copy = pltpu.make_async_remote_copy(
                src_ref=ref.at[me], dst_ref=ref.at[me],
                send_sem=sum_send_sems.at[offset + k], recv_sem=sum_recv_sems.at[offset + k],
                device_id=peer, device_id_type=MESH,
            )
            copy.start()
            copies.append(copy)
        for copy in copies:
            copy.wait()
        total = ref[0]
        for other in range(1, ref.shape[0]):
            total = total + ref[other]
        return total

    stage2_ref[base] = share_out(stage_ref, freq, ring, 0)
    total = share_out(stage2_ref, base, line, len(ring))
    spectrum_ref[...] = total

    def finish(n, carry):
        for k in range(RADIX):
            target, _, _, copy = piece(n, k)

            @pl.when(target != freq)
            def _():
                copy.wait_send()
        return carry

    lax.fori_loop(0, shares * parts, finish, 0)


def power_and_spectrum(h, dh, dl, bins, grid, freq_count, base_count, split, width, scale):
    channels, _, slab, both = h.shape
    cols = both // 2
    share_rows = grid // freq_count
    chunk = min(64, share_rows)
    parts, shares = share_rows // chunk, slab // share_rows
    high_count = NBINS // BIN_LOW
    cells = share_rows * width
    sems = freq_count + base_count - 2
    f32, bf16 = jnp.float32, jnp.bfloat16
    vmem = pl.BlockSpec(memory_space=pltpu.VMEM)
    hbm = pl.BlockSpec(memory_space=pltpu.HBM)
    return pl.pallas_call(
        functools.partial(power_kernel, grid, freq_count, base_count, split, scale),
        out_shape=(
            jax.ShapeDtypeStruct((share_rows, width), f32),
            jax.ShapeDtypeStruct((8, 4 * BIN_LOW), f32),
        ),
        in_specs=[vmem, vmem, vmem, hbm],
        out_specs=(vmem, vmem),
        scratch_shapes=[
            pltpu.VMEM((bins.shape[0], share_rows), jnp.int32),
            pltpu.SemaphoreType.DMA,
            pltpu.VMEM(h.shape, bf16),
            pltpu.VMEM(h.shape, bf16),
            pltpu.VMEM((2, RADIX, 2 * chunk, both), f32),
            pltpu.VMEM((grid, cols), f32),
            pltpu.VMEM((freq_count, share_rows, cols), f32),
            pltpu.VMEM((high_count, cells), bf16),
            pltpu.VMEM((2 * high_count, chunk * width), bf16),
            pltpu.VMEM((BIN_LOW, cells), bf16),
            pltpu.VMEM((freq_count, 8, 4 * BIN_LOW), f32),
            pltpu.VMEM((base_count, 8, 4 * BIN_LOW), f32),
            pltpu.SemaphoreType.DMA((shares * parts, RADIX)),
            pltpu.SemaphoreType.DMA((freq_count, parts)),
            pltpu.SemaphoreType.DMA((sems,)),
            pltpu.SemaphoreType.DMA((sems,)),
        ],
        compiler_params=pltpu.CompilerParams(
            collective_id=1, has_side_effects=True, vmem_limit_bytes=24 * 2**20
        ),
        name="power_and_spectrum",
    )(h, dh, dl, in_hbm(bins))


def finish_kernel(share_ref, sums_ref, power_ref, spectrum_ref):
    power_ref[...] = share_ref[...]
    mean = sums_ref[0:4, :] / sums_ref[4:8, :]
    width = mean.shape[1]
    for n in range(4):
        spectrum_ref[n * width:(n + 1) * width] = mean[n]


def finish(share, sums):
    vmem = pl.BlockSpec(memory_space=pltpu.VMEM)
    return pl.pallas_call(
        finish_kernel,
        out_shape=(
            jax.ShapeDtypeStruct(share.shape, share.dtype), jax.ShapeDtypeStruct((NBINS,), jnp.float32)
        ),
        in_specs=[vmem, vmem],
        out_specs=(vmem, vmem),
        compiler_params=pltpu.CompilerParams(vmem_limit_bytes=4 * 2**20),
        name="finish",
    )(share, sums)


def per_device(visibility, tile_of, u_within, v_cell, kernel_index, kernel, live_count, bin_map):
    base_count = lax.axis_size("base")
    freq_count = lax.axis_size("freq")
    grid = bin_map.shape[1]
    width = grid // base_count
    split = 2 if width % (2 * LANES) == 0 and freq_count % 2 == 0 else 1
    channels_here, slots = u_within.shape
    dh, dl = transform_tables(grid)
    scale = 1.0 / (channels_here * freq_count * slots * base_count) / (Z_SCALE * W_SCALE) ** 2
    gathered = gather_fields(
        split, base_count, grid // base_count, grid, width // split,
        visibility, tile_of.transpose(0, 2, 1), u_within, v_cell, kernel_index, live_count.T, kernel.T,
    )
    h, dh, dl = grid_visibilities(*gathered, jnp.asarray(dh), jnp.asarray(dl), grid)
    share_rows = grid // freq_count
    bins = bin_map
    if share_rows % LANES:
        bins = lax.dynamic_slice_in_dim(bin_map, lax.axis_index("freq") * share_rows, share_rows, 1)
    share, sums = power_and_spectrum(
        h, dh, dl, bins, grid, freq_count, base_count, split, width, scale
    )
    return finish(share, sums)


def solution(mesh):
    in_specs = (
        P(None, "freq", "base"),
        P("freq", "base", None),
        P("freq", "base"),
        P("freq", "base"),
        P(None, "freq", "base"),
        P(),
        P("freq", "base"),
        P("base", None),
    )
    out_specs = (P("freq", "base"), P())
    return jax.shard_map(
        per_device, mesh=mesh, in_specs=in_specs, out_specs=out_specs, check_vma=False
    )
```
